128 devices in a mesh: chain: 8 (over x, core), quad: 16 (over z, y).
Axes of the slice: x: 4, y: 4, z: 4, core: 2. Of those that a mesh axis runs over, the one named last changes fastest.
Arguments:
- sections: bfloat16 [8, 4096, 4096], P('chain', 'quad'), may hold values from -8 to 8
- anchor: bfloat16 [4096, 4096], P('quad'), may hold values from -8 to 8
Outputs:
- registered: bfloat16 [8, 4096, 4096], P('chain', 'quad')
- accumulated: float32 [8, 64, 128], P('chain')
The draws below stay inside these ranges and needn't reach their ends.
All inputs are finite; a program needn't handle non-finite values.
Results may differ from the reference program's by a relative error of at most 0.00135.
The reference program's roundings to bfloat16 on the way count: a program that leaves them out, or rounds other values in their place, can miss the bound.
Values may be sent and summed in bfloat16 or wider, within the bound.
No kernel may reach another device: no remote copies, remote signals or barrier semaphores. Data moves between devices by JAX's collectives and lax.ppermute only.
A program may use at most 128 MiB of HBM per device.

```python
import math
import jax
import jax.numpy as jnp
from jax import lax

GRID_SIZE = 64
ITERATIONS = 4
HEIGHT = 4096
COLUMNS = 4096
SLICES = 8


def box_blur(values, window, which_axis):
    lead_pad = window // 2 + 1
    tail_pad = window - 1 - window // 2
    pad_spec = [(0, 0), (0, 0)]
    pad_spec[which_axis] = (lead_pad, tail_pad)
    padded = jnp.pad(values, pad_spec, mode='wrap')
    running = jnp.cumsum(padded, axis=which_axis)
    length = values.shape[which_axis]
    upper_sums = lax.slice_in_dim(running, window, window + length, axis=which_axis)
    lower_sums = lax.slice_in_dim(running, 0, length, axis=which_axis)
    return (upper_sums - lower_sums) / window


def mode_table(point_count, mode_count):
    positions = (jnp.arange(point_count, dtype=jnp.float32) + 0.5) / point_count
    orders = jnp.arange(mode_count, dtype=jnp.float32)
    return jnp.cos(math.pi * positions[:, None] * orders[None, :])


def stack_helper(key):
    base_key = jax.random.fold_in(key, 4111)
    key_list = jax.random.split(base_key, 4)
    row_spread, col_spread, floor_gain, background, noise_level, sway_scale = (3.0, 1.5, 0.5, 0.3, 0.25, 0.3)
    texture = jax.random.normal(key_list[0], (HEIGHT, COLUMNS), jnp.float32)
    for which_axis in (0, 1):
        texture = box_blur(box_blur(texture, 3, which_axis), 3, which_axis)
    texture = texture - jnp.mean(texture)
    texture = texture / jnp.sqrt(jnp.mean(texture * texture))
    row_pos = (jnp.arange(HEIGHT, dtype=jnp.float32) + 0.5) / HEIGHT
    col_pos = (jnp.arange(COLUMNS, dtype=jnp.float32) + 0.5) / COLUMNS
    gain_field = floor_gain * jnp.exp(math.log(row_spread) * row_pos[:, None] + math.log(col_spread) * col_pos[None, :])
    row_modes = mode_table(HEIGHT, 4)
    col_modes = mode_table(COLUMNS, 4)
    steps_xy = sway_scale * jax.random.normal(key_list[1], (SLICES + 1, 2, 4, 4), jnp.float32)
    totals = jnp.cumsum(steps_xy, axis=0)
    stains = jnp.exp(jax.random.uniform(key_list[2], (SLICES + 1,), jnp.float32, -0.25, 0.25))
    flat_texture = texture.reshape(-1)
    row_coord = jnp.arange(HEIGHT, dtype=jnp.float32)[:, None]
    col_coord = jnp.arange(COLUMNS, dtype=jnp.float32)[None, :]

    def one_slice(slice_number):
        mixing = totals[slice_number]
        move_x = jnp.dot(jnp.dot(row_modes, mixing[0]), col_modes.T)
        move_y = jnp.dot(jnp.dot(row_modes, mixing[1]), col_modes.T)
        pos_y = jnp.clip(row_coord + move_y, 0.0, HEIGHT - 1.0)
        pos_x = jnp.clip(col_coord + move_x, 0.0, COLUMNS - 1.0)
        floor_y = jnp.floor(pos_y)
        floor_x = jnp.floor(pos_x)
        frac_y = pos_y - floor_y
        frac_x = pos_x - floor_x
        low_y = floor_y.astype(jnp.int32)
        low_x = floor_x.astype(jnp.int32)
        high_y = jnp.minimum(low_y + 1, HEIGHT - 1)
        high_x = jnp.minimum(low_x + 1, COLUMNS - 1)
        sample = (1.0 - frac_y) * (1.0 - frac_x) * flat_texture[low_y * COLUMNS + low_x]
        sample = sample + (1.0 - frac_y) * frac_x * flat_texture[low_y * COLUMNS + high_x]
        sample = sample + frac_y * (1.0 - frac_x) * flat_texture[high_y * COLUMNS + low_x]
        sample = sample + frac_y * frac_x * flat_texture[high_y * COLUMNS + high_x]
        noise_field = jax.random.normal(jax.random.fold_in(key_list[3], slice_number), (HEIGHT, COLUMNS), jnp.float32)
        section_image = stains[slice_number] * gain_field * sample + background + noise_level * noise_field
        return jnp.clip(section_image, -8.0, 8.0)
    return lax.map(one_slice, jnp.arange(SLICES + 1, dtype=jnp.int32))


def draw_sections(key, part):
    return stack_helper(key)[1:].astype(jnp.bfloat16)


def draw_anchor(key, part):
    return stack_helper(key)[0].astype(jnp.bfloat16)


def setup_inputs(seed: int = 0) -> dict:
    streams_of = jax.random.split(jax.random.key(seed), 3)
    return {
        "sections": draw_sections(jax.random.fold_in(streams_of[2], 71), 0),
        "anchor": draw_anchor(jax.random.fold_in(streams_of[2], 71), 0),
    }


EPSILON = 1e-06
SMOOTHING = 0.25
EXACT_PRECISION = lax.Precision.HIGHEST

def spline_weight(offset):
    distance = jnp.abs(offset)
    near_part = 2.0 / 3.0 - distance * distance + 0.5 * distance * distance * distance
    remain = 2.0 - distance
    far_part = remain * remain * remain / 6.0
    return jnp.where(distance < 1.0, near_part, jnp.where(distance < 2.0, far_part, 0.0 * distance))

def spline_basis(first_row, pixel_count, extent):
    spacing = extent // GRID_SIZE
    pixels = (first_row + jnp.arange(pixel_count, dtype=jnp.int32)).astype(jnp.float32)
    knot_pos = jnp.arange(GRID_SIZE, dtype=jnp.int32).astype(jnp.float32)
    offset = (pixels[:, None] + 0.5) / spacing - knot_pos[None, :] - 0.5
    return spline_weight(offset)

def slopes(images):
    padded = jnp.pad(images, ((0, 0), (1, 1), (1, 1)))
    along_x = 0.5 * (padded[:, 1:-1, 2:] - padded[:, 1:-1, :-2])
    along_y = 0.5 * (padded[:, 2:, 1:-1] - padded[:, :-2, 1:-1])
    return (along_x, along_y)

def displace(coefficients, row_basis, col_half):
    row_mixed = jnp.einsum('hg,bgk->bhk', row_basis, coefficients, precision=EXACT_PRECISION)
    row_mixed = row_mixed.astype(jnp.bfloat16).astype(jnp.float32)
    col_wide = col_half.astype(jnp.float32)
    shift_x = jnp.einsum('bhg,wg->bhw', row_mixed[:, :, :GRID_SIZE], col_wide, precision=EXACT_PRECISION)
    shift_y = jnp.einsum('bhg,wg->bhw', row_mixed[:, :, GRID_SIZE:], col_wide, precision=EXACT_PRECISION)
    return (shift_x, shift_y)

def project(field_x, field_y, row_basis, col_half):
    col_wide = col_half.astype(jnp.float32)
    rounded_x = field_x.astype(jnp.bfloat16).astype(jnp.float32)
    rounded_y = field_y.astype(jnp.bfloat16).astype(jnp.float32)
    cols_x = jnp.einsum('bhw,wg->bhg', rounded_x, col_wide, precision=EXACT_PRECISION)
    cols_y = jnp.einsum('bhw,wg->bhg', rounded_y, col_wide, precision=EXACT_PRECISION)
    joined = jnp.concatenate([cols_x, cols_y], axis=2)
    return jnp.einsum('hg,bhk->bgk', row_basis, joined, precision=EXACT_PRECISION)

def normalized(gradient):
    magnitude = lax.optimization_barrier(jnp.mean(gradient * gradient, axis=(1, 2), keepdims=True))
    return gradient / jnp.sqrt(magnitude + EPSILON)

def ncc_direction(moving, fixed_image, coefficients, row_basis, col_half):
    along_x, along_y = slopes(moving)
    shift_x, shift_y = displace(coefficients, row_basis, col_half)
    warped = moving + shift_x * along_x + shift_y * along_y
    pixel_count = moving.shape[1] * moving.shape[2]
    centred_f = fixed_image - lax.optimization_barrier(jnp.mean(fixed_image, axis=(1, 2), keepdims=True))
    centred_m = warped - lax.optimization_barrier(jnp.mean(warped, axis=(1, 2), keepdims=True))
    moving_var = lax.optimization_barrier(jnp.sum(centred_m * centred_m, axis=(1, 2), keepdims=True))
    cross_var = lax.optimization_barrier(jnp.sum(centred_f * centred_m, axis=(1, 2), keepdims=True))
    denominator = jnp.sqrt(moving_var + EPSILON)
    ncc_score = cross_var / denominator
    pixel_grad = pixel_count * (centred_f / denominator - ncc_score / (moving_var + EPSILON) * centred_m)
    return normalized(project(pixel_grad * along_x, pixel_grad * along_y, row_basis, col_half))

def reference(sections, anchor):
    slice_total, height, columns = sections.shape
    row_basis = spline_basis(0, height, height)
    col_half = spline_basis(0, columns, columns).astype(jnp.bfloat16)
    step_rate = 1.0 / ITERATIONS
    previous = jnp.concatenate([anchor[None], sections[:-1]], axis=0)
    moving_blocks = sections.reshape(slice_total, 1, height, columns)
    fixed_blocks = previous.reshape(slice_total, 1, height, columns)
    coefficients = jnp.zeros((slice_total, GRID_SIZE, 2 * GRID_SIZE), jnp.float32)

    def one_block(packed):
        moving, fixed_image, block_coef = packed
        return ncc_direction(moving.astype(jnp.float32), fixed_image.astype(jnp.float32), block_coef, row_basis, col_half)
    for iteration in range(ITERATIONS):
        shaped = coefficients.reshape(slice_total, 1, GRID_SIZE, 2 * GRID_SIZE)
        direction = lax.map(one_block, (moving_blocks, fixed_blocks, shaped))
        direction = direction.reshape(slice_total, GRID_SIZE, 2 * GRID_SIZE)
        padded = jnp.pad(coefficients, ((1, 1), (0, 0), (0, 0)))
        smooth = padded[:-2] - 2.0 * coefficients + padded[2:]
        coefficients = coefficients + step_rate * direction + SMOOTHING * smooth
    accumulated = jnp.cumsum(coefficients, axis=0)

    def warp_block(packed):
        moving, block_coef = packed
        moving = moving.astype(jnp.float32)
        along_x, along_y = slopes(moving)
        shift_x, shift_y = displace(block_coef, row_basis, col_half)
        return (moving + shift_x * along_x + shift_y * along_y).astype(jnp.bfloat16)
    registered = lax.map(warp_block, (moving_blocks, accumulated.reshape(slice_total, 1, GRID_SIZE, 2 * GRID_SIZE)))
    registered = registered.reshape(slice_total, height, columns)
    return (registered, accumulated)
```

```python
import jax
import jax.numpy as jnp
import numpy as np
from jax import lax
from jax.experimental import pallas as pl
from jax.experimental.pallas import tpu as pltpu
from jax.sharding import PartitionSpec as P

GRID = 64
SPACING = 64
ROWS = 256
COLS = 4096
BLOCK = 1024
STEPS = COLS // BLOCK
CHUNK = 32
EXT = 72
PIXELS = 4096.0 * 4096.0
EPS = 1e-6
RATE = 0.25
SMOOTH = 0.25
BF = jnp.bfloat16
F32 = jnp.float32


def weight(offset, xp):
    d = xp.abs(offset)
    near = 2.0 / 3.0 - d * d + 0.5 * d * d * d
    r = 2.0 - d
    far = r * r * r / 6.0
    return xp.where(d < 1.0, near, xp.where(d < 2.0, far, 0.0 * d))


def local_rows():
    r = np.arange(ROWS, dtype=np.float32)
    j = np.arange(8, dtype=np.float32) - 2.0
    off = (r[:, None] + np.float32(0.5)) / np.float32(SPACING) - j[None, :] - np.float32(0.5)
    return weight(off.astype(np.float32), np).astype(np.float32)


def hi_lo(a):
    hi = a.astype(BF)
    return hi, (a - hi.astype(F32)).astype(BF)


def split3(a):
    hi = a.astype(BF)
    rest = a - hi.astype(F32)
    mid = rest.astype(BF)
    lo = (rest - mid.astype(F32)).astype(BF)
    return jnp.concatenate([hi.astype(F32), mid.astype(F32), lo.astype(F32)], axis=0).astype(BF)


def sum3(a, n):
    return a[0:n] + a[n : 2 * n] + a[2 * n : 3 * n]


def two(a):
    hi = a.astype(np.dtype(BF)).astype(np.float32)
    return np.concatenate([hi, a - hi], 0)


def host_tables():
    r8 = local_rows()
    pairs = np.zeros((32, ROWS), np.float32)
    c8 = r8.astype(np.dtype(BF)).astype(np.float32)
    lanes = np.zeros((BLOCK, 128), np.float32)
    cols = np.zeros((BLOCK, 128), np.float32)
    place = np.zeros((STEPS * 128, 256), np.float32)
    put = np.zeros((STEPS * 128, 128), np.float32)
    for s in range(4):
        cols[256 * s : 256 * s + 256, 8 * s : 8 * s + 8] = c8
    for d in range(4):
        for e in range(8 - d):
            pairs[d * 8 + e] = r8[:, e] * r8[:, e + d]
            for s in range(4):
                lanes[256 * s : 256 * s + 256, 32 * s + 8 * d + e] = c8[:, e] * c8[:, e + d]
                for t in range(STEPS):
                    i = 16 * t + 4 * s - 2 + e
                    if i >= 0 and i + d < GRID:
                        place[128 * t + 32 * s + 8 * d + e, 64 * d + i] = 1.0
    for t in range(STEPS):
        for s in range(4):
            for e in range(8):
                i = 16 * t + 4 * s - 2 + e
                if 0 <= i < GRID:
                    put[128 * t + 8 * s + e, i] = 1.0
    diff = np.zeros((8, ROWS), np.float32)
    diff[:, 1:] += 0.5 * r8.T[:, :-1]
    diff[:, :-1] -= 0.5 * r8.T[:, 1:]
    lanes_hi = lanes.astype(np.dtype(BF)).astype(np.float32)
    table = np.concatenate([lanes_hi, lanes - lanes_hi, cols], 1)
    plain = np.concatenate([two(r8.T), two(diff), np.ones((16, ROWS), np.float32)], 0)
    edge = np.stack([-0.5 * r8[0], 0.5 * r8[ROWS - 1]], 0).reshape(16, 1) * np.ones((1, 128), np.float32)
    bf = [jnp.asarray(a.astype(np.dtype(BF))) for a in (two(pairs), two(r8.T), plain, table, place, put)]
    return r8, bf, edge


def slope_tables():
    down = 0.5 * (np.eye(ROWS, k=1) - np.eye(ROWS, k=-1))
    across = np.zeros((512, 256), np.float32)
    o = np.arange(256)
    across[o + 129, o] = 0.5
    across[o + 127, o] = -0.5
    return jnp.asarray(down.astype(np.dtype(BF))), jnp.asarray(across.astype(np.dtype(BF)))


def col_table():
    x = jnp.arange(COLS, dtype=jnp.int32).astype(F32)
    j = jnp.arange(GRID, dtype=jnp.int32).astype(F32)
    return weight((x[None, :] + 0.5) / SPACING - j[:, None] - 0.5, jnp).astype(BF)


def dot(a, b):
    return jnp.dot(a, b, preferred_element_type=F32)


def rims(pos_ref, left_ref, right_ref, up_ref, dn_ref, step):
    left = jnp.where(step > 0, left_ref[...].astype(F32), 0.0).astype(BF)
    right = jnp.where(step < STEPS - 1, right_ref[...].astype(F32), 0.0).astype(BF)
    up = jnp.where(pos_ref[1] > 0, up_ref[...].astype(F32), 0.0)
    dn = jnp.where(pos_ref[1] < 15, dn_ref[...].astype(F32), 0.0)
    return left, right, up, dn


def slopes(m_ref, rim, down_ref, across_ref, xs, ys, s):
    left, right, up, dn = rim
    at = pl.ds(256 * s, 256)
    if s == 0:
        wide = jnp.concatenate([left, m_ref[:, 0:384]], axis=1)
    elif s == BLOCK // 256 - 1:
        wide = jnp.concatenate([m_ref[:, BLOCK - 384 : BLOCK], right], axis=1)
    else:
        wide = m_ref[:, 256 * s - 128 : 256 * s + 384]
    xs[:, at] = dot(wide, across_ref[...])
    ys[:, at] = dot(down_ref[...], m_ref[:, at])
    ys[0:1, at] = ys[0:1, at] - 0.5 * up[:, 256 * s : 256 * s + 256]
    ys[ROWS - 1 : ROWS, at] = ys[ROWS - 1 : ROWS, at] + 0.5 * dn[:, 256 * s : 256 * s + 256]


def fold8(a):
    return jnp.sum(a.reshape(CHUNK // 8, 8, a.shape[1]), axis=0)


def lanes_to_row(a):
    s = jnp.sum(a, axis=0, keepdims=True)
    out = s[:, 0:128]
    for t in range(1, s.shape[1] // 128):
        out = out + s[:, 128 * t : 128 * t + 128]
    return out


def rows_of(lin, hi, lo):
    a = dot(lin, hi)
    b = dot(lin, lo)
    return a[0:8] + a[8:16] + b[0:8]


def stage0(pos_ref, m_ref, left_ref, right_ref, up_ref, dn_ref, down_ref, across_ref, pairs_ref, lin_ref, plain_ref, tab_ref, place_ref, put_ref, edge_ref, h_ref, p_ref, xs, ys, fxx, fxy, fyy, mxh, mxl, myh, myl, zacc, lacc, sums):
    step = pl.program_id(0)
    rim = rims(pos_ref, left_ref, right_ref, up_ref, dn_ref, step)
    pairs = pairs_ref[...]
    lin = lin_ref[...]
    sumsq = jnp.zeros((8, 256), F32)
    t_parts, lx, ly = [], [], []
    for s in range(BLOCK // 256):
        at = pl.ds(256 * s, 256)
        slopes(m_ref, rim, down_ref, across_ref, xs, ys, s)
        for c in range(ROWS // CHUNK):
            rows = pl.ds(CHUNK * c, CHUNK)
            m, x, y = m_ref[rows, at].astype(F32), xs[rows, at], ys[rows, at]
            fxx[rows, at] = (x * x).astype(BF)
            fxy[rows, at] = (x * y).astype(BF)
            fyy[rows, at] = (y * y).astype(BF)
            mxh[rows, at], mxl[rows, at] = hi_lo(m * x)
            myh[rows, at], myl[rows, at] = hi_lo(m * y)
            sumsq = sumsq + fold8(m * m)
        trio = []
        for f in (fxx, fxy, fyy):
            t = dot(pairs, f[:, at])
            trio.append(t[0:32] + t[32:64])
        t_parts.append(jnp.concatenate(trio, axis=0))
        lx.append(rows_of(lin, mxh[:, at], mxl[:, at]))
        ly.append(rows_of(lin, myh[:, at], myl[:, at]))
    t_hi, t_lo = hi_lo(jnp.concatenate(t_parts, axis=1))
    z = dot(t_hi, tab_ref[:, 0:256]) + dot(t_lo, tab_ref[:, 0:256])
    zacc[pl.ds(96 * step, 96), :] = z[:, 0:128] + z[:, 128:256]
    ext = jnp.concatenate([rim[0], m_ref[...], rim[1]], axis=1)
    ones = dot(plain_ref[...], ext)
    l1 = ones[0:8] + ones[8:16]
    l1x = 0.5 * (pltpu.roll(l1, BLOCK + 255, 1) - pltpu.roll(l1, 1, 1))[:, 128 : 128 + BLOCK]
    l1y = (ones[16:24] + ones[24:32])[:, 128 : 128 + BLOCK]
    l1y = l1y + edge_ref[0:8, 0:1] * rim[2] + edge_ref[8:16, 0:1] * rim[3]
    rows4 = jnp.concatenate([jnp.concatenate(lx, axis=1), jnp.concatenate(ly, axis=1), l1x, l1y], axis=0)
    lacc[pl.ds(32 * step, 32), :] = sum3(dot(split3(rows4), tab_ref[:, 256:384]), 32)
    both = jnp.concatenate([lanes_to_row(ones[32:33, 128 : 128 + BLOCK]), lanes_to_row(sumsq), jnp.zeros((6, 128), F32)], axis=0)

    @pl.when(step == 0)
    def _():
        sums[...] = both

    @pl.when(step > 0)
    def _():
        sums[...] += both

    @pl.when(step == STEPS - 1)
    def _():
        h = jnp.zeros((288, 256), F32)
        p = jnp.zeros((96, 128), F32)
        for t in range(STEPS):
            h = h + dot(split3(zacc[96 * t : 96 * t + 96, :]), place_ref[128 * t : 128 * t + 128, :])
            p = p + dot(split3(lacc[32 * t : 32 * t + 32, :]), put_ref[128 * t : 128 * t + 128, :])
        h = sum3(h, 96)
        hi, lo = hi_lo(h)
        low = [lo[32 * t : 32 * t + 16, 0:128] for t in range(3)]
        for t in range(16):
            h_ref[t, 0:96, :] = hi
            h_ref[t, 96:112, :] = jnp.concatenate(low[0:2], axis=1)
            h_ref[t, 112:128, :] = jnp.concatenate([low[2], jnp.zeros((16, 128), BF)], axis=1)
        p = sum3(p, 32)
        p_ref[0:8, :] = p[0:8] + pltpu.roll(p[8:16], 64, 1)
        p_ref[8:16, :] = p[16:24] + pltpu.roll(p[24:32], 64, 1)
        p_ref[16:24, :] = sums[...]


def stage1(pos_ref, m_ref, left_ref, right_ref, up_ref, dn_ref, down_ref, across_ref, lin_ref, tab_ref, put_ref, anchor_ref, prior_ref, p_ref, out_ref, xs, ys, fxh, fxl, fyh, fyl, lacc, sums):
    step = pl.program_id(0)
    rim = rims(pos_ref, left_ref, right_ref, up_ref, dn_ref, step)
    lin = lin_ref[...]
    cross = jnp.zeros((8, 256), F32)
    whole_sum = jnp.zeros((8, 256), F32)
    first = pos_ref[0] == 0
    lx, ly = [], []
    for s in range(BLOCK // 256):
        at = pl.ds(256 * s, 256)
        slopes(m_ref, rim, down_ref, across_ref, xs, ys, s)
        for c in range(ROWS // CHUNK):
            rows = pl.ds(CHUNK * c, CHUNK)
            m, x, y = m_ref[rows, at].astype(F32), xs[rows, at], ys[rows, at]
            f = jnp.where(first, anchor_ref[rows, at].astype(F32), prior_ref[rows, at].astype(F32))
            fxh[rows, at], fxl[rows, at] = hi_lo(f * x)
            fyh[rows, at], fyl[rows, at] = hi_lo(f * y)
            cross = cross + fold8(f * m)
            whole_sum = whole_sum + fold8(f)
        lx.append(rows_of(lin, fxh[:, at], fxl[:, at]))
        ly.append(rows_of(lin, fyh[:, at], fyl[:, at]))
    rows2 = jnp.concatenate([jnp.concatenate(lx, axis=1), jnp.concatenate(ly, axis=1)], axis=0)
    lacc[pl.ds(16 * step, 16), :] = sum3(dot(split3(rows2), tab_ref[:, 256:384]), 16)
    both = jnp.concatenate([lanes_to_row(cross), lanes_to_row(whole_sum), jnp.zeros((6, 128), F32)], axis=0)

    @pl.when(step == 0)
    def _():
        sums[...] = both

    @pl.when(step > 0)
    def _():
        sums[...] += both

    @pl.when(step == STEPS - 1)
    def _():
        p = jnp.zeros((48, 128), F32)
        for t in range(STEPS):
            p = p + dot(split3(lacc[16 * t : 16 * t + 16, :]), put_ref[128 * t : 128 * t + 128, :])
        p = sum3(p, 16)
        for t in range(16):
            out_ref[t, 0:8, :] = p[0:8] + pltpu.roll(p[8:16], 64, 1)
            out_ref[t, 8:16, :] = sums[...]
            out_ref[t, 16:40, :] = p_ref[...]


def shifted(a, by, axis):
    n = a.shape[axis]
    by = by % n
    return a if by == 0 else pltpu.roll(a, by, axis)


def stacked(pieces):
    pad = jnp.zeros((8, pieces[0].shape[1]), F32)
    even = jnp.concatenate(pieces[0::2] + [pad], axis=0)
    odd = jnp.concatenate(pieces[1::2] + [pad], axis=0)
    return even + pltpu.roll(odd, 4, 0)


def build_operator(h_ref, a1, a2):
    lane = lax.broadcasted_iota(jnp.int32, (EXT, 128), 1)
    low = lane < 64
    for dj in range(4):
        grid = []
        for comp in range(3):
            r = 4 * comp + dj
            base = 16 * (r // 2)
            off = 8 * (r % 2)
            pieces = []
            for q in range(16):
                piece = h_ref[q, base : base + 16, :].astype(F32)[off : off + 8, :]
                if dj < 2:
                    at = 96 + 16 * (comp // 2)
                    side = 128 * (comp % 2)
                    rest = h_ref[q, at : at + 16, side : side + 128].astype(F32)[8 * dj : 8 * dj + 8, :]
                    piece = jnp.concatenate([piece[:, 0:128] + rest, piece[:, 128:256]], axis=1)
                pieces.append(piece)
            grid.append(stacked(pieces))
        for pair in range(2):
            xx, xy, yy = [g[:, 128 * pair : 128 * pair + 128] for g in grid]
            xx_s, xy_s, yy_s = [pltpu.roll(v, 64, 1) for v in (xx, xy, yy)]
            for odd in range(2):
                di = 2 * pair + odd
                if odd == 0:
                    one = jnp.where(low, xx, yy_s)
                    two = jnp.where(low, xy, xy_s)
                else:
                    one = jnp.where(low, xx_s, yy)
                    two = jnp.where(low, xy_s, xy)
                a1[dj * 7 + 3 + di] = one
                a2[dj * 7 + 3 + di] = two
                if di > 0:
                    a1[dj * 7 + 3 - di] = pltpu.roll(one, di, 1)
                    a2[dj * 7 + 3 - di] = pltpu.roll(two, di, 1)


def apply_operator(a1, a2, c):
    cs = pltpu.roll(c, 64, 1)
    plain = [(shifted(c, -di, 1), shifted(cs, -di, 1)) for di in range(-3, 4)]
    y = jnp.zeros((EXT, 128), F32)
    for dj in range(4):
        ahead = jnp.zeros((EXT, 128), F32)
        back = jnp.zeros((EXT, 128), F32)
        for t in range(7):
            p, s = plain[t]
            u, v = a1[dj * 7 + t], a2[dj * 7 + t]
            ahead = ahead + u * shifted(p, -dj, 0) + v * shifted(s, -dj, 0)
            if dj:
                back = back + u * p + v * s
        y = y + ahead
        if dj:
            y = y + pltpu.roll(back, dj, 0)
    return y


def total(a):
    return jnp.sum(jnp.sum(a, axis=0, keepdims=True), axis=1, keepdims=True)


def fields(p_ref):
    row = lax.broadcasted_iota(jnp.int32, (EXT, 128), 0)
    valid = (row >= 2) & (row < 66)
    out = []
    for at in (0, 16, 24):
        out.append(jnp.where(valid, stacked([p_ref[q, at : at + 8, :] for q in range(16)]), 0.0))
    sums = []
    for at in (8, 9, 32, 33):
        acc = p_ref[0, at : at + 1, :]
        for q in range(1, 16):
            acc = acc + p_ref[q, at : at + 1, :]
        sums.append(jnp.sum(acc, axis=1, keepdims=True))
    return valid, out, sums


def direction(valid, grads, sums, c, hc):
    gf, gm, g1 = grads
    s_fm, s_f, s_m, s_mm = sums
    mean_f = s_f / PIXELS
    if c is None:
        s_w, s_ww, s_fw, gw = s_m, s_mm, s_fm, gm
    else:
        s_w = s_m + total(g1 * c)
        s_ww = s_mm + total(c * (2.0 * gm + hc))
        s_fw = s_fm + total(gf * c)
        gw = gm + hc
    mean_w = s_w / PIXELS
    var = s_ww - PIXELS * mean_w * mean_w
    cross = s_fw - PIXELS * mean_f * mean_w
    den = jnp.sqrt(var + EPS)
    ratio = cross / den / (var + EPS)
    g = PIXELS * ((gf - mean_f * g1) / den - ratio * (gw - mean_w * g1))
    g = jnp.where(valid, g, 0.0)
    return g / jnp.sqrt(total(g * g) / 8192.0 + EPS)


def solve_a(h_ref, p_ref, out_ref, lead_ref, a1, a2):
    build_operator(h_ref, a1, a2)
    valid, grads, sums = fields(p_ref)
    c = RATE * direction(valid, grads, sums, None, None)
    hc = apply_operator(a1, a2, c)
    out_ref[0:EXT, :] = c
    lead_ref[...] = c
    out_ref[EXT : 2 * EXT, :] = direction(valid, grads, sums, c, hc)


def solve_b(pos_ref, h_ref, p_ref, own_ref, prev_ref, next_ref, prev2_ref, next2_ref, out_ref, a1, a2):
    k = pos_ref[0]
    build_operator(h_ref, a1, a2)
    valid, grads, sums = fields(p_ref)

    def lap(a, b, c):
        return a - 2.0 * b + c

    c1, d1 = own_ref[0:EXT, :], own_ref[EXT : 2 * EXT, :]
    has_prev, has_next = k > 0, k < 7
    cl, dl = [jnp.where(has_prev, v, 0.0) for v in (prev_ref[0:EXT, :], prev_ref[EXT : 2 * EXT, :])]
    cr, dr = [jnp.where(has_next, v, 0.0) for v in (next_ref[0:EXT, :], next_ref[EXT : 2 * EXT, :])]
    cll = jnp.where(k > 1, prev2_ref[...], 0.0)
    crr = jnp.where(k < 6, next2_ref[...], 0.0)
    c2 = c1 + RATE * d1 + SMOOTH * lap(cl, c1, cr)
    c2l = jnp.where(has_prev, cl + RATE * dl + SMOOTH * lap(cll, cl, c1), 0.0)
    c2r = jnp.where(has_next, cr + RATE * dr + SMOOTH * lap(c1, cr, crr), 0.0)
    d2 = direction(valid, grads, sums, c2, apply_operator(a1, a2, c2))
    c3 = c2 + RATE * d2 + SMOOTH * lap(c2l, c2, c2r)
    d3 = direction(valid, grads, sums, c3, apply_operator(a1, a2, c3))
    u = c3 + RATE * d3
    for t in range(8):
        w = SMOOTH * (jnp.where(k == t + 1, 1.0, 0.0) - jnp.where(k == t, 1.0, 0.0) - jnp.where(k == 0, 1.0, 0.0))
        out_ref[t] = jnp.where(k <= t, 1.0, 0.0) * u + w * c3


def finish(pos_ref, m_ref, left_ref, right_ref, up_ref, dn_ref, down_ref, across_ref, parts_ref, r8_ref, turned_ref, out_ref, acc_ref, xs, ys, sx, sy, total_ref, mixed):
    step = pl.program_id(0)
    rim = rims(pos_ref, left_ref, right_ref, up_ref, dn_ref, step)

    @pl.when(step == 0)
    def _():
        acc = parts_ref[0]
        for t in range(1, 8):
            acc = acc + parts_ref[t]
        total_ref[...] = acc
        acc_ref[...] = total_ref[2:66, :]
        c8 = total_ref[pl.ds(4 * pos_ref[1], 8), :]
        rows = jnp.dot(r8_ref[...], c8, precision=lax.Precision.HIGHEST, preferred_element_type=F32)
        mixed[...] = rows.astype(BF)

    for s in range(BLOCK // 256):
        at = pl.ds(256 * s, 256)
        slopes(m_ref, rim, down_ref, across_ref, xs, ys, s)
        sx[:, at] = dot(mixed[:, 0:64], turned_ref[:, at])
        sy[:, at] = dot(mixed[:, 64:128], turned_ref[:, at])
        for c in range(ROWS // CHUNK):
            rows = pl.ds(CHUNK * c, CHUNK)
            m = m_ref[rows, at].astype(F32)
            out_ref[rows, at] = (m + sx[rows, at] * xs[rows, at] + sy[rows, at] * ys[rows, at]).astype(BF)


def strip_specs():
    return [
        pl.BlockSpec((ROWS, BLOCK), lambda j, pos: (0, j)),
        pl.BlockSpec((ROWS, 128), lambda j, pos: (0, jnp.maximum(8 * j - 1, 0))),
        pl.BlockSpec((ROWS, 128), lambda j, pos: (0, jnp.minimum(8 * j + 8, COLS // 128 - 1))),
        pl.BlockSpec((1, BLOCK), lambda j, pos: (0, j)),
        pl.BlockSpec((1, BLOCK), lambda j, pos: (0, j)),
        whole((ROWS, ROWS)),
        whole((512, 256)),
    ]


def whole(shape):
    return pl.BlockSpec(shape, lambda j, pos: (0,) * len(shape))


def ring(array, axis, by):
    n = lax.axis_size(axis)
    return lax.ppermute(array, axis, [(i, (i + by) % n) for i in range(n)])


FIELD = pltpu.VMEM((ROWS, BLOCK), BF)
WIDE = pltpu.VMEM((ROWS, BLOCK), F32)


def local(sections, anchor):
    strip = sections[0]
    pos = jnp.stack([lax.axis_index("chain"), lax.axis_index("quad")]).astype(jnp.int32)
    r8, (pairs, lin, plain, table, place, put), edge = host_tables()
    down, across = slope_tables()
    prior = ring(strip, "chain", 1)
    up = ring(strip[ROWS - 1 : ROWS], "quad", 1)
    dn = ring(strip[0:1], "quad", -1)
    turned = col_table()
    blocks = (strip, strip, strip, up, dn, down, across)
    h, p = pl.pallas_call(
        stage0,
        grid_spec=pltpu.PrefetchScalarGridSpec(
            num_scalar_prefetch=1,
            grid=(STEPS,),
            in_specs=strip_specs() + [whole(a.shape) for a in (pairs, lin, plain, table, place, put, edge)],
            out_specs=[whole((16, 128, 256)), whole((24, 128))],
            scratch_shapes=[WIDE] * 2 + [FIELD] * 7 + [pltpu.VMEM((96 * STEPS, 128), F32), pltpu.VMEM((32 * STEPS, 128), F32), pltpu.VMEM((8, 128), F32)],
        ),
        out_shape=[jax.ShapeDtypeStruct((16, 128, 256), BF), jax.ShapeDtypeStruct((24, 128), F32)],
        name="stage0",
    )(pos, *blocks, pairs, lin, plain, table, place, put, jnp.asarray(edge))
    h_all = lax.all_to_all(h, "quad", 0, 0, tiled=True)
    packed = pl.pallas_call(
        stage1,
        grid_spec=pltpu.PrefetchScalarGridSpec(
            num_scalar_prefetch=1,
            grid=(STEPS,),
            in_specs=strip_specs()
            + [whole(a.shape) for a in (lin, table, put)]
            + [
                pl.BlockSpec((ROWS, BLOCK), lambda j, pos: (0, jnp.where(pos[0] == 0, j, 0))),
                pl.BlockSpec((ROWS, BLOCK), lambda j, pos: (0, jnp.where(pos[0] == 0, 0, j))),
                whole((24, 128)),
            ],
            out_specs=whole((16, 40, 128)),
            scratch_shapes=[WIDE] * 2 + [FIELD] * 4 + [pltpu.VMEM((16 * STEPS, 128), F32), pltpu.VMEM((8, 128), F32)],
        ),
        out_shape=jax.ShapeDtypeStruct((16, 40, 128), F32),
        name="stage1",
    )(pos, *blocks, lin, table, put, anchor, prior, p)
    p_all = lax.all_to_all(packed, "quad", 0, 0, tiled=True)
    operator = [pltpu.VMEM((28, EXT, 128), F32)] * 2
    first, lead = pl.pallas_call(
        solve_a,
        out_shape=[jax.ShapeDtypeStruct((2 * EXT, 128), F32), jax.ShapeDtypeStruct((EXT, 128), F32)],
        scratch_shapes=operator,
        name="solve_a",
        compiler_params=pltpu.CompilerParams(vmem_limit_bytes=12 << 20),
    )(h_all, p_all)
    around = [ring(first, "chain", 1), ring(first, "chain", -1), ring(lead, "chain", 2), ring(lead, "chain", -2)]
    vm = pl.BlockSpec(memory_space=pltpu.VMEM)
    parts = pl.pallas_call(
        solve_b,
        in_specs=[pl.BlockSpec(memory_space=pltpu.SMEM)] + [vm] * 7,
        out_shape=jax.ShapeDtypeStruct((8, EXT, 128), F32),
        scratch_shapes=operator,
        name="solve_b",
        compiler_params=pltpu.CompilerParams(vmem_limit_bytes=12 << 20),
    )(pos, h_all, p_all, first, *around)
    parts = lax.all_to_all(parts, "chain", 0, 0, tiled=True)
    registered, accumulated = pl.pallas_call(
        finish,
        grid_spec=pltpu.PrefetchScalarGridSpec(
            num_scalar_prefetch=1,
            grid=(STEPS,),
            in_specs=strip_specs() + [whole((8, EXT, 128)), whole((ROWS, 8)), pl.BlockSpec((GRID, BLOCK), lambda j, pos: (0, j))],
            out_specs=[pl.BlockSpec((ROWS, BLOCK), lambda j, pos: (0, j)), whole((GRID, 128))],
            scratch_shapes=[WIDE] * 4 + [pltpu.VMEM((EXT, 128), F32), pltpu.VMEM((ROWS, 128), BF)],
        ),
        out_shape=[jax.ShapeDtypeStruct((ROWS, COLS), BF), jax.ShapeDtypeStruct((GRID, 128), F32)],
        name="finish",
    )(pos, *blocks, parts, jnp.asarray(r8), turned)
    return registered[None], accumulated[None]


def solution(mesh):
    in_specs = (P("chain", "quad", None), P("quad", None))
    out_specs = (P("chain", "quad", None), P("chain", None, None))
    return jax.shard_map(local, mesh=mesh, in_specs=in_specs, out_specs=out_specs, check_vma=False)
```

```python
import jax
import jax.numpy as jnp
import numpy as np
from jax import lax
from jax.experimental import pallas as pl
from jax.experimental.pallas import tpu as pltpu
from jax.sharding import PartitionSpec as P

GRID = 64
SPACING = 64
ROWS = 256
COLS = 4096
BLOCK = 1024
STEPS = COLS // BLOCK
CHUNK = 32
EXT = 72
PIXELS = 4096.0 * 4096.0
EPS = 1e-6
RATE = 0.25
SMOOTH = 0.25
BF = jnp.bfloat16
F32 = jnp.float32


def weight(offset, xp):
    d = xp.abs(offset)
    near = 2.0 / 3.0 - d * d + 0.5 * d * d * d
    r = 2.0 - d
    far = r * r * r / 6.0
    return xp.where(d < 1.0, near, xp.where(d < 2.0, far, 0.0 * d))


def local_rows():
    r = np.arange(ROWS, dtype=np.float32)
    j = np.arange(8, dtype=np.float32) - 2.0
    off = (r[:, None] + np.float32(0.5)) / np.float32(SPACING) - j[None, :] - np.float32(0.5)
    return weight(off.astype(np.float32), np).astype(np.float32)


def hi_lo(a):
    hi = a.astype(BF)
    return hi, (a - hi.astype(F32)).astype(BF)


def split3(a):
    hi = a.astype(BF)
    rest = a - hi.astype(F32)
    mid = rest.astype(BF)
    lo = (rest - mid.astype(F32)).astype(BF)
    return jnp.concatenate([hi.astype(F32), mid.astype(F32), lo.astype(F32)], axis=0).astype(BF)


def sum3(a, n):
    return a[0:n] + a[n : 2 * n] + a[2 * n : 3 * n]


def two(a):
    hi = a.astype(np.dtype(BF)).astype(np.float32)
    return np.concatenate([hi, a - hi], 0)


def host_tables():
    r8 = local_rows()
    pairs = np.zeros((32, ROWS), np.float32)
    c8 = r8.astype(np.dtype(BF)).astype(np.float32)
    lanes = np.zeros((BLOCK, 128), np.float32)
    cols = np.zeros((BLOCK, 128), np.float32)
    place = np.zeros((STEPS * 128, 256), np.float32)
    put = np.zeros((STEPS * 128, 128), np.float32)
    for s in range(4):
        cols[256 * s : 256 * s + 256, 8 * s : 8 * s + 8] = c8
    for d in range(4):
        for e in range(8 - d):
            pairs[d * 8 + e] = r8[:, e] * r8[:, e + d]
            for s in range(4):
                lanes[256 * s : 256 * s + 256, 32 * s + 8 * d + e] = c8[:, e] * c8[:, e + d]
                for t in range(STEPS):
                    i = 16 * t + 4 * s - 2 + e
                    if i >= 0 and i + d < GRID:
                        place[128 * t + 32 * s + 8 * d + e, 64 * d + i] = 1.0
    for t in range(STEPS):
        for s in range(4):
            for e in range(8):
                i = 16 * t + 4 * s - 2 + e
                if 0 <= i < GRID:
                    put[128 * t + 8 * s + e, i] = 1.0
    diff = np.zeros((8, ROWS), np.float32)
    diff[:, 1:] += 0.5 * r8.T[:, :-1]
    diff[:, :-1] -= 0.5 * r8.T[:, 1:]
    lanes_hi = lanes.astype(np.dtype(BF)).astype(np.float32)
    down = 0.5 * (np.eye(ROWS, k=1) - np.eye(ROWS, k=-1))
    across = np.zeros((512, 256), np.float32)
    o = np.arange(256)
    across[o + 129, o] = 0.5
    across[o + 127, o] = -0.5
    plain = np.concatenate([two(r8.T), two(diff), np.ones((16, ROWS), np.float32)], 0)
    wide = np.concatenate([lanes_hi, lanes - lanes_hi], 1)
    halves = np.concatenate([np.concatenate([cols[0:512], cols[512:1024]], 1), np.concatenate([put[0:256], put[256:512]], 1)], 0)
    blob = np.concatenate([down, across, two(pairs), two(r8.T), plain, wide, place, halves], 0)
    edge = np.stack([-0.5 * r8[0], 0.5 * r8[ROWS - 1]], 0).reshape(16, 1) * np.ones((1, 128), np.float32)
    return r8, jnp.asarray(blob.astype(np.dtype(BF))), jnp.asarray(edge.astype(np.float32))


DOWN, ACROSS, PAIRS, LIN, PLAIN, TABLE, PLACE, COLT, PUT, BLOB = 0, 256, 768, 832, 848, 896, 1920, 2432, 2944, 3200


def col_part(blob_ref, lhs):
    return dot(lhs[:, 0:512], blob_ref[COLT : COLT + 512, 0:128]) + dot(lhs[:, 512:1024], blob_ref[COLT : COLT + 512, 128:256])


def put_rows(blob_ref, t):
    return blob_ref[PUT + 128 * (t % 2) : PUT + 128 * (t % 2) + 128, 128 * (t // 2) : 128 * (t // 2) + 128]


def col_table():
    x = jnp.arange(COLS, dtype=jnp.int32).astype(F32)
    j = jnp.arange(GRID, dtype=jnp.int32).astype(F32)
    return weight((x[None, :] + 0.5) / SPACING - j[:, None] - 0.5, jnp).astype(BF)


def dot(a, b):
    return jnp.dot(a, b, preferred_element_type=F32)


def tile(step, size=BLOCK):
    return pl.ds(pl.multiple_of(size * step, size), size)


def slopes(pos_ref, m_ref, up_ref, dn_ref, blob_ref, lhs, xs, ys, step):
    start = BLOCK * step
    left = m_ref[:, pl.ds(pl.multiple_of(jnp.maximum(start - 128, 0), 128), 128)]
    right = m_ref[:, pl.ds(pl.multiple_of(jnp.minimum(start + BLOCK, COLS - 128), 128), 128)]
    left = jnp.where(step > 0, left.astype(F32), 0.0).astype(BF)
    right = jnp.where(step < STEPS - 1, right.astype(F32), 0.0).astype(BF)
    block = m_ref[:, tile(step)]
    ext = jnp.concatenate([left, block, right], axis=1)
    stack = jnp.concatenate([ext[:, 256 * s : 256 * s + 512] for s in range(4)], axis=0)
    x = dot(stack, blob_ref[ACROSS : ACROSS + 512, :])
    for s in range(4):
        xs[:, pl.ds(pl.multiple_of(start + 256 * s, 256), 256)] = x[256 * s : 256 * s + 256]
    up = jnp.where(pos_ref[1] > 0, up_ref[:, tile(step)].astype(F32), 0.0)
    dn = jnp.where(pos_ref[1] < 15, dn_ref[:, tile(step)].astype(F32), 0.0)
    both = dot(jnp.concatenate([blob_ref[DOWN : DOWN + 256, :], lhs], axis=0), block)
    at = tile(step)
    ys[:, at] = both[0:256]
    ys[0:1, at] = ys[0:1, at] - 0.5 * up
    ys[ROWS - 1 : ROWS, at] = ys[ROWS - 1 : ROWS, at] + 0.5 * dn
    return up, dn, both[256:]


def fold8(a):
    return jnp.sum(a.reshape(CHUNK // 8, 8, a.shape[1]), axis=0)


def lanes_to_row(a):
    s = jnp.sum(a, axis=0, keepdims=True)
    out = s[:, 0:128]
    for t in range(1, s.shape[1] // 128):
        out = out + s[:, 128 * t : 128 * t + 128]
    return out


def rows_of(lin, hi, lo):
    a = dot(lin, hi)
    b = dot(lin, lo)
    return a[0:8] + a[8:16] + b[0:8]


def stage0(pos_ref, m_ref, up_ref, dn_ref, blob_ref, edge_ref, h_ref, p_ref, xs, ys, fxx, fxy, fyy, mxh, mxl, myh, myl, zacc, lacc, l1_ref, sums):
    sums[...] = jnp.zeros((8, 128), F32)

    def body(step, carry):
        up, dn, ones = slopes(pos_ref, m_ref, up_ref, dn_ref, blob_ref, blob_ref[PLAIN : PLAIN + 48, :], xs, ys, step)
        pairs = blob_ref[PAIRS : PAIRS + 64, :]
        lin = blob_ref[LIN : LIN + 16, :]
        sumsq = jnp.zeros((8, 256), F32)
        t_parts, lx, ly = [], [], []
        for s in range(BLOCK // 256):
            at = pl.ds(256 * s, 256)
            from_m = pl.ds(pl.multiple_of(BLOCK * step + 256 * s, 256), 256)
            for c in range(ROWS // CHUNK):
                rows = pl.ds(CHUNK * c, CHUNK)
                m, x, y = m_ref[rows, from_m].astype(F32), xs[rows, from_m], ys[rows, from_m]
                fxx[rows, at] = (x * x).astype(BF)
                fxy[rows, at] = (x * y).astype(BF)
                fyy[rows, at] = (y * y).astype(BF)
                mxh[rows, at], mxl[rows, at] = hi_lo(m * x)
                myh[rows, at], myl[rows, at] = hi_lo(m * y)
                sumsq = sumsq + fold8(m * m)
            trio = []
            for f in (fxx, fxy, fyy):
                t = dot(pairs, f[:, at])
                trio.append(t[0:32] + t[32:64])
            t_parts.append(jnp.concatenate(trio, axis=0))
            lx.append(rows_of(lin, mxh[:, at], mxl[:, at]))
            ly.append(rows_of(lin, myh[:, at], myl[:, at]))
        t_hi, t_lo = hi_lo(jnp.concatenate(t_parts, axis=1))
        z = dot(jnp.concatenate([t_hi, t_lo], axis=0), blob_ref[TABLE : TABLE + 1024, :])
        z = z[0:96] + z[96:192]
        zacc[tile(step, 96), :] = z[:, 0:128] + z[:, 128:256]
        l1_ref[:, tile(step)] = ones[0:8] + ones[8:16]
        l1y = ones[16:24] + ones[24:32]
        l1y = l1y + edge_ref[0:8, 0:1] * up + edge_ref[8:16, 0:1] * dn
        rows3 = jnp.concatenate([jnp.concatenate(lx, axis=1), jnp.concatenate(ly, axis=1), l1y], axis=0)
        lacc[tile(step, 24), :] = sum3(col_part(blob_ref, split3(rows3)), 24)
        sums[0:1, :] += lanes_to_row(ones[32:33])
        sums[1:2, :] += lanes_to_row(sumsq)
        return carry

    lax.fori_loop(0, STEPS, body, 0)
    l1 = l1_ref[...]
    col = lax.broadcasted_iota(jnp.int32, l1.shape, 1)
    after = jnp.where(col < COLS - 1, pltpu.roll(l1, COLS - 1, 1), 0.0)
    before = jnp.where(col > 0, pltpu.roll(l1, 1, 1), 0.0)
    l1x = split3(0.5 * (after - before))
    h = jnp.zeros((288, 256), F32)
    p = jnp.zeros((96, 128), F32)
    for t in range(STEPS):
        h = h + dot(split3(zacc[96 * t : 96 * t + 96, :]), blob_ref[PLACE + 128 * t : PLACE + 128 * t + 128, :])
        one = sum3(col_part(blob_ref, l1x[:, BLOCK * t : BLOCK * t + BLOCK]), 8)
        p = p + dot(split3(jnp.concatenate([lacc[24 * t : 24 * t + 24, :], one], axis=0)), put_rows(blob_ref, t))
    h_ref[...] = sum3(h, 96)
    p = sum3(p, 32)
    p_ref[0:8, :] = p[0:8] + pltpu.roll(p[8:16], 64, 1)
    p_ref[8:16, :] = p[24:32] + pltpu.roll(p[16:24], 64, 1)
    p_ref[16:24, :] = sums[...]


def cross_part(pos_ref, m_ref, xs, ys, blob_ref, anchor_hbm, prior_hbm, fxh, fxl, fyh, fyl, f_ref, fetched, lacc, sums):
    def fetch(i, from_hbm):
        return pltpu.make_async_copy(from_hbm.at[:, tile(i)], f_ref.at[:, tile(i)], fetched.at[i])

    for i in range(STEPS):

        @pl.when(pos_ref[0] == 0)
        def _():
            fetch(i, anchor_hbm).start()

        @pl.when(pos_ref[0] > 0)
        def _():
            fetch(i, prior_hbm).start()

    sums[...] = jnp.zeros((8, 128), F32)

    def body(step, carry):
        fetch(step, prior_hbm).wait()
        lin = blob_ref[LIN : LIN + 16, :]
        cross = jnp.zeros((8, 256), F32)
        whole_sum = jnp.zeros((8, 256), F32)
        lx, ly = [], []
        for s in range(BLOCK // 256):
            at = pl.ds(256 * s, 256)
            from_m = pl.ds(pl.multiple_of(BLOCK * step + 256 * s, 256), 256)
            for c in range(ROWS // CHUNK):
                rows = pl.ds(CHUNK * c, CHUNK)
                m, x, y = m_ref[rows, from_m].astype(F32), xs[rows, from_m], ys[rows, from_m]
                f = f_ref[rows, from_m].astype(F32)
                fxh[rows, at], fxl[rows, at] = hi_lo(f * x)
                fyh[rows, at], fyl[rows, at] = hi_lo(f * y)
                cross = cross + fold8(f * m)
                whole_sum = whole_sum + fold8(f)
            lx.append(rows_of(lin, fxh[:, at], fxl[:, at]))
            ly.append(rows_of(lin, fyh[:, at], fyl[:, at]))
        rows2 = jnp.concatenate([jnp.concatenate(lx, axis=1), jnp.concatenate(ly, axis=1)], axis=0)
        lacc[tile(step, 16), :] = sum3(col_part(blob_ref, split3(rows2)), 16)
        sums[0:1, :] += lanes_to_row(cross)
        sums[1:2, :] += lanes_to_row(whole_sum)
        return carry

    lax.fori_loop(0, STEPS, body, 0)
    p = jnp.zeros((48, 128), F32)
    for i in range(STEPS):
        p = p + dot(split3(lacc[16 * i : 16 * i + 16, :]), put_rows(blob_ref, i))
    p = sum3(p, 16)
    return p[0:8] + pltpu.roll(p[8:16], 64, 1)


def rows8(shape):
    return lax.broadcasted_iota(jnp.int32, shape, 0) % 8


def stage1(pos_ref, m_ref, xs, ys, blob_ref, anchor_hbm, prior_hbm, h_ref, p_ref, out_ref, *scratch):
    sums = scratch[-1]
    part = cross_part(pos_ref, m_ref, xs, ys, blob_ref, anchor_hbm, prior_hbm, *scratch)
    row = rows8((8, 256))
    lane = lax.broadcasted_iota(jnp.int32, (8, 256), 1)
    last = jnp.zeros((8, 256), F32)
    for t, v in enumerate((sums[0:1, :], sums[1:2, :], p_ref[16:17, :], p_ref[17:18, :])):
        rest = jnp.sum(v, axis=1, keepdims=True)
        for u in range(3):
            piece = rest.astype(BF).astype(F32)
            rest = rest - piece
            last = last + jnp.where((row == 6) & (lane == 4 * u + t), piece, 0.0)
    groups = []
    lows = []
    for c in range(3):
        a, b, d, e = [h_ref[32 * c + 8 * t : 32 * c + 8 * t + 8, :] for t in range(4)]
        groups += [a, b + jnp.where(row == 7, pltpu.roll(e, 3, 0), 0.0), d + jnp.where(row > 5, pltpu.roll(e, 4, 0), 0.0)]
        last = last + jnp.where((row == 2 * c) | (row == 2 * c + 1), shifted(e, 2 * c, 0), 0.0)
        low = [v[:, 0:128] - v[:, 0:128].astype(BF).astype(F32) for v in (a, b)]
        lows.append(jnp.concatenate(low, axis=1))
    groups.append(last)
    groups += lows
    for v in (part, p_ref[0:8, :], p_ref[8:16, :]):
        groups.append(jnp.concatenate([v, v - v.astype(BF).astype(F32)], axis=1))
    packed = jnp.concatenate(groups, axis=0).astype(BF)
    for t in range(16):
        out_ref[t] = packed


def shifted(a, by, axis):
    n = a.shape[axis]
    by = by % n
    return a if by == 0 else pltpu.roll(a, by, axis)


def unpack(h_ref):
    out = [([], []) for _ in range(16)]
    for q in range(16):
        for t in range(8):
            both = h_ref[q, 16 * t : 16 * t + 16, :].astype(F32)
            out[2 * t][q % 2].append(both[0:8])
            out[2 * t + 1][q % 2].append(both[8:16])
    return [[jnp.concatenate(v, axis=0) for v in pair] for pair in out]


def stacked(even, odd):
    pad = jnp.zeros((8, even.shape[1]), F32)
    return jnp.concatenate([even, pad], axis=0) + pltpu.roll(jnp.concatenate([odd, pad], axis=0), 4, 0)


def build_operator(groups, a1, a2):
    lane = lax.broadcasted_iota(jnp.int32, (EXT, 128), 1)
    low = lane < 64
    row = rows8((64, 256))
    pad = jnp.zeros((64, 128), F32)

    def piece(c, dj, side):
        a, b, d, last, rest = [groups[g][side] for g in (3 * c, 3 * c + 1, 3 * c + 2, 9, 10 + c)]
        if dj == 0:
            return a + jnp.concatenate([rest[:, 0:128], pad], axis=1)
        if dj == 1:
            return jnp.where(row < 7, b, 0.0) + jnp.concatenate([rest[:, 128:256], pad], axis=1)
        if dj == 2:
            return jnp.where(row < 6, d, 0.0)
        e = jnp.where(row == 4, pltpu.roll(b, 61, 0), jnp.where(row > 1, pltpu.roll(d, 60, 0), shifted(last, -2 * c, 0)))
        return jnp.where(row < 5, e, 0.0)

    for dj in range(4):
        grid = [stacked(piece(c, dj, 0), piece(c, dj, 1)) for c in range(3)]
        for pair in range(2):
            xx, xy, yy = [g[:, 128 * pair : 128 * pair + 128] for g in grid]
            xx_s, xy_s, yy_s = [pltpu.roll(v, 64, 1) for v in (xx, xy, yy)]
            for odd in range(2):
                di = 2 * pair + odd
                if odd == 0:
                    one = jnp.where(low, xx, yy_s)
                    two = jnp.where(low, xy, xy_s)
                else:
                    one = jnp.where(low, xx_s, yy)
                    two = jnp.where(low, xy_s, xy)
                a1[dj * 7 + 3 + di] = one
                a2[dj * 7 + 3 + di] = two
                if di > 0:
                    a1[dj * 7 + 3 - di] = pltpu.roll(one, di, 1)
                    a2[dj * 7 + 3 - di] = pltpu.roll(two, di, 1)


def apply_operator(a1, a2, c):
    cs = pltpu.roll(c, 64, 1)
    plain = [(shifted(c, -di, 1), shifted(cs, -di, 1)) for di in range(-3, 4)]
    y = jnp.zeros((EXT, 128), F32)
    for dj in range(4):
        ahead = jnp.zeros((EXT, 128), F32)
        back = jnp.zeros((EXT, 128), F32)
        for t in range(7):
            p, s = plain[t]
            u, v = a1[dj * 7 + t], a2[dj * 7 + t]
            ahead = ahead + u * shifted(p, -dj, 0) + v * shifted(s, -dj, 0)
            if dj:
                back = back + u * p + v * s
        y = y + ahead
        if dj:
            y = y + pltpu.roll(back, dj, 0)
    return y


def total(a):
    return jnp.sum(jnp.sum(a, axis=0, keepdims=True), axis=1, keepdims=True)


def fields(groups):
    row = lax.broadcasted_iota(jnp.int32, (EXT, 128), 0)
    valid = (row >= 2) & (row < 66)
    grads = []
    for g in (13, 14, 15):
        even, odd = [v[:, 0:128] + v[:, 128:256] for v in groups[g]]
        grads.append(jnp.where(valid, stacked(even, odd), 0.0))
    last = (groups[9][0] + groups[9][1])[:, 0:128]
    lane = lax.broadcasted_iota(jnp.int32, (64, 128), 1)
    here = (rows8((64, 128)) == 6) & (lane < 12)
    sums = [total(jnp.where(here & (lane % 4 == t), last, 0.0)) for t in range(4)]
    return valid, grads, sums


def narrow(a):
    return pltpu.roll(a, EXT - 2, 0)[0:GRID]


def widen(a):
    return pltpu.roll(jnp.concatenate([a, jnp.zeros((EXT - GRID, 128), F32)], axis=0), 2, 0)


def direction(valid, grads, sums, c, hc):
    gf, gm, g1 = grads
    s_fm, s_f, s_m, s_mm = sums
    mean_f = s_f / PIXELS
    if c is None:
        s_w, s_ww, s_fw, gw = s_m, s_mm, s_fm, gm
    else:
        s_w = s_m + total(g1 * c)
        s_ww = s_mm + total(c * (2.0 * gm + hc))
        s_fw = s_fm + total(gf * c)
        gw = gm + hc
    mean_w = s_w / PIXELS
    var = s_ww - PIXELS * mean_w * mean_w
    cross = s_fw - PIXELS * mean_f * mean_w
    den = jnp.sqrt(var + EPS)
    ratio = cross / den / (var + EPS)
    g = PIXELS * ((gf - mean_f * g1) / den - ratio * (gw - mean_w * g1))
    g = jnp.where(valid, g, 0.0)
    return g / jnp.sqrt(total(g * g) / 8192.0 + EPS)


def solve_a(h_ref, out_ref, lead_ref, a1, a2):
    groups = unpack(h_ref)
    build_operator(groups, a1, a2)
    valid, grads, sums = fields(groups)
    c = RATE * direction(valid, grads, sums, None, None)
    d = direction(valid, grads, sums, c, apply_operator(a1, a2, c))
    lead = narrow(c)
    out_ref[0:GRID, :] = lead
    lead_ref[...] = lead
    out_ref[GRID : 2 * GRID, :] = narrow(d)


def solve_b(pos_ref, h_ref, own_ref, prev_ref, next_ref, prev2_ref, next2_ref, out_ref, a1, a2):
    k = pos_ref[0]
    groups = unpack(h_ref)
    build_operator(groups, a1, a2)
    valid, grads, sums = fields(groups)

    def lap(a, b, c):
        return a - 2.0 * b + c

    def pair(ref, there):
        return [jnp.where(there, widen(ref[GRID * t : GRID * t + GRID, :]), 0.0) for t in range(2)]

    has_prev, has_next = k > 0, k < 7
    c1, d1 = pair(own_ref, k >= 0)
    cl, dl = pair(prev_ref, has_prev)
    cr, dr = pair(next_ref, has_next)
    cll = jnp.where(k > 1, widen(prev2_ref[...]), 0.0)
    crr = jnp.where(k < 6, widen(next2_ref[...]), 0.0)
    c2 = c1 + RATE * d1 + SMOOTH * lap(cl, c1, cr)
    c2l = jnp.where(has_prev, cl + RATE * dl + SMOOTH * lap(cll, cl, c1), 0.0)
    c2r = jnp.where(has_next, cr + RATE * dr + SMOOTH * lap(c1, cr, crr), 0.0)
    d2 = direction(valid, grads, sums, c2, apply_operator(a1, a2, c2))
    c3 = c2 + RATE * d2 + SMOOTH * lap(c2l, c2, c2r)
    d3 = direction(valid, grads, sums, c3, apply_operator(a1, a2, c3))
    u = narrow(c3 + RATE * d3)
    c3 = narrow(c3)
    for t in range(8):
        w = SMOOTH * (jnp.where(k == t + 1, 1.0, 0.0) - jnp.where(k == t, 1.0, 0.0) - jnp.where(k == 0, 1.0, 0.0))
        out_ref[t] = jnp.where(k <= t, 1.0, 0.0) * u + w * c3


def finish(pos_ref, m_ref, xs, ys, parts_ref, r8_hbm, turned_ref, out_ref, acc_ref, sx, sy, total_ref, mixed, buf, r8_ref, sems, fetched):
    bring = pltpu.make_async_copy(r8_hbm, r8_ref, fetched)
    bring.start()
    acc = parts_ref[0]
    for t in range(1, 8):
        acc = acc + parts_ref[t]
    acc_ref[...] = acc
    total_ref[...] = widen(acc)
    c8 = total_ref[pl.ds(4 * pos_ref[1], 8), :]
    bring.wait()
    mixed[...] = jnp.dot(r8_ref[...], c8, precision=lax.Precision.HIGHEST, preferred_element_type=F32).astype(BF)

    def copy(step):
        return pltpu.make_async_copy(buf.at[:, tile(step)], out_ref.at[:, tile(step)], sems.at[step])

    def body(step, carry):
        sx[...] = dot(mixed[:, 0:64], turned_ref[:, tile(step)])
        sy[...] = dot(mixed[:, 64:128], turned_ref[:, tile(step)])
        for s in range(BLOCK // 256):
            at = pl.ds(256 * s, 256)
            from_m = pl.ds(pl.multiple_of(BLOCK * step + 256 * s, 256), 256)
            for c in range(ROWS // CHUNK):
                rows = pl.ds(CHUNK * c, CHUNK)
                m = m_ref[rows, from_m].astype(F32)
                buf[rows, from_m] = (m + sx[rows, at] * xs[rows, from_m] + sy[rows, at] * ys[rows, from_m]).astype(BF)
        copy(step).start()
        return carry

    lax.fori_loop(0, STEPS, body, 0)
    for step in range(STEPS):
        copy(step).wait()


def ring(array, axis, by):
    n = lax.axis_size(axis)
    return lax.ppermute(array, axis, [(i, (i + by) % n) for i in range(n)])


FIELD = pltpu.VMEM((ROWS, BLOCK), BF)
WIDE = pltpu.VMEM((ROWS, BLOCK), F32)
SMALL = pltpu.VMEM((8, 128), F32)


def call(kernel, name, args, outs, scratch, limit, hbm_out=False, hbm_in=()):
    vm = pl.BlockSpec(memory_space=pltpu.VMEM)
    specs = [pl.BlockSpec(memory_space=pltpu.SMEM) if a.dtype == jnp.int32 else vm for a in args]
    for i in hbm_in:
        specs[i] = pl.BlockSpec(memory_space=pltpu.HBM)
    return pl.pallas_call(
        kernel,
        in_specs=specs,
        out_specs=[pl.BlockSpec(memory_space=pl.ANY) if hbm_out and i == 0 else vm for i in range(len(outs))],
        out_shape=outs,
        scratch_shapes=scratch,
        name=name,
        compiler_params=pltpu.CompilerParams(vmem_limit_bytes=limit << 20),
    )(*args)


def local(sections, anchor):
    strip = sections[0]
    pos = jnp.stack([lax.axis_index("chain"), lax.axis_index("quad")]).astype(jnp.int32)
    r8, blob, edge = host_tables()
    prior = ring(strip, "chain", 1)
    up = ring(strip[ROWS - 1 : ROWS], "quad", 1)
    dn = ring(strip[0:1], "quad", -1)
    turned = col_table()
    shape = jax.ShapeDtypeStruct
    slope = shape((ROWS, COLS), F32)
    h, p, xs, ys = call(
        stage0,
        "stage0",
        (pos, strip, up, dn, blob, edge),
        [shape((96, 256), F32), shape((24, 128), F32), slope, slope],
        [FIELD] * 7 + [pltpu.VMEM((96 * STEPS, 128), F32), pltpu.VMEM((24 * STEPS, 128), F32), pltpu.VMEM((8, COLS), F32), SMALL],
        24,
    )
    (packed,) = call(
        stage1,
        "stage1",
        (pos, strip, xs, ys, blob, anchor, prior, h, p),
        [shape((16, 128, 256), BF)],
        [FIELD] * 4 + [pltpu.VMEM((ROWS, COLS), BF), pltpu.SemaphoreType.DMA((STEPS,)), pltpu.VMEM((16 * STEPS, 128), F32), SMALL],
        20,
        hbm_in=(5, 6),
    )
    packed, turned = lax.optimization_barrier((packed, turned))
    h_all = lax.all_to_all(packed, "quad", 0, 0, tiled=True)
    operator = [pltpu.VMEM((28, EXT, 128), F32)] * 2
    first, lead = call(solve_a, "solve_a", (h_all,), [shape((2 * GRID, 128), F32), shape((GRID, 128), F32)], operator, 12)
    around = [ring(first, "chain", 1), ring(first, "chain", -1), ring(lead, "chain", 2), ring(lead, "chain", -2)]
    (parts,) = call(solve_b, "solve_b", (pos, h_all, first, *around), [shape((8, GRID, 128), F32)], operator, 12)
    parts = lax.all_to_all(parts, "chain", 0, 0, tiled=True)
    registered, accumulated = call(
        finish,
        "finish",
        (pos, strip, xs, ys, parts, jnp.asarray(r8), turned),
        [shape((ROWS, COLS), BF), shape((GRID, 128), F32)],
        [WIDE] * 2
        + [pltpu.VMEM((EXT, 128), F32), pltpu.VMEM((ROWS, 128), BF), pltpu.VMEM((ROWS, COLS), BF), pltpu.VMEM((ROWS, 8), F32)]
        + [pltpu.SemaphoreType.DMA((STEPS,)), pltpu.SemaphoreType.DMA],
        24,
        hbm_out=True,
        hbm_in=(5,),
    )
    return registered[None], accumulated[None]


def solution(mesh):
    in_specs = (P("chain", "quad", None), P("quad", None))
    out_specs = (P("chain", "quad", None), P("chain", None, None))
    return jax.shard_map(local, mesh=mesh, in_specs=in_specs, out_specs=out_specs, check_vma=False)
```

```python
import jax
import jax.numpy as jnp
import numpy as np
from jax import lax
from jax.experimental import pallas as pl
from jax.experimental.pallas import tpu as pltpu
from jax.sharding import PartitionSpec as P

GRID = 64
SPACING = 64
ROWS = 256
COLS = 4096
BLOCK = 1024
STEPS = COLS // BLOCK
CHUNK = 32
EXT = 72
PIXELS = 4096.0 * 4096.0
EPS = 1e-6
RATE = 0.25
SMOOTH = 0.25
BF = jnp.bfloat16
F32 = jnp.float32


def weight(offset, xp):
    d = xp.abs(offset)
    near = 2.0 / 3.0 - d * d + 0.5 * d * d * d
    r = 2.0 - d
    far = r * r * r / 6.0
    return xp.where(d < 1.0, near, xp.where(d < 2.0, far, 0.0 * d))


def local_rows():
    r = np.arange(ROWS, dtype=np.float32)
    j = np.arange(8, dtype=np.float32) - 2.0
    off = (r[:, None] + np.float32(0.5)) / np.float32(SPACING) - j[None, :] - np.float32(0.5)
    return weight(off.astype(np.float32), np).astype(np.float32)


def hi_lo(a):
    hi = a.astype(BF)
    return hi, (a - hi.astype(F32)).astype(BF)


def split3(a):
    hi = a.astype(BF)
    rest = a - hi.astype(F32)
    mid = rest.astype(BF)
    lo = (rest - mid.astype(F32)).astype(BF)
    return jnp.concatenate([hi.astype(F32), mid.astype(F32), lo.astype(F32)], axis=0).astype(BF)


def sum3(a, n):
    return a[0:n] + a[n : 2 * n] + a[2 * n : 3 * n]


def two(a):
    hi = a.astype(np.dtype(BF)).astype(np.float32)
    return np.concatenate([hi, a - hi], 0)


def host_tables():
    r8 = local_rows()
    pairs = np.zeros((32, ROWS), np.float32)
    c8 = r8.astype(np.dtype(BF)).astype(np.float32)
    lanes = np.zeros((BLOCK, 128), np.float32)
    cols = np.zeros((BLOCK, 128), np.float32)
    place = np.zeros((STEPS * 128, 256), np.float32)
    put = np.zeros((STEPS * 128, 128), np.float32)
    for s in range(4):
        cols[256 * s : 256 * s + 256, 8 * s : 8 * s + 8] = c8
    for d in range(4):
        for e in range(8 - d):
            pairs[d * 8 + e] = r8[:, e] * r8[:, e + d]
            for s in range(4):
                lanes[256 * s : 256 * s + 256, 32 * s + 8 * d + e] = c8[:, e] * c8[:, e + d]
                for t in range(STEPS):
                    i = 16 * t + 4 * s - 2 + e
                    if i >= 0 and i + d < GRID:
                        place[128 * t + 32 * s + 8 * d + e, 64 * d + i] = 1.0
    for t in range(STEPS):
        for s in range(4):
            for e in range(8):
                i = 16 * t + 4 * s - 2 + e
                if 0 <= i < GRID:
                    put[128 * t + 8 * s + e, i] = 1.0
    diff = np.zeros((8, ROWS), np.float32)
    diff[:, 1:] += 0.5 * r8.T[:, :-1]
    diff[:, :-1] -= 0.5 * r8.T[:, 1:]
    lanes_hi = lanes.astype(np.dtype(BF)).astype(np.float32)
    down = 0.5 * (np.eye(ROWS, k=1) - np.eye(ROWS, k=-1))
    across = np.zeros((512, 256), np.float32)
    o = np.arange(256)
    across[o + 129, o] = 0.5
    across[o + 127, o] = -0.5
    plain = np.concatenate([two(r8.T), two(diff), np.ones((16, ROWS), np.float32)], 0)
    wide = np.concatenate([lanes_hi, lanes - lanes_hi], 1)
    halves = np.concatenate([np.concatenate([cols[0:512], cols[512:1024]], 1), np.concatenate([put[0:256], put[256:512]], 1)], 0)
    blob = np.concatenate([down, across, two(pairs), two(r8.T), plain, wide, place, halves], 0)
    edge = np.stack([-0.5 * r8[0], 0.5 * r8[ROWS - 1]], 0).reshape(16, 1) * np.ones((1, 128), np.float32)
    return r8, jnp.asarray(blob.astype(np.dtype(BF))), jnp.asarray(edge.astype(np.float32))


DOWN, ACROSS, PAIRS, LIN, PLAIN, TABLE, PLACE, COLT, PUT, BLOB = 0, 256, 768, 832, 848, 896, 1920, 2432, 2944, 3200


def col_part(blob_ref, lhs):
    return dot(lhs[:, 0:512], blob_ref[COLT : COLT + 512, 0:128]) + dot(lhs[:, 512:1024], blob_ref[COLT : COLT + 512, 128:256])


def put_rows(blob_ref, t):
    return blob_ref[PUT + 128 * (t % 2) : PUT + 128 * (t % 2) + 128, 128 * (t // 2) : 128 * (t // 2) + 128]


def col_table():
    x = jnp.arange(COLS, dtype=jnp.int32).astype(F32)
    j = jnp.arange(GRID, dtype=jnp.int32).astype(F32)
    return weight((x[None, :] + 0.5) / SPACING - j[:, None] - 0.5, jnp).astype(BF)


def dot(a, b):
    return jnp.dot(a, b, preferred_element_type=F32)


def tile(step, size=BLOCK):
    return pl.ds(pl.multiple_of(size * step, size), size)


def slopes(pos_ref, m_ref, up_ref, dn_ref, blob_ref, lhs, xs, ys, step):
    start = BLOCK * step
    left = m_ref[:, pl.ds(pl.multiple_of(jnp.maximum(start - 128, 0), 128), 128)]
    right = m_ref[:, pl.ds(pl.multiple_of(jnp.minimum(start + BLOCK, COLS - 128), 128), 128)]
    left = jnp.where(step > 0, left.astype(F32), 0.0).astype(BF)
    right = jnp.where(step < STEPS - 1, right.astype(F32), 0.0).astype(BF)
    block = m_ref[:, tile(step)]
    ext = jnp.concatenate([left, block, right], axis=1)
    stack = jnp.concatenate([ext[:, 256 * s : 256 * s + 512] for s in range(4)], axis=0)
    x = dot(stack, blob_ref[ACROSS : ACROSS + 512, :])
    for s in range(4):
        xs[:, pl.ds(pl.multiple_of(start + 256 * s, 256), 256)] = x[256 * s : 256 * s + 256]
    up = jnp.where(pos_ref[1] > 0, up_ref[:, tile(step)].astype(F32), 0.0)
    dn = jnp.where(pos_ref[1] < 15, dn_ref[:, tile(step)].astype(F32), 0.0)
    both = dot(jnp.concatenate([blob_ref[DOWN : DOWN + 256, :], lhs], axis=0), block)
    at = tile(step)
    ys[:, at] = both[0:256]
    ys[0:1, at] = ys[0:1, at] - 0.5 * up
    ys[ROWS - 1 : ROWS, at] = ys[ROWS - 1 : ROWS, at] + 0.5 * dn
    return up, dn, both[256:]


def fold8(a):
    return jnp.sum(a.reshape(CHUNK // 8, 8, a.shape[1]), axis=0)


def lanes_to_row(a):
    s = jnp.sum(a, axis=0, keepdims=True)
    out = s[:, 0:128]
    for t in range(1, s.shape[1] // 128):
        out = out + s[:, 128 * t : 128 * t + 128]
    return out


def rows_of(lin, hi, lo):
    a = dot(lin, hi)
    b = dot(lin, lo)
    return a[0:8] + a[8:16] + b[0:8]


def stage0(pos_ref, m_ref, up_ref, dn_ref, blob_ref, edge_ref, anchor_hbm, h_ref, p_ref, xs, ys, anchor_ref, fetched, fxx, fxy, fyy, mxh, mxl, myh, myl, zacc, lacc, l1_ref, sums):
    bring = pltpu.make_async_copy(anchor_hbm, anchor_ref, fetched)
    bring.start()
    sums[...] = jnp.zeros((8, 128), F32)

    def body(step, carry):
        up, dn, ones = slopes(pos_ref, m_ref, up_ref, dn_ref, blob_ref, blob_ref[PLAIN : PLAIN + 48, :], xs, ys, step)
        pairs = blob_ref[PAIRS : PAIRS + 64, :]
        lin = blob_ref[LIN : LIN + 16, :]
        sumsq = jnp.zeros((8, 256), F32)
        t_parts, lx, ly = [], [], []
        for s in range(BLOCK // 256):
            at = pl.ds(256 * s, 256)
            from_m = pl.ds(pl.multiple_of(BLOCK * step + 256 * s, 256), 256)
            for c in range(ROWS // CHUNK):
                rows = pl.ds(CHUNK * c, CHUNK)
                m, x, y = m_ref[rows, from_m].astype(F32), xs[rows, from_m], ys[rows, from_m]
                fxx[rows, at] = (x * x).astype(BF)
                fxy[rows, at] = (x * y).astype(BF)
                fyy[rows, at] = (y * y).astype(BF)
                mxh[rows, at], mxl[rows, at] = hi_lo(m * x)
                myh[rows, at], myl[rows, at] = hi_lo(m * y)
                sumsq = sumsq + fold8(m * m)
            trio = []
            for f in (fxx, fxy, fyy):
                t = dot(pairs, f[:, at])
                trio.append(t[0:32] + t[32:64])
            t_parts.append(jnp.concatenate(trio, axis=0))
            lx.append(rows_of(lin, mxh[:, at], mxl[:, at]))
            ly.append(rows_of(lin, myh[:, at], myl[:, at]))
        t_hi, t_lo = hi_lo(jnp.concatenate(t_parts, axis=1))
        z = dot(jnp.concatenate([t_hi, t_lo], axis=0), blob_ref[TABLE : TABLE + 1024, :])
        z = z[0:96] + z[96:192]
        zacc[tile(step, 96), :] = z[:, 0:128] + z[:, 128:256]
        l1_ref[:, tile(step)] = ones[0:8] + ones[8:16]
        l1y = ones[16:24] + ones[24:32]
        l1y = l1y + edge_ref[0:8, 0:1] * up + edge_ref[8:16, 0:1] * dn
        rows3 = jnp.concatenate([jnp.concatenate(lx, axis=1), jnp.concatenate(ly, axis=1), l1y], axis=0)
        lacc[tile(step, 24), :] = sum3(col_part(blob_ref, split3(rows3)), 24)
        sums[0:1, :] += lanes_to_row(ones[32:33])
        sums[1:2, :] += lanes_to_row(sumsq)
        return carry

    lax.fori_loop(0, STEPS, body, 0)
    bring.wait()
    l1 = l1_ref[...]
    col = lax.broadcasted_iota(jnp.int32, l1.shape, 1)
    after = jnp.where(col < COLS - 1, pltpu.roll(l1, COLS - 1, 1), 0.0)
    before = jnp.where(col > 0, pltpu.roll(l1, 1, 1), 0.0)
    l1x = split3(0.5 * (after - before))
    h = jnp.zeros((288, 256), F32)
    p = jnp.zeros((96, 128), F32)
    for t in range(STEPS):
        h = h + dot(split3(zacc[96 * t : 96 * t + 96, :]), blob_ref[PLACE + 128 * t : PLACE + 128 * t + 128, :])
        one = sum3(col_part(blob_ref, l1x[:, BLOCK * t : BLOCK * t + BLOCK]), 8)
        p = p + dot(split3(jnp.concatenate([lacc[24 * t : 24 * t + 24, :], one], axis=0)), put_rows(blob_ref, t))
    h_ref[...] = sum3(h, 96)
    p = sum3(p, 32)
    p_ref[0:8, :] = p[0:8] + pltpu.roll(p[8:16], 64, 1)
    p_ref[8:16, :] = p[24:32] + pltpu.roll(p[16:24], 64, 1)
    p_ref[16:24, :] = sums[...]


def cross_part(pos_ref, m_ref, xs, ys, blob_ref, anchor_ref, prior_ref, fxh, fxl, fyh, fyl, lacc, sums):
    first = pos_ref[0] == 0
    sums[...] = jnp.zeros((8, 128), F32)

    def body(step, carry):
        lin = blob_ref[LIN : LIN + 16, :]
        cross = jnp.zeros((8, 256), F32)
        whole_sum = jnp.zeros((8, 256), F32)
        lx, ly = [], []
        for s in range(BLOCK // 256):
            at = pl.ds(256 * s, 256)
            from_m = pl.ds(pl.multiple_of(BLOCK * step + 256 * s, 256), 256)
            for c in range(ROWS // CHUNK):
                rows = pl.ds(CHUNK * c, CHUNK)
                m, x, y = m_ref[rows, from_m].astype(F32), xs[rows, from_m], ys[rows, from_m]
                f = jnp.where(first, anchor_ref[rows, from_m].astype(F32), prior_ref[rows, from_m].astype(F32))
                fxh[rows, at], fxl[rows, at] = hi_lo(f * x)
                fyh[rows, at], fyl[rows, at] = hi_lo(f * y)
                cross = cross + fold8(f * m)
                whole_sum = whole_sum + fold8(f)
            lx.append(rows_of(lin, fxh[:, at], fxl[:, at]))
            ly.append(rows_of(lin, fyh[:, at], fyl[:, at]))
        rows2 = jnp.concatenate([jnp.concatenate(lx, axis=1), jnp.concatenate(ly, axis=1)], axis=0)
        lacc[tile(step, 16), :] = sum3(col_part(blob_ref, split3(rows2)), 16)
        sums[0:1, :] += lanes_to_row(cross)
        sums[1:2, :] += lanes_to_row(whole_sum)
        return carry

    lax.fori_loop(0, STEPS, body, 0)
    p = jnp.zeros((48, 128), F32)
    for i in range(STEPS):
        p = p + dot(split3(lacc[16 * i : 16 * i + 16, :]), put_rows(blob_ref, i))
    p = sum3(p, 16)
    return p[0:8] + pltpu.roll(p[8:16], 64, 1)


def rows8(shape):
    return lax.broadcasted_iota(jnp.int32, shape, 0) % 8


def stage1(pos_ref, m_ref, xs, ys, blob_ref, anchor_ref, prior_ref, h_ref, p_ref, out_ref, *scratch):
    sums = scratch[-1]
    part = cross_part(pos_ref, m_ref, xs, ys, blob_ref, anchor_ref, prior_ref, *scratch)
    row = rows8((8, 256))
    lane = lax.broadcasted_iota(jnp.int32, (8, 256), 1)
    last = jnp.zeros((8, 256), F32)
    for t, v in enumerate((sums[0:1, :], sums[1:2, :], p_ref[16:17, :], p_ref[17:18, :])):
        rest = jnp.sum(v, axis=1, keepdims=True)
        for u in range(3):
            piece = rest.astype(BF).astype(F32)
            rest = rest - piece
            last = last + jnp.where((row == 6) & (lane == 4 * u + t), piece, 0.0)
    groups = []
    lows = []
    for c in range(3):
        a, b, d, e = [h_ref[32 * c + 8 * t : 32 * c + 8 * t + 8, :] for t in range(4)]
        groups += [a, b + jnp.where(row == 7, pltpu.roll(e, 3, 0), 0.0), d + jnp.where(row > 5, pltpu.roll(e, 4, 0), 0.0)]
        last = last + jnp.where((row == 2 * c) | (row == 2 * c + 1), shifted(e, 2 * c, 0), 0.0)
        low = [v[:, 0:128] - v[:, 0:128].astype(BF).astype(F32) for v in (a, b)]
        lows.append(jnp.concatenate(low, axis=1))
    groups.append(last)
    groups += lows
    for v in (part, p_ref[0:8, :], p_ref[8:16, :]):
        groups.append(jnp.concatenate([v, v - v.astype(BF).astype(F32)], axis=1))
    packed = jnp.concatenate(groups, axis=0).astype(BF)
    out_ref[...] = packed


def shifted(a, by, axis):
    n = a.shape[axis]
    by = by % n
    return a if by == 0 else pltpu.roll(a, by, axis)


def stacked(even, odd):
    pad = jnp.zeros((8, even.shape[1]), F32)
    return jnp.concatenate([even, pad], axis=0) + pltpu.roll(jnp.concatenate([odd, pad], axis=0), 4, 0)


def merge(pos_ref, near0, near1, near2, near3, out_ref, all_ref):
    y = pos_ref[1] % 4
    for e, ref in enumerate((near0, near1, near2, near3)):
        all_ref[(y + 4 - e) % 4] = ref[...]
    groups = [([], []) for _ in range(16)]
    for q in range(4):
        for t in range(8):
            both = all_ref[q, 16 * t : 16 * t + 16, :].astype(F32)
            groups[2 * t][q % 2].append(both[0:8])
            groups[2 * t + 1][q % 2].append(both[8:16])
    groups = [[jnp.concatenate(v, axis=0) for v in pair] for pair in groups]
    row = rows8((16, 256))
    pad = jnp.zeros((16, 128), F32)

    def piece(c, dj, side):
        a, b, d, last, rest = [groups[g][side] for g in (3 * c, 3 * c + 1, 3 * c + 2, 9, 10 + c)]
        if dj == 0:
            return a + jnp.concatenate([rest[:, 0:128], pad], axis=1)
        if dj == 1:
            return jnp.where(row < 7, b, 0.0) + jnp.concatenate([rest[:, 128:256], pad], axis=1)
        if dj == 2:
            return jnp.where(row < 6, d, 0.0)
        e = jnp.where(row == 4, pltpu.roll(b, 13, 0), jnp.where(row > 1, pltpu.roll(d, 12, 0), shifted(last, -2 * c, 0)))
        return jnp.where(row < 5, e, 0.0)

    items, lows = [], []
    for c in range(3):
        four = [stacked(piece(c, dj, 0), piece(c, dj, 1)) for dj in range(4)]
        items += four
        lows.append(jnp.concatenate([v[:, 0:128] - v[:, 0:128].astype(BF).astype(F32) for v in four[0:2]], axis=1))
    last = groups[9][0] + groups[9][1]
    lane = lax.broadcasted_iota(jnp.int32, (16, 256), 1)
    here = (row == 6) & (lane < 12)
    row24 = lax.broadcasted_iota(jnp.int32, (24, 256), 0)
    lane24 = lax.broadcasted_iota(jnp.int32, (24, 256), 1)
    for t in range(4):
        rest = total(jnp.where(here & (lane % 4 == t), last, 0.0))
        for u in range(3):
            part = rest.astype(BF).astype(F32)
            rest = rest - part
            items[3] = items[3] + jnp.where((row24 == 19) & (lane24 == 4 * u + t), part, 0.0)
    items += lows
    for g in (13, 14, 15):
        even, odd = [v[:, 0:128] + v[:, 128:256] for v in groups[g]]
        v = stacked(even, odd)
        items.append(jnp.concatenate([v, v - v.astype(BF).astype(F32)], axis=1))
    room = jnp.zeros((16, 256), F32)
    pairs = []
    for p in range(9):
        a, b = [jnp.concatenate([v, room], axis=0) for v in items[2 * p : 2 * p + 2]]
        pairs.append(a + pltpu.roll(b, 20, 0))
    out_ref[...] = jnp.concatenate(pairs, axis=0).astype(BF)


def unpack(pos_ref, far, all_ref):
    z = pos_ref[1] // 4
    for d in range(4):
        all_ref[(z + 4 - d) % 4] = far[d][...]
    blocks = [all_ref[t].astype(F32) for t in range(4)]
    row = lax.broadcasted_iota(jnp.int32, (8, 256), 0)
    lane = lax.broadcasted_iota(jnp.int32, (8, 256), 1)
    eight = jnp.zeros((8, 256), F32)
    out = []
    sums = None
    for i in range(18):
        body, tails = [], [eight, eight]
        for t in range(4):
            full = blocks[t][40 * (i // 2) : 40 * (i // 2) + 40]
            if i % 2:
                full = pltpu.roll(full, 20, 0)
            body.append(full[0:16])
            tail = full[16:24]
            if i == 3:
                sums = tail if sums is None else sums + tail
            tails += [jnp.where(row < (3 if i == 3 else 4), tail, 0.0), eight]
        out.append(jnp.concatenate(body + [eight], axis=0) + jnp.concatenate(tails[:-1], axis=0))
    here = (row == 3) & (lane < 12)
    return out, [total(jnp.where(here & (lane % 4 == t), sums, 0.0)) for t in range(4)]


def build_operator(items, a1, a2):
    lane = lax.broadcasted_iota(jnp.int32, (EXT, 128), 1)
    low = lane < 64
    for dj in range(4):
        for pair in range(2):
            three = []
            for c in range(3):
                v = items[4 * c + dj][:, 128 * pair : 128 * pair + 128]
                if pair == 0 and dj < 2:
                    v = v + items[12 + c][:, 128 * dj : 128 * dj + 128]
                three.append(v)
            xx, xy, yy = three
            xx_s, xy_s, yy_s = [pltpu.roll(v, 64, 1) for v in (xx, xy, yy)]
            for odd in range(2):
                di = 2 * pair + odd
                if odd == 0:
                    one = jnp.where(low, xx, yy_s)
                    two = jnp.where(low, xy, xy_s)
                else:
                    one = jnp.where(low, xx_s, yy)
                    two = jnp.where(low, xy_s, xy)
                a1[dj * 7 + 3 + di] = one
                a2[dj * 7 + 3 + di] = two
                if di > 0:
                    a1[dj * 7 + 3 - di] = pltpu.roll(one, di, 1)
                    a2[dj * 7 + 3 - di] = pltpu.roll(two, di, 1)


def apply_operator(a1, a2, c):
    cs = pltpu.roll(c, 64, 1)
    plain = [(shifted(c, -di, 1), shifted(cs, -di, 1)) for di in range(-3, 4)]
    y = jnp.zeros((EXT, 128), F32)
    for dj in range(4):
        ahead = jnp.zeros((EXT, 128), F32)
        back = jnp.zeros((EXT, 128), F32)
        for t in range(7):
            p, s = plain[t]
            u, v = a1[dj * 7 + t], a2[dj * 7 + t]
            ahead = ahead + u * shifted(p, -dj, 0) + v * shifted(s, -dj, 0)
            if dj:
                back = back + u * p + v * s
        y = y + ahead
        if dj:
            y = y + pltpu.roll(back, dj, 0)
    return y


def total(a):
    return jnp.sum(jnp.sum(a, axis=0, keepdims=True), axis=1, keepdims=True)


def fields(items):
    row = lax.broadcasted_iota(jnp.int32, (EXT, 128), 0)
    valid = (row >= 2) & (row < 66)
    return valid, [jnp.where(valid, v[:, 0:128] + v[:, 128:256], 0.0) for v in items[15:18]]


def narrow(a):
    return pltpu.roll(a, EXT - 2, 0)[0:GRID]


def widen(a):
    return pltpu.roll(jnp.concatenate([a, jnp.zeros((EXT - GRID, 128), F32)], axis=0), 2, 0)


def direction(valid, grads, sums, c, hc):
    gf, gm, g1 = grads
    s_fm, s_f, s_m, s_mm = sums
    mean_f = s_f / PIXELS
    if c is None:
        s_w, s_ww, s_fw, gw = s_m, s_mm, s_fm, gm
    else:
        s_w = s_m + total(g1 * c)
        s_ww = s_mm + total(c * (2.0 * gm + hc))
        s_fw = s_fm + total(gf * c)
        gw = gm + hc
    mean_w = s_w / PIXELS
    var = s_ww - PIXELS * mean_w * mean_w
    cross = s_fw - PIXELS * mean_f * mean_w
    den = jnp.sqrt(var + EPS)
    ratio = cross / den / (var + EPS)
    g = PIXELS * ((gf - mean_f * g1) / den - ratio * (gw - mean_w * g1))
    g = jnp.where(valid, g, 0.0)
    return g / jnp.sqrt(total(g * g) / 8192.0 + EPS)


def solve_a(pos_ref, far0, far1, far2, far3, out_ref, lead_ref, a1, a2, all_ref):
    items, sums = unpack(pos_ref, (far0, far1, far2, far3), all_ref)
    build_operator(items, a1, a2)
    valid, grads = fields(items)
    c = RATE * direction(valid, grads, sums, None, None)
    d = direction(valid, grads, sums, c, apply_operator(a1, a2, c))
    lead = narrow(c)
    out_ref[0:GRID, :] = lead
    lead_ref[...] = lead
    out_ref[GRID : 2 * GRID, :] = narrow(d)


def solve_b(pos_ref, far0, far1, far2, far3, own_ref, prev_ref, next_ref, prev2_ref, next2_ref, out_ref, a1, a2, all_ref):
    k = pos_ref[0]
    items, sums = unpack(pos_ref, (far0, far1, far2, far3), all_ref)
    build_operator(items, a1, a2)
    valid, grads = fields(items)

    def lap(a, b, c):
        return a - 2.0 * b + c

    def pair(ref, there):
        return [jnp.where(there, widen(ref[GRID * t : GRID * t + GRID, :]), 0.0) for t in range(2)]

    has_prev, has_next = k > 0, k < 7
    c1, d1 = pair(own_ref, k >= 0)
    cl, dl = pair(prev_ref, has_prev)
    cr, dr = pair(next_ref, has_next)
    cll = jnp.where(k > 1, widen(prev2_ref[...]), 0.0)
    crr = jnp.where(k < 6, widen(next2_ref[...]), 0.0)
    c2 = c1 + RATE * d1 + SMOOTH * lap(cl, c1, cr)
    c2l = jnp.where(has_prev, cl + RATE * dl + SMOOTH * lap(cll, cl, c1), 0.0)
    c2r = jnp.where(has_next, cr + RATE * dr + SMOOTH * lap(c1, cr, crr), 0.0)
    d2 = direction(valid, grads, sums, c2, apply_operator(a1, a2, c2))
    c3 = c2 + RATE * d2 + SMOOTH * lap(c2l, c2, c2r)
    d3 = direction(valid, grads, sums, c3, apply_operator(a1, a2, c3))
    u = narrow(c3 + RATE * d3)
    c3 = narrow(c3)
    for t in range(8):
        w = SMOOTH * (jnp.where(k == t + 1, 1.0, 0.0) - jnp.where(k == t, 1.0, 0.0) - jnp.where(k == 0, 1.0, 0.0))
        out_ref[t] = jnp.where(k <= t, 1.0, 0.0) * u + w * c3


def finish(pos_ref, m_ref, xs, ys, parts_ref, r8_hbm, turned_ref, out_ref, acc_ref, sx, sy, total_ref, mixed, buf, r8_ref, sems, fetched):
    bring = pltpu.make_async_copy(r8_hbm, r8_ref, fetched)
    bring.start()
    acc = parts_ref[0]
    for t in range(1, 8):
        acc = acc + parts_ref[t]
    acc_ref[...] = acc
    total_ref[...] = widen(acc)
    c8 = total_ref[pl.ds(4 * pos_ref[1], 8), :]
    bring.wait()
    mixed[...] = jnp.dot(r8_ref[...], c8, precision=lax.Precision.HIGHEST, preferred_element_type=F32).astype(BF)

    def copy(step):
        return pltpu.make_async_copy(buf.at[:, tile(step)], out_ref.at[:, tile(step)], sems.at[step])

    def body(step, carry):
        sx[...] = dot(mixed[:, 0:64], turned_ref[:, tile(step)])
        sy[...] = dot(mixed[:, 64:128], turned_ref[:, tile(step)])
        for s in range(BLOCK // 256):
            at = pl.ds(256 * s, 256)
            from_m = pl.ds(pl.multiple_of(BLOCK * step + 256 * s, 256), 256)
            for c in range(ROWS // CHUNK):
                rows = pl.ds(CHUNK * c, CHUNK)
                m = m_ref[rows, from_m].astype(F32)
                buf[rows, from_m] = (m + sx[rows, at] * xs[rows, from_m] + sy[rows, at] * ys[rows, from_m]).astype(BF)
        copy(step).start()
        return carry

    lax.fori_loop(0, STEPS, body, 0)
    for step in range(STEPS):
        copy(step).wait()


def around_four(array, stride, by):
    def to(q):
        here = q // stride % 4
        return q + stride * ((here + by) % 4 - here)

    return lax.ppermute(array, "quad", [(q, to(q)) for q in range(16)])


def ring(array, axis, by):
    n = lax.axis_size(axis)
    return lax.ppermute(array, axis, [(i, (i + by) % n) for i in range(n)])


FIELD = pltpu.VMEM((ROWS, BLOCK), BF)
WIDE = pltpu.VMEM((ROWS, BLOCK), F32)
SMALL = pltpu.VMEM((8, 128), F32)


def call(kernel, name, args, outs, scratch, limit, hbm_out=False, hbm_in=()):
    vm = pl.BlockSpec(memory_space=pltpu.VMEM)
    specs = [pl.BlockSpec(memory_space=pltpu.SMEM) if a.dtype == jnp.int32 else vm for a in args]
    for i in hbm_in:
        specs[i] = pl.BlockSpec(memory_space=pltpu.HBM)
    return pl.pallas_call(
        kernel,
        in_specs=specs,
        out_specs=[pl.BlockSpec(memory_space=pl.ANY) if hbm_out and i == 0 else vm for i in range(len(outs))],
        out_shape=outs,
        scratch_shapes=scratch,
        name=name,
        compiler_params=pltpu.CompilerParams(vmem_limit_bytes=limit << 20),
    )(*args)


def local(sections, anchor):
    strip = sections[0]
    pos = jnp.stack([lax.axis_index("chain"), lax.axis_index("quad")]).astype(jnp.int32)
    r8, blob, edge = host_tables()
    prior = ring(strip, "chain", 1)
    up = ring(strip[ROWS - 1 : ROWS], "quad", 1)
    dn = ring(strip[0:1], "quad", -1)
    turned = col_table()
    shape = jax.ShapeDtypeStruct
    slope = shape((ROWS, COLS), F32)
    h, p, xs, ys, before = call(
        stage0,
        "stage0",
        (pos, strip, up, dn, blob, edge, anchor),
        [shape((96, 256), F32), shape((24, 128), F32), slope, slope, shape((ROWS, COLS), BF)],
        [pltpu.SemaphoreType.DMA] + [FIELD] * 7 + [pltpu.VMEM((96 * STEPS, 128), F32), pltpu.VMEM((24 * STEPS, 128), F32), pltpu.VMEM((8, COLS), F32), SMALL],
        24,
        hbm_in=(6,),
    )
    (packed,) = call(
        stage1,
        "stage1",
        (pos, strip, xs, ys, blob, before, prior, h, p),
        [shape((128, 256), BF)],
        [FIELD] * 4 + [pltpu.VMEM((16 * STEPS, 128), F32), SMALL],
        20,
    )
    packed, turned = lax.optimization_barrier((packed, turned))
    four = [packed] + [around_four(packed, 1, d) for d in (1, 2, 3)]
    (near,) = call(merge, "merge", (pos, *four), [shape((360, 256), BF)], [pltpu.VMEM((4, 128, 256), BF)], 12)
    far = [near] + [around_four(near, 4, d) for d in (1, 2, 3)]
    operator = [pltpu.VMEM((28, EXT, 128), F32)] * 2 + [pltpu.VMEM((4, 360, 256), BF)]
    first, lead = call(solve_a, "solve_a", (pos, *far), [shape((2 * GRID, 128), F32), shape((GRID, 128), F32)], operator, 12)
    around = [ring(first, "chain", 1), ring(first, "chain", -1), ring(lead, "chain", 2), ring(lead, "chain", -2)]
    (parts,) = call(solve_b, "solve_b", (pos, *far, first, *around), [shape((8, GRID, 128), F32)], operator, 12)
    parts = lax.all_to_all(parts, "chain", 0, 0, tiled=True)
    registered, accumulated = call(
        finish,
        "finish",
        (pos, strip, xs, ys, parts, jnp.asarray(r8), turned),
        [shape((ROWS, COLS), BF), shape((GRID, 128), F32)],
        [WIDE] * 2
        + [pltpu.VMEM((EXT, 128), F32), pltpu.VMEM((ROWS, 128), BF), pltpu.VMEM((ROWS, COLS), BF), pltpu.VMEM((ROWS, 8), F32)]
        + [pltpu.SemaphoreType.DMA((STEPS,)), pltpu.SemaphoreType.DMA],
        24,
        hbm_out=True,
        hbm_in=(5,),
    )
    return registered[None], accumulated[None]


def solution(mesh):
    in_specs = (P("chain", "quad", None), P("quad", None))
    out_specs = (P("chain", "quad", None), P("chain", None, None))
    return jax.shard_map(local, mesh=mesh, in_specs=in_specs, out_specs=out_specs, check_vma=False)
```

```python
import jax
import jax.numpy as jnp
import numpy as np
from jax import lax
from jax.experimental import pallas as pl
from jax.experimental.pallas import tpu as pltpu
from jax.sharding import PartitionSpec as P

GRID = 64
SPACING = 64
ROWS = 256
COLS = 4096
BLOCK = 1024
STEPS = COLS // BLOCK
CHUNK = 32
EXT = 72
PIXELS = 4096.0 * 4096.0
EPS = 1e-6
RATE = 0.25
SMOOTH = 0.25
BF = jnp.bfloat16
F32 = jnp.float32


def weight(offset, xp):
    d = xp.abs(offset)
    near = 2.0 / 3.0 - d * d + 0.5 * d * d * d
    r = 2.0 - d
    far = r * r * r / 6.0
    return xp.where(d < 1.0, near, xp.where(d < 2.0, far, 0.0 * d))


def local_rows():
    r = np.arange(ROWS, dtype=np.float32)
    j = np.arange(8, dtype=np.float32) - 2.0
    off = (r[:, None] + np.float32(0.5)) / np.float32(SPACING) - j[None, :] - np.float32(0.5)
    return weight(off.astype(np.float32), np).astype(np.float32)


def hi_lo(a):
    hi = a.astype(BF)
    return hi, (a - hi.astype(F32)).astype(BF)


def split3(a):
    hi = a.astype(BF)
    rest = a - hi.astype(F32)
    mid = rest.astype(BF)
    lo = (rest - mid.astype(F32)).astype(BF)
    return jnp.concatenate([hi.astype(F32), mid.astype(F32), lo.astype(F32)], axis=0).astype(BF)


def sum3(a, n):
    return a[0:n] + a[n : 2 * n] + a[2 * n : 3 * n]


def two(a):
    hi = a.astype(np.dtype(BF)).astype(np.float32)
    return np.concatenate([hi, a - hi], 0)


def host_tables():
    r8 = local_rows()
    pairs = np.zeros((32, ROWS), np.float32)
    c8 = r8.astype(np.dtype(BF)).astype(np.float32)
    lanes = np.zeros((BLOCK, 128), np.float32)
    cols = np.zeros((BLOCK, 128), np.float32)
    place = np.zeros((STEPS * 128, 256), np.float32)
    put = np.zeros((STEPS * 128, 128), np.float32)
    for s in range(4):
        cols[256 * s : 256 * s + 256, 8 * s : 8 * s + 8] = c8
    for d in range(4):
        for e in range(8 - d):
            pairs[d * 8 + e] = r8[:, e] * r8[:, e + d]
            for s in range(4):
                lanes[256 * s : 256 * s + 256, 32 * s + 8 * d + e] = c8[:, e] * c8[:, e + d]
                for t in range(STEPS):
                    i = 16 * t + 4 * s - 2 + e
                    if i >= 0 and i + d < GRID:
                        place[128 * t + 32 * s + 8 * d + e, 64 * d + i] = 1.0
    for t in range(STEPS):
        for s in range(4):
            for e in range(8):
                i = 16 * t + 4 * s - 2 + e
                if 0 <= i < GRID:
                    put[128 * t + 8 * s + e, i] = 1.0
    diff = np.zeros((8, ROWS), np.float32)
    diff[:, 1:] += 0.5 * r8.T[:, :-1]
    diff[:, :-1] -= 0.5 * r8.T[:, 1:]
    lanes_hi = lanes.astype(np.dtype(BF)).astype(np.float32)
    down = 0.5 * (np.eye(ROWS, k=1) - np.eye(ROWS, k=-1))
    across = np.zeros((512, 256), np.float32)
    o = np.arange(256)
    across[o + 129, o] = 0.5
    across[o + 127, o] = -0.5
    plain = np.concatenate([two(r8.T), two(diff), np.ones((16, ROWS), np.float32)], 0)
    wide = np.concatenate([lanes_hi, lanes - lanes_hi], 1)
    halves = np.concatenate([np.concatenate([cols[0:512], cols[512:1024]], 1), np.concatenate([put[0:256], put[256:512]], 1)], 0)
    blob = np.concatenate([down, across, two(pairs), two(r8.T), plain, wide, place, halves], 0)
    edge = np.stack([-0.5 * r8[0], 0.5 * r8[ROWS - 1]], 0).reshape(16, 1) * np.ones((1, 128), np.float32)
    return r8, jnp.asarray(blob.astype(np.dtype(BF))), jnp.asarray(edge.astype(np.float32))


DOWN, ACROSS, PAIRS, LIN, PLAIN, TABLE, PLACE, COLT, PUT, BLOB = 0, 256, 768, 832, 848, 896, 1920, 2432, 2944, 3200


def col_part(blob_ref, lhs):
    return dot(lhs[:, 0:512], blob_ref[COLT : COLT + 512, 0:128]) + dot(lhs[:, 512:1024], blob_ref[COLT : COLT + 512, 128:256])


def put_rows(blob_ref, t):
    return blob_ref[PUT + 128 * (t % 2) : PUT + 128 * (t % 2) + 128, 128 * (t // 2) : 128 * (t // 2) + 128]


def col_table():
    x = jnp.arange(COLS, dtype=jnp.int32).astype(F32)
    j = jnp.arange(GRID, dtype=jnp.int32).astype(F32)
    return weight((x[None, :] + 0.5) / SPACING - j[:, None] - 0.5, jnp).astype(BF)


def dot(a, b):
    return jnp.dot(a, b, preferred_element_type=F32)


def tile(step, size=BLOCK):
    return pl.ds(pl.multiple_of(size * step, size), size)


def slopes(pos_ref, m_ref, up_ref, dn_ref, blob_ref, lhs, xs, ys, step):
    start = BLOCK * step
    left = m_ref[:, pl.ds(pl.multiple_of(jnp.maximum(start - 128, 0), 128), 128)]
    right = m_ref[:, pl.ds(pl.multiple_of(jnp.minimum(start + BLOCK, COLS - 128), 128), 128)]
    left = jnp.where(step > 0, left.astype(F32), 0.0).astype(BF)
    right = jnp.where(step < STEPS - 1, right.astype(F32), 0.0).astype(BF)
    block = m_ref[:, tile(step)]
    ext = jnp.concatenate([left, block, right], axis=1)
    stack = jnp.concatenate([ext[:, 256 * s : 256 * s + 512] for s in range(4)], axis=0)
    x = dot(stack, blob_ref[ACROSS : ACROSS + 512, :])
    for s in range(4):
        xs[:, pl.ds(pl.multiple_of(start + 256 * s, 256), 256)] = x[256 * s : 256 * s + 256]
    up = jnp.where(pos_ref[1] > 0, up_ref[:, tile(step)].astype(F32), 0.0)
    dn = jnp.where(pos_ref[1] < 15, dn_ref[:, tile(step)].astype(F32), 0.0)
    both = dot(jnp.concatenate([blob_ref[DOWN : DOWN + 256, :], lhs], axis=0), block)
    at = tile(step)
    ys[:, at] = both[0:256]
    ys[0:1, at] = ys[0:1, at] - 0.5 * up
    ys[ROWS - 1 : ROWS, at] = ys[ROWS - 1 : ROWS, at] + 0.5 * dn
    return up, dn, both[256:]


def fold8(a):
    return jnp.sum(a.reshape(CHUNK // 8, 8, a.shape[1]), axis=0)


def lanes_to_row(a):
    s = jnp.sum(a, axis=0, keepdims=True)
    out = s[:, 0:128]
    for t in range(1, s.shape[1] // 128):
        out = out + s[:, 128 * t : 128 * t + 128]
    return out


def rows_of(lin, hi, lo):
    a = dot(lin, hi)
    b = dot(lin, lo)
    return a[0:8] + a[8:16] + b[0:8]


def stage0(pos_ref, m_ref, up_ref, dn_ref, blob_ref, edge_ref, anchor_hbm, h_ref, p_ref, xs, ys, anchor_ref, fetched, fxx, fxy, fyy, mxh, mxl, myh, myl, zacc, lacc, l1_ref, sums):
    bring = pltpu.make_async_copy(anchor_hbm, anchor_ref, fetched)
    bring.start()
    sums[...] = jnp.zeros((8, 128), F32)

    def body(step, carry):
        up, dn, ones = slopes(pos_ref, m_ref, up_ref, dn_ref, blob_ref, blob_ref[PLAIN : PLAIN + 48, :], xs, ys, step)
        pairs = blob_ref[PAIRS : PAIRS + 64, :]
        lin = blob_ref[LIN : LIN + 16, :]
        sumsq = jnp.zeros((8, 256), F32)
        t_parts, lx, ly = [], [], []
        for s in range(BLOCK // 256):
            at = pl.ds(256 * s, 256)
            from_m = pl.ds(pl.multiple_of(BLOCK * step + 256 * s, 256), 256)
            for c in range(ROWS // CHUNK):
                rows = pl.ds(CHUNK * c, CHUNK)
                m, x, y = m_ref[rows, from_m].astype(F32), xs[rows, from_m], ys[rows, from_m]
                fxx[rows, at] = (x * x).astype(BF)
                fxy[rows, at] = (x * y).astype(BF)
                fyy[rows, at] = (y * y).astype(BF)
                mxh[rows, at], mxl[rows, at] = hi_lo(m * x)
                myh[rows, at], myl[rows, at] = hi_lo(m * y)
                sumsq = sumsq + fold8(m * m)
            trio = []
            for f in (fxx, fxy, fyy):
                t = dot(pairs, f[:, at])
                trio.append(t[0:32] + t[32:64])
            t_parts.append(jnp.concatenate(trio, axis=0))
            lx.append(rows_of(lin, mxh[:, at], mxl[:, at]))
            ly.append(rows_of(lin, myh[:, at], myl[:, at]))
        t_hi, t_lo = hi_lo(jnp.concatenate(t_parts, axis=1))
        z = dot(jnp.concatenate([t_hi, t_lo], axis=0), blob_ref[TABLE : TABLE + 1024, :])
        z = z[0:96] + z[96:192]
        zacc[tile(step, 96), :] = z[:, 0:128] + z[:, 128:256]
        l1_ref[:, tile(step)] = ones[0:8] + ones[8:16]
        l1y = ones[16:24] + ones[24:32]
        l1y = l1y + edge_ref[0:8, 0:1] * up + edge_ref[8:16, 0:1] * dn
        rows3 = jnp.concatenate([jnp.concatenate(lx, axis=1), jnp.concatenate(ly, axis=1), l1y], axis=0)
        lacc[tile(step, 24), :] = sum3(col_part(blob_ref, split3(rows3)), 24)
        sums[0:1, :] += lanes_to_row(ones[32:33])
        sums[1:2, :] += lanes_to_row(sumsq)
        return carry

    lax.fori_loop(0, STEPS, body, 0)
    bring.wait()
    l1 = l1_ref[...]
    col = lax.broadcasted_iota(jnp.int32, l1.shape, 1)
    after = jnp.where(col < COLS - 1, pltpu.roll(l1, COLS - 1, 1), 0.0)
    before = jnp.where(col > 0, pltpu.roll(l1, 1, 1), 0.0)
    l1x = split3(0.5 * (after - before))
    h = jnp.zeros((288, 256), F32)
    p = jnp.zeros((96, 128), F32)
    for t in range(STEPS):
        h = h + dot(split3(zacc[96 * t : 96 * t + 96, :]), blob_ref[PLACE + 128 * t : PLACE + 128 * t + 128, :])
        one = sum3(col_part(blob_ref, l1x[:, BLOCK * t : BLOCK * t + BLOCK]), 8)
        p = p + dot(split3(jnp.concatenate([lacc[24 * t : 24 * t + 24, :], one], axis=0)), put_rows(blob_ref, t))
    h_ref[...] = sum3(h, 96)
    p = sum3(p, 32)
    p_ref[0:8, :] = p[0:8] + pltpu.roll(p[8:16], 64, 1)
    p_ref[8:16, :] = p[24:32] + pltpu.roll(p[16:24], 64, 1)
    p_ref[16:24, :] = sums[...]


def cross_part(pos_ref, m_ref, xs, ys, blob_ref, anchor_ref, prior_ref, fxh, fxl, fyh, fyl, lacc, sums):
    sums[...] = jnp.zeros((8, 128), F32)

    def body(f_ref, step, carry):
        lin = blob_ref[LIN : LIN + 16, :]
        cross = jnp.zeros((8, 256), F32)
        whole_sum = jnp.zeros((8, 256), F32)
        lx, ly = [], []
        for s in range(BLOCK // 256):
            at = pl.ds(256 * s, 256)
            from_m = pl.ds(pl.multiple_of(BLOCK * step + 256 * s, 256), 256)
            for c in range(ROWS // CHUNK):
                rows = pl.ds(CHUNK * c, CHUNK)
                m, x, y = m_ref[rows, from_m].astype(F32), xs[rows, from_m], ys[rows, from_m]
                f = f_ref[rows, from_m].astype(F32)
                fxh[rows, at], fxl[rows, at] = hi_lo(f * x)
                fyh[rows, at], fyl[rows, at] = hi_lo(f * y)
                cross = cross + fold8(f * m)
                whole_sum = whole_sum + fold8(f)
            lx.append(rows_of(lin, fxh[:, at], fxl[:, at]))
            ly.append(rows_of(lin, fyh[:, at], fyl[:, at]))
        rows2 = jnp.concatenate([jnp.concatenate(lx, axis=1), jnp.concatenate(ly, axis=1)], axis=0)
        lacc[tile(step, 16), :] = sum3(col_part(blob_ref, split3(rows2)), 16)
        sums[0:1, :] += lanes_to_row(cross)
        sums[1:2, :] += lanes_to_row(whole_sum)
        return carry

    @pl.when(pos_ref[0] == 0)
    def _():
        lax.fori_loop(0, STEPS, lambda i, c: body(anchor_ref, i, c), 0)

    @pl.when(pos_ref[0] > 0)
    def _():
        lax.fori_loop(0, STEPS, lambda i, c: body(prior_ref, i, c), 0)

    p = jnp.zeros((48, 128), F32)
    for i in range(STEPS):
        p = p + dot(split3(lacc[16 * i : 16 * i + 16, :]), put_rows(blob_ref, i))
    p = sum3(p, 16)
    return p[0:8] + pltpu.roll(p[8:16], 64, 1)


def rows8(shape):
    return lax.broadcasted_iota(jnp.int32, shape, 0) % 8


def stage1(pos_ref, m_ref, xs, ys, blob_ref, anchor_ref, prior_ref, h_ref, p_ref, out_ref, *scratch):
    sums = scratch[-1]
    part = cross_part(pos_ref, m_ref, xs, ys, blob_ref, anchor_ref, prior_ref, *scratch)
    row = rows8((8, 256))
    lane = lax.broadcasted_iota(jnp.int32, (8, 256), 1)
    last = jnp.zeros((8, 256), F32)
    for t, v in enumerate((sums[0:1, :], sums[1:2, :], p_ref[16:17, :], p_ref[17:18, :])):
        rest = jnp.sum(v, axis=1, keepdims=True)
        for u in range(3):
            piece = rest.astype(BF).astype(F32)
            rest = rest - piece
            last = last + jnp.where((row == 6) & (lane == 4 * u + t), piece, 0.0)
    groups = []
    lows = []
    for c in range(3):
        a, b, d, e = [h_ref[32 * c + 8 * t : 32 * c + 8 * t + 8, :] for t in range(4)]
        groups += [a, b + jnp.where(row == 7, pltpu.roll(e, 3, 0), 0.0), d + jnp.where(row > 5, pltpu.roll(e, 4, 0), 0.0)]
        last = last + jnp.where((row == 2 * c) | (row == 2 * c + 1), shifted(e, 2 * c, 0), 0.0)
        low = [v[:, 0:128] - v[:, 0:128].astype(BF).astype(F32) for v in (a, b)]
        lows.append(jnp.concatenate(low, axis=1))
    groups.append(last)
    groups += lows
    for v in (part, p_ref[0:8, :], p_ref[8:16, :]):
        groups.append(jnp.concatenate([v, v - v.astype(BF).astype(F32)], axis=1))
    packed = jnp.concatenate(groups, axis=0).astype(BF)
    out_ref[...] = packed


def shifted(a, by, axis):
    n = a.shape[axis]
    by = by % n
    return a if by == 0 else pltpu.roll(a, by, axis)


def stacked(even, odd):
    pad = jnp.zeros((8, even.shape[1]), F32)
    return jnp.concatenate([even, pad], axis=0) + pltpu.roll(jnp.concatenate([odd, pad], axis=0), 4, 0)


def merge(pos_ref, near0, near1, near2, near3, out_ref, all_ref):
    y = pos_ref[1] % 4
    for e, ref in enumerate((near0, near1, near2, near3)):
        all_ref[(y + 4 - e) % 4] = ref[...]
    groups = [([], []) for _ in range(16)]
    for q in range(4):
        for t in range(8):
            both = all_ref[q, 16 * t : 16 * t + 16, :].astype(F32)
            groups[2 * t][q % 2].append(both[0:8])
            groups[2 * t + 1][q % 2].append(both[8:16])
    groups = [[jnp.concatenate(v, axis=0) for v in pair] for pair in groups]
    row = rows8((16, 256))
    pad = jnp.zeros((16, 128), F32)

    def piece(c, dj, side):
        a, b, d, last, rest = [groups[g][side] for g in (3 * c, 3 * c + 1, 3 * c + 2, 9, 10 + c)]
        if dj == 0:
            return a + jnp.concatenate([rest[:, 0:128], pad], axis=1)
        if dj == 1:
            return jnp.where(row < 7, b, 0.0) + jnp.concatenate([rest[:, 128:256], pad], axis=1)
        if dj == 2:
            return jnp.where(row < 6, d, 0.0)
        e = jnp.where(row == 4, pltpu.roll(b, 13, 0), jnp.where(row > 1, pltpu.roll(d, 12, 0), shifted(last, -2 * c, 0)))
        return jnp.where(row < 5, e, 0.0)

    items, lows = [], []
    for c in range(3):
        four = [stacked(piece(c, dj, 0), piece(c, dj, 1)) for dj in range(4)]
        items += four
        lows.append(jnp.concatenate([v[:, 0:128] - v[:, 0:128].astype(BF).astype(F32) for v in four[0:2]], axis=1))
    last = groups[9][0] + groups[9][1]
    lane = lax.broadcasted_iota(jnp.int32, (16, 256), 1)
    here = (row == 6) & (lane < 12)
    row24 = lax.broadcasted_iota(jnp.int32, (24, 256), 0)
    lane24 = lax.broadcasted_iota(jnp.int32, (24, 256), 1)
    for t in range(4):
        rest = total(jnp.where(here & (lane % 4 == t), last, 0.0))
        for u in range(3):
            part = rest.astype(BF).astype(F32)
            rest = rest - part
            items[3] = items[3] + jnp.where((row24 == 19) & (lane24 == 4 * u + t), part, 0.0)
    items += lows
    for g in (13, 14, 15):
        even, odd = [v[:, 0:128] + v[:, 128:256] for v in groups[g]]
        v = stacked(even, odd)
        items.append(jnp.concatenate([v, v - v.astype(BF).astype(F32)], axis=1))
    room = jnp.zeros((16, 256), F32)
    pairs = []
    for p in range(9):
        a, b = [jnp.concatenate([v, room], axis=0) for v in items[2 * p : 2 * p + 2]]
        pairs.append(a + pltpu.roll(b, 20, 0))
    out_ref[...] = jnp.concatenate(pairs, axis=0).astype(BF)


def unpack(pos_ref, far, all_ref):
    z = pos_ref[1] // 4
    for d in range(4):
        all_ref[(z + 4 - d) % 4] = far[d][...]
    blocks = [all_ref[t].astype(F32) for t in range(4)]
    row = lax.broadcasted_iota(jnp.int32, (8, 256), 0)
    lane = lax.broadcasted_iota(jnp.int32, (8, 256), 1)
    eight = jnp.zeros((8, 256), F32)
    out = []
    sums = None
    for i in range(18):
        body, tails = [], [eight, eight]
        for t in range(4):
            full = blocks[t][40 * (i // 2) : 40 * (i // 2) + 40]
            if i % 2:
                full = pltpu.roll(full, 20, 0)
            body.append(full[0:16])
            tail = full[16:24]
            if i == 3:
                sums = tail if sums is None else sums + tail
            tails += [jnp.where(row < (3 if i == 3 else 4), tail, 0.0), eight]
        out.append(jnp.concatenate(body + [eight], axis=0) + jnp.concatenate(tails[:-1], axis=0))
    here = (row == 3) & (lane < 12)
    return out, [total(jnp.where(here & (lane % 4 == t), sums, 0.0)) for t in range(4)]


def build_operator(items, a1, a2):
    lane = lax.broadcasted_iota(jnp.int32, (EXT, 128), 1)
    low = lane < 64
    for dj in range(4):
        for pair in range(2):
            three = []
            for c in range(3):
                v = items[4 * c + dj][:, 128 * pair : 128 * pair + 128]
                if pair == 0 and dj < 2:
                    v = v + items[12 + c][:, 128 * dj : 128 * dj + 128]
                three.append(v)
            xx, xy, yy = three
            xx_s, xy_s, yy_s = [pltpu.roll(v, 64, 1) for v in (xx, xy, yy)]
            for odd in range(2):
                di = 2 * pair + odd
                if odd == 0:
                    one = jnp.where(low, xx, yy_s)
                    two = jnp.where(low, xy, xy_s)
                else:
                    one = jnp.where(low, xx_s, yy)
                    two = jnp.where(low, xy_s, xy)
                a1[dj * 7 + 3 + di] = one
                a2[dj * 7 + 3 + di] = two
                if di > 0:
                    a1[dj * 7 + 3 - di] = pltpu.roll(one, di, 1)
                    a2[dj * 7 + 3 - di] = pltpu.roll(two, di, 1)


def apply_operator(a1, a2, c):
    cs = pltpu.roll(c, 64, 1)
    plain = [(shifted(c, -di, 1), shifted(cs, -di, 1)) for di in range(-3, 4)]
    y = jnp.zeros((EXT, 128), F32)
    for dj in range(4):
        ahead = jnp.zeros((EXT, 128), F32)
        back = jnp.zeros((EXT, 128), F32)
        for t in range(7):
            p, s = plain[t]
            u, v = a1[dj * 7 + t], a2[dj * 7 + t]
            ahead = ahead + u * shifted(p, -dj, 0) + v * shifted(s, -dj, 0)
            if dj:
                back = back + u * p + v * s
        y = y + ahead
        if dj:
            y = y + pltpu.roll(back, dj, 0)
    return y


def total(a):
    return jnp.sum(jnp.sum(a, axis=0, keepdims=True), axis=1, keepdims=True)


def fields(items):
    row = lax.broadcasted_iota(jnp.int32, (EXT, 128), 0)
    valid = (row >= 2) & (row < 66)
    return valid, [jnp.where(valid, v[:, 0:128] + v[:, 128:256], 0.0) for v in items[15:18]]


def narrow(a):
    return pltpu.roll(a, EXT - 2, 0)[0:GRID]


def widen(a):
    return pltpu.roll(jnp.concatenate([a, jnp.zeros((EXT - GRID, 128), F32)], axis=0), 2, 0)


def direction(valid, grads, sums, c, hc):
    gf, gm, g1 = grads
    s_fm, s_f, s_m, s_mm = sums
    mean_f = s_f / PIXELS
    if c is None:
        s_w, s_ww, s_fw, gw = s_m, s_mm, s_fm, gm
    else:
        s_w = s_m + total(g1 * c)
        s_ww = s_mm + total(c * (2.0 * gm + hc))
        s_fw = s_fm + total(gf * c)
        gw = gm + hc
    mean_w = s_w / PIXELS
    var = s_ww - PIXELS * mean_w * mean_w
    cross = s_fw - PIXELS * mean_f * mean_w
    den = jnp.sqrt(var + EPS)
    ratio = cross / den / (var + EPS)
    g = PIXELS * ((gf - mean_f * g1) / den - ratio * (gw - mean_w * g1))
    g = jnp.where(valid, g, 0.0)
    return g / jnp.sqrt(total(g * g) / 8192.0 + EPS)


def solve_a(pos_ref, far0, far1, far2, far3, out_ref, lead_ref, a1, a2, kept_ref, all_ref):
    items, sums = unpack(pos_ref, (far0, far1, far2, far3), all_ref)
    build_operator(items, a1, a2)
    valid, grads = fields(items)
    for t in range(3):
        kept_ref[EXT * t : EXT * t + EXT, :] = grads[t]
    for t in range(4):
        kept_ref[3 * EXT + t : 3 * EXT + t + 1, :] = jnp.broadcast_to(sums[t], (1, 128))
    c = RATE * direction(valid, grads, sums, None, None)
    d = direction(valid, grads, sums, c, apply_operator(a1, a2, c))
    lead = narrow(c)
    out_ref[0:GRID, :] = lead
    lead_ref[...] = lead
    out_ref[GRID : 2 * GRID, :] = narrow(d)


def solve_b(pos_ref, a1, a2, kept_ref, own_ref, prev_ref, next_ref, prev2_ref, next2_ref, out_ref):
    k = pos_ref[0]
    row = lax.broadcasted_iota(jnp.int32, (EXT, 128), 0)
    valid = (row >= 2) & (row < 66)
    grads = [kept_ref[EXT * t : EXT * t + EXT, :] for t in range(3)]
    sums = [kept_ref[3 * EXT + t : 3 * EXT + t + 1, 0:1] for t in range(4)]

    def lap(a, b, c):
        return a - 2.0 * b + c

    def pair(ref, there):
        return [jnp.where(there, widen(ref[GRID * t : GRID * t + GRID, :]), 0.0) for t in range(2)]

    has_prev, has_next = k > 0, k < 7
    c1, d1 = pair(own_ref, k >= 0)
    cl, dl = pair(prev_ref, has_prev)
    cr, dr = pair(next_ref, has_next)
    cll = jnp.where(k > 1, widen(prev2_ref[...]), 0.0)
    crr = jnp.where(k < 6, widen(next2_ref[...]), 0.0)
    c2 = c1 + RATE * d1 + SMOOTH * lap(cl, c1, cr)
    c2l = jnp.where(has_prev, cl + RATE * dl + SMOOTH * lap(cll, cl, c1), 0.0)
    c2r = jnp.where(has_next, cr + RATE * dr + SMOOTH * lap(c1, cr, crr), 0.0)
    d2 = direction(valid, grads, sums, c2, apply_operator(a1, a2, c2))
    c3 = c2 + RATE * d2 + SMOOTH * lap(c2l, c2, c2r)
    d3 = direction(valid, grads, sums, c3, apply_operator(a1, a2, c3))
    out_ref[0:GRID, :] = narrow(c3 + RATE * d3)
    out_ref[GRID : 2 * GRID, :] = narrow(c3)


def pair_sum(pos_ref, own_ref, other_ref, out_ref, more_ref):
    k = pos_ref[0]
    even = jnp.where(k % 2 == 0, own_ref[GRID : 2 * GRID, :], other_ref[GRID : 2 * GRID, :])
    both = own_ref[0:GRID, :] + other_ref[0:GRID, :] - jnp.where(k < 2, SMOOTH, 0.0) * even
    out_ref[...] = both
    more_ref[0:GRID, :] = both
    more_ref[GRID : 2 * GRID, :] = even


def finish(pos_ref, m_ref, xs, ys, own_ref, other_ref, one_ref, two_ref, more_ref, r8_hbm, turned_ref, out_ref, acc_ref, sx, sy, total_ref, mixed, buf, r8_ref, sems, fetched):
    bring = pltpu.make_async_copy(r8_hbm, r8_ref, fetched)
    bring.start()
    k = pos_ref[0]
    odd = k % 2 == 1
    own_c, other_c = own_ref[GRID : 2 * GRID, :], other_ref[GRID : 2 * GRID, :]
    after = jnp.where(odd, jnp.where(k < 7, more_ref[GRID : 2 * GRID, :], 0.0), other_c)
    acc = own_ref[0:GRID, :] + jnp.where(odd, other_ref[0:GRID, :], 0.0) + SMOOTH * (after - own_c)
    acc = acc - jnp.where(k < 2, SMOOTH, 0.0) * jnp.where(odd, other_c, own_c)
    acc = acc + jnp.where(k > 1, one_ref[...], 0.0) + jnp.where(k > 3, two_ref[...], 0.0)
    acc = acc + jnp.where(k > 5, more_ref[0:GRID, :], 0.0)
    acc_ref[...] = acc
    total_ref[...] = widen(acc)
    c8 = total_ref[pl.ds(4 * pos_ref[1], 8), :]
    bring.wait()
    mixed[...] = jnp.dot(r8_ref[...], c8, precision=lax.Precision.HIGHEST, preferred_element_type=F32).astype(BF)

    def copy(step):
        return pltpu.make_async_copy(buf.at[:, tile(step)], out_ref.at[:, tile(step)], sems.at[step])

    def body(step, carry):
        sx[...] = dot(mixed[:, 0:64], turned_ref[:, tile(step)])
        sy[...] = dot(mixed[:, 64:128], turned_ref[:, tile(step)])
        for s in range(BLOCK // 256):
            at = pl.ds(256 * s, 256)
            from_m = pl.ds(pl.multiple_of(BLOCK * step + 256 * s, 256), 256)
            for c in range(ROWS // CHUNK):
                rows = pl.ds(CHUNK * c, CHUNK)
                m = m_ref[rows, from_m].astype(F32)
                buf[rows, from_m] = (m + sx[rows, at] * xs[rows, from_m] + sy[rows, at] * ys[rows, from_m]).astype(BF)
        copy(step).start()
        return carry

    lax.fori_loop(0, STEPS, body, 0)
    for step in range(STEPS):
        copy(step).wait()


def around_four(array, stride, by):
    def to(q):
        here = q // stride % 4
        return q + stride * ((here + by) % 4 - here)

    return lax.ppermute(array, "quad", [(q, to(q)) for q in range(16)])


def ring(array, axis, by):
    n = lax.axis_size(axis)
    return lax.ppermute(array, axis, [(i, (i + by) % n) for i in range(n)])


FIELD = pltpu.VMEM((ROWS, BLOCK), BF)
WIDE = pltpu.VMEM((ROWS, BLOCK), F32)
SMALL = pltpu.VMEM((8, 128), F32)


def call(kernel, name, args, outs, scratch, limit, hbm_out=False, hbm_in=()):
    vm = pl.BlockSpec(memory_space=pltpu.VMEM)
    specs = [pl.BlockSpec(memory_space=pltpu.SMEM) if a.dtype == jnp.int32 else vm for a in args]
    for i in hbm_in:
        specs[i] = pl.BlockSpec(memory_space=pltpu.HBM)
    return pl.pallas_call(
        kernel,
        in_specs=specs,
        out_specs=[pl.BlockSpec(memory_space=pl.ANY) if hbm_out and i == 0 else vm for i in range(len(outs))],
        out_shape=outs,
        scratch_shapes=scratch,
        name=name,
        compiler_params=pltpu.CompilerParams(vmem_limit_bytes=limit << 20),
    )(*args)


def local(sections, anchor):
    strip = sections[0]
    pos = jnp.stack([lax.axis_index("chain"), lax.axis_index("quad")]).astype(jnp.int32)
    r8, blob, edge = host_tables()
    prior = ring(strip, "chain", 1)
    up = ring(strip[ROWS - 1 : ROWS], "quad", 1)
    dn = ring(strip[0:1], "quad", -1)
    turned = col_table()
    shape = jax.ShapeDtypeStruct
    slope = shape((ROWS, COLS), F32)
    h, p, xs, ys, before = call(
        stage0,
        "stage0",
        (pos, strip, up, dn, blob, edge, anchor),
        [shape((96, 256), F32), shape((24, 128), F32), slope, slope, shape((ROWS, COLS), BF)],
        [pltpu.SemaphoreType.DMA] + [FIELD] * 7 + [pltpu.VMEM((96 * STEPS, 128), F32), pltpu.VMEM((24 * STEPS, 128), F32), pltpu.VMEM((8, COLS), F32), SMALL],
        24,
        hbm_in=(6,),
    )
    (packed,) = call(
        stage1,
        "stage1",
        (pos, strip, xs, ys, blob, before, prior, h, p),
        [shape((128, 256), BF)],
        [FIELD] * 4 + [pltpu.VMEM((16 * STEPS, 128), F32), SMALL],
        20,
    )
    packed, turned = lax.optimization_barrier((packed, turned))
    four = [packed] + [around_four(packed, 1, d) for d in (1, 2, 3)]
    (near,) = call(merge, "merge", (pos, *four), [shape((360, 256), BF)], [pltpu.VMEM((4, 128, 256), BF)], 12)
    far = [near] + [around_four(near, 4, d) for d in (1, 2, 3)]
    operator = [shape((28, EXT, 128), F32)] * 2
    first, lead, a1, a2, kept = call(
        solve_a,
        "solve_a",
        (pos, *far),
        [shape((2 * GRID, 128), F32), shape((GRID, 128), F32), *operator, shape((3 * EXT + 8, 128), F32)],
        [pltpu.VMEM((4, 360, 256), BF)],
        12,
    )
    around = [ring(first, "chain", 1), ring(first, "chain", -1), ring(lead, "chain", 2), ring(lead, "chain", -2)]
    (own,) = call(solve_b, "solve_b", (pos, a1, a2, kept, first, *around), [shape((2 * GRID, 128), F32)], [], 12)
    other = lax.ppermute(own, "chain", [(i, i ^ 1) for i in range(8)])
    both, more = call(pair_sum, "pair_sum", (pos, own, other), [shape((GRID, 128), F32), shape((2 * GRID, 128), F32)], [], 12)
    earlier = [ring(both, "chain", 2), ring(both, "chain", 4), ring(more, "chain", -2)]
    registered, accumulated = call(
        finish,
        "finish",
        (pos, strip, xs, ys, own, other, *earlier, jnp.asarray(r8), turned),
        [shape((ROWS, COLS), BF), shape((GRID, 128), F32)],
        [WIDE] * 2
        + [pltpu.VMEM((EXT, 128), F32), pltpu.VMEM((ROWS, 128), BF), pltpu.VMEM((ROWS, COLS), BF), pltpu.VMEM((ROWS, 8), F32)]
        + [pltpu.SemaphoreType.DMA((STEPS,)), pltpu.SemaphoreType.DMA],
        24,
        hbm_out=True,
        hbm_in=(9,),
    )
    return registered[None], accumulated[None]


def solution(mesh):
    in_specs = (P("chain", "quad", None), P("quad", None))
    out_specs = (P("chain", "quad", None), P("chain", None, None))
    return jax.shard_map(local, mesh=mesh, in_specs=in_specs, out_specs=out_specs, check_vma=False)
```

```python
import jax
import jax.numpy as jnp
import numpy as np
from jax import lax
from jax.experimental import pallas as pl
from jax.experimental.pallas import tpu as pltpu
from jax.sharding import PartitionSpec as P

GRID = 64
SPACING = 64
ROWS = 256
COLS = 4096
BLOCK = 1024
STEPS = COLS // BLOCK
CHUNK = 32
EXT = 72
PIXELS = 4096.0 * 4096.0
EPS = 1e-6
RATE = 0.25
SMOOTH = 0.25
BF = jnp.bfloat16
F32 = jnp.float32


def weight(offset, xp):
    d = xp.abs(offset)
    near = 2.0 / 3.0 - d * d + 0.5 * d * d * d
    r = 2.0 - d
    far = r * r * r / 6.0
    return xp.where(d < 1.0, near, xp.where(d < 2.0, far, 0.0 * d))


def local_rows():
    r = np.arange(ROWS, dtype=np.float32)
    j = np.arange(8, dtype=np.float32) - 2.0
    off = (r[:, None] + np.float32(0.5)) / np.float32(SPACING) - j[None, :] - np.float32(0.5)
    return weight(off.astype(np.float32), np).astype(np.float32)


def hi_lo(a):
    hi = a.astype(BF)
    return hi, (a - hi.astype(F32)).astype(BF)


def split3(a):
    hi = a.astype(BF)
    rest = a - hi.astype(F32)
    mid = rest.astype(BF)
    lo = (rest - mid.astype(F32)).astype(BF)
    return jnp.concatenate([hi.astype(F32), mid.astype(F32), lo.astype(F32)], axis=0).astype(BF)


def sum3(a, n):
    return a[0:n] + a[n : 2 * n] + a[2 * n : 3 * n]


def two(a):
    hi = a.astype(np.dtype(BF)).astype(np.float32)
    return np.concatenate([hi, a - hi], 0)


def host_tables():
    r8 = local_rows()
    pairs = np.zeros((32, ROWS), np.float32)
    c8 = r8.astype(np.dtype(BF)).astype(np.float32)
    lanes = np.zeros((BLOCK, 128), np.float32)
    cols = np.zeros((BLOCK, 128), np.float32)
    place = np.zeros((STEPS * 128, 256), np.float32)
    put = np.zeros((STEPS * 128, 128), np.float32)
    for s in range(4):
        cols[256 * s : 256 * s + 256, 8 * s : 8 * s + 8] = c8
    for d in range(4):
        for e in range(8 - d):
            pairs[d * 8 + e] = r8[:, e] * r8[:, e + d]
            for s in range(4):
                lanes[256 * s : 256 * s + 256, 32 * s + 8 * d + e] = c8[:, e] * c8[:, e + d]
                for t in range(STEPS):
                    i = 16 * t + 4 * s - 2 + e
                    if i >= 0 and i + d < GRID:
                        place[128 * t + 32 * s + 8 * d + e, 64 * d + i] = 1.0
    for t in range(STEPS):
        for s in range(4):
            for e in range(8):
                i = 16 * t + 4 * s - 2 + e
                if 0 <= i < GRID:
                    put[128 * t + 8 * s + e, i] = 1.0
    diff = np.zeros((8, ROWS), np.float32)
    diff[:, 1:] += 0.5 * r8.T[:, :-1]
    diff[:, :-1] -= 0.5 * r8.T[:, 1:]
    lanes_hi = lanes.astype(np.dtype(BF)).astype(np.float32)
    down = 0.5 * (np.eye(ROWS, k=1) - np.eye(ROWS, k=-1))
    across = np.zeros((512, 256), np.float32)
    o = np.arange(256)
    across[o + 129, o] = 0.5
    across[o + 127, o] = -0.5
    plain = np.concatenate([two(r8.T), two(diff), np.ones((16, ROWS), np.float32)], 0)
    wide = np.concatenate([lanes_hi, lanes - lanes_hi], 1)
    halves = np.concatenate([np.concatenate([cols[0:512], cols[512:1024]], 1), np.concatenate([put[0:256], put[256:512]], 1)], 0)
    blob = np.concatenate([down, across, two(pairs), two(r8.T), plain, wide, place, halves], 0)
    edge = np.stack([-0.5 * r8[0], 0.5 * r8[ROWS - 1]], 0).reshape(16, 1) * np.ones((1, 128), np.float32)
    return r8, jnp.asarray(blob.astype(np.dtype(BF))), jnp.asarray(edge.astype(np.float32))


DOWN, ACROSS, PAIRS, LIN, PLAIN, TABLE, PLACE, COLT, PUT, BLOB = 0, 256, 768, 832, 848, 896, 1920, 2432, 2944, 3200


def col_part(blob_ref, lhs):
    return dot(lhs[:, 0:512], blob_ref[COLT : COLT + 512, 0:128]) + dot(lhs[:, 512:1024], blob_ref[COLT : COLT + 512, 128:256])


def put_rows(blob_ref, t):
    return blob_ref[PUT + 128 * (t % 2) : PUT + 128 * (t % 2) + 128, 128 * (t // 2) : 128 * (t // 2) + 128]


def col_table():
    x = jnp.arange(COLS, dtype=jnp.int32).astype(F32)
    j = jnp.arange(GRID, dtype=jnp.int32).astype(F32)
    return weight((x[None, :] + 0.5) / SPACING - j[:, None] - 0.5, jnp).astype(BF)


def dot(a, b):
    return jnp.dot(a, b, preferred_element_type=F32)


def tile(step, size=BLOCK):
    return pl.ds(pl.multiple_of(size * step, size), size)


def slopes(pos_ref, m_ref, up_ref, dn_ref, blob_ref, lhs, xs, ys, step):
    start = BLOCK * step
    left = m_ref[:, pl.ds(pl.multiple_of(jnp.maximum(start - 128, 0), 128), 128)]
    right = m_ref[:, pl.ds(pl.multiple_of(jnp.minimum(start + BLOCK, COLS - 128), 128), 128)]
    left = jnp.where(step > 0, left.astype(F32), 0.0).astype(BF)
    right = jnp.where(step < STEPS - 1, right.astype(F32), 0.0).astype(BF)
    block = m_ref[:, tile(step)]
    ext = jnp.concatenate([left, block, right], axis=1)
    stack = jnp.concatenate([ext[:, 256 * s : 256 * s + 512] for s in range(4)], axis=0)
    x = dot(stack, blob_ref[ACROSS : ACROSS + 512, :])
    for s in range(4):
        xs[:, pl.ds(pl.multiple_of(start + 256 * s, 256), 256)] = x[256 * s : 256 * s + 256]
    up = jnp.where(pos_ref[1] > 0, up_ref[:, tile(step)].astype(F32), 0.0)
    dn = jnp.where(pos_ref[1] < 15, dn_ref[:, tile(step)].astype(F32), 0.0)
    both = dot(jnp.concatenate([blob_ref[DOWN : DOWN + 256, :], lhs], axis=0), block)
    at = tile(step)
    ys[:, at] = both[0:256]
    ys[0:1, at] = ys[0:1, at] - 0.5 * up
    ys[ROWS - 1 : ROWS, at] = ys[ROWS - 1 : ROWS, at] + 0.5 * dn
    return up, dn, both[256:]


def fold8(a):
    return jnp.sum(a.reshape(CHUNK // 8, 8, a.shape[1]), axis=0)


def lanes_to_row(a):
    s = jnp.sum(a, axis=0, keepdims=True)
    out = s[:, 0:128]
    for t in range(1, s.shape[1] // 128):
        out = out + s[:, 128 * t : 128 * t + 128]
    return out


def rows_of(lin, hi, lo):
    a = dot(lin, hi)
    b = dot(lin, lo)
    return a[0:8] + a[8:16] + b[0:8]


def stage0(pos_ref, m_ref, up_ref, dn_ref, blob_ref, edge_ref, anchor_hbm, h_ref, p_ref, xs, ys, anchor_ref, fetched, fxx, fxy, fyy, mxh, mxl, myh, myl, zacc, lacc, l1_ref, sums):
    bring = pltpu.make_async_copy(anchor_hbm, anchor_ref, fetched)
    bring.start()
    sums[...] = jnp.zeros((8, 128), F32)

    def body(step, carry):
        up, dn, ones = slopes(pos_ref, m_ref, up_ref, dn_ref, blob_ref, blob_ref[PLAIN : PLAIN + 48, :], xs, ys, step)
        pairs = blob_ref[PAIRS : PAIRS + 64, :]
        lin = blob_ref[LIN : LIN + 16, :]
        sumsq = jnp.zeros((8, 256), F32)
        t_parts, lx, ly = [], [], []
        for s in range(BLOCK // 256):
            at = pl.ds(256 * s, 256)
            from_m = pl.ds(pl.multiple_of(BLOCK * step + 256 * s, 256), 256)
            for c in range(ROWS // CHUNK):
                rows = pl.ds(CHUNK * c, CHUNK)
                m, x, y = m_ref[rows, from_m].astype(F32), xs[rows, from_m], ys[rows, from_m]
                fxx[rows, at] = (x * x).astype(BF)
                fxy[rows, at] = (x * y).astype(BF)
                fyy[rows, at] = (y * y).astype(BF)
                mxh[rows, at], mxl[rows, at] = hi_lo(m * x)
                myh[rows, at], myl[rows, at] = hi_lo(m * y)
                sumsq = sumsq + fold8(m * m)
            trio = []
            for f in (fxx, fxy, fyy):
                t = dot(pairs, f[:, at])
                trio.append(t[0:32] + t[32:64])
            t_parts.append(jnp.concatenate(trio, axis=0))
            lx.append(rows_of(lin, mxh[:, at], mxl[:, at]))
            ly.append(rows_of(lin, myh[:, at], myl[:, at]))
        t_hi, t_lo = hi_lo(jnp.concatenate(t_parts, axis=1))
        z = dot(jnp.concatenate([t_hi, t_lo], axis=0), blob_ref[TABLE : TABLE + 1024, :])
        z = z[0:96] + z[96:192]
        zacc[tile(step, 96), :] = z[:, 0:128] + z[:, 128:256]
        l1_ref[:, tile(step)] = ones[0:8] + ones[8:16]
        l1y = ones[16:24] + ones[24:32]
        l1y = l1y + edge_ref[0:8, 0:1] * up + edge_ref[8:16, 0:1] * dn
        rows3 = jnp.concatenate([jnp.concatenate(lx, axis=1), jnp.concatenate(ly, axis=1), l1y], axis=0)
        lacc[tile(step, 24), :] = sum3(col_part(blob_ref, split3(rows3)), 24)
        sums[0:1, :] += lanes_to_row(ones[32:33])
        sums[1:2, :] += lanes_to_row(sumsq)
        return carry

    lax.fori_loop(0, STEPS, body, 0)
    bring.wait()
    l1 = l1_ref[...]
    col = lax.broadcasted_iota(jnp.int32, l1.shape, 1)
    after = jnp.where(col < COLS - 1, pltpu.roll(l1, COLS - 1, 1), 0.0)
    before = jnp.where(col > 0, pltpu.roll(l1, 1, 1), 0.0)
    l1x = split3(0.5 * (after - before))
    h = jnp.zeros((288, 256), F32)
    p = jnp.zeros((96, 128), F32)
    for t in range(STEPS):
        h = h + dot(split3(zacc[96 * t : 96 * t + 96, :]), blob_ref[PLACE + 128 * t : PLACE + 128 * t + 128, :])
        one = sum3(col_part(blob_ref, l1x[:, BLOCK * t : BLOCK * t + BLOCK]), 8)
        p = p + dot(split3(jnp.concatenate([lacc[24 * t : 24 * t + 24, :], one], axis=0)), put_rows(blob_ref, t))
    h_ref[...] = sum3(h, 96)
    p = sum3(p, 32)
    p_ref[0:8, :] = p[0:8] + pltpu.roll(p[8:16], 64, 1)
    p_ref[8:16, :] = p[24:32] + pltpu.roll(p[16:24], 64, 1)
    p_ref[16:24, :] = sums[...]


def cross_part(pos_ref, m_ref, xs, ys, blob_ref, anchor_ref, prior_ref, fxh, fxl, fyh, fyl, lacc, sums):
    sums[...] = jnp.zeros((8, 128), F32)

    def body(f_ref, step, carry):
        lin = blob_ref[LIN : LIN + 16, :]
        cross = jnp.zeros((8, 256), F32)
        whole_sum = jnp.zeros((8, 256), F32)
        lx, ly = [], []
        for s in range(BLOCK // 256):
            at = pl.ds(256 * s, 256)
            from_m = pl.ds(pl.multiple_of(BLOCK * step + 256 * s, 256), 256)
            for c in range(ROWS // CHUNK):
                rows = pl.ds(CHUNK * c, CHUNK)
                m, x, y = m_ref[rows, from_m].astype(F32), xs[rows, from_m], ys[rows, from_m]
                f = f_ref[rows, from_m].astype(F32)
                fxh[rows, at], fxl[rows, at] = hi_lo(f * x)
                fyh[rows, at], fyl[rows, at] = hi_lo(f * y)
                cross = cross + fold8(f * m)
                whole_sum = whole_sum + fold8(f)
            lx.append(rows_of(lin, fxh[:, at], fxl[:, at]))
            ly.append(rows_of(lin, fyh[:, at], fyl[:, at]))
        rows2 = jnp.concatenate([jnp.concatenate(lx, axis=1), jnp.concatenate(ly, axis=1)], axis=0)
        lacc[tile(step, 16), :] = sum3(col_part(blob_ref, split3(rows2)), 16)
        sums[0:1, :] += lanes_to_row(cross)
        sums[1:2, :] += lanes_to_row(whole_sum)
        return carry

    @pl.when(pos_ref[0] == 0)
    def _():
        lax.fori_loop(0, STEPS, lambda i, c: body(anchor_ref, i, c), 0)

    @pl.when(pos_ref[0] > 0)
    def _():
        lax.fori_loop(0, STEPS, lambda i, c: body(prior_ref, i, c), 0)

    p = jnp.zeros((48, 128), F32)
    for i in range(STEPS):
        p = p + dot(split3(lacc[16 * i : 16 * i + 16, :]), put_rows(blob_ref, i))
    p = sum3(p, 16)
    return p[0:8] + pltpu.roll(p[8:16], 64, 1)


def rows8(shape):
    return lax.broadcasted_iota(jnp.int32, shape, 0) % 8


def stage1(pos_ref, m_ref, xs, ys, blob_ref, anchor_ref, prior_ref, h_ref, p_ref, out_ref, *scratch):
    sums = scratch[-1]
    part = cross_part(pos_ref, m_ref, xs, ys, blob_ref, anchor_ref, prior_ref, *scratch)
    row = rows8((8, 256))
    lane = lax.broadcasted_iota(jnp.int32, (8, 256), 1)
    last = jnp.zeros((8, 256), F32)
    for t, v in enumerate((sums[0:1, :], sums[1:2, :], p_ref[16:17, :], p_ref[17:18, :])):
        rest = jnp.sum(v, axis=1, keepdims=True)
        for u in range(3):
            piece = rest.astype(BF).astype(F32)
            rest = rest - piece
            last = last + jnp.where((row == 6) & (lane == 4 * u + t), piece, 0.0)
    groups = []
    lows = []
    for c in range(3):
        a, b, d, e = [h_ref[32 * c + 8 * t : 32 * c + 8 * t + 8, :] for t in range(4)]
        groups += [a, b + jnp.where(row == 7, pltpu.roll(e, 3, 0), 0.0), d + jnp.where(row > 5, pltpu.roll(e, 4, 0), 0.0)]
        last = last + jnp.where((row == 2 * c) | (row == 2 * c + 1), shifted(e, 2 * c, 0), 0.0)
        low = [v[:, 0:128] - v[:, 0:128].astype(BF).astype(F32) for v in (a, b)]
        lows.append(jnp.concatenate(low, axis=1))
    groups.append(last)
    groups += lows
    for v in (part, p_ref[0:8, :], p_ref[8:16, :]):
        groups.append(jnp.concatenate([v, v - v.astype(BF).astype(F32)], axis=1))
    packed = jnp.concatenate(groups, axis=0).astype(BF)
    out_ref[...] = packed


def shifted(a, by, axis):
    n = a.shape[axis]
    by = by % n
    return a if by == 0 else pltpu.roll(a, by, axis)


def stacked(even, odd):
    pad = jnp.zeros((8, even.shape[1]), F32)
    return jnp.concatenate([even, pad], axis=0) + pltpu.roll(jnp.concatenate([odd, pad], axis=0), 4, 0)


def merge(pos_ref, near0, near1, near2, near3, out_ref, all_ref):
    y = pos_ref[1] % 4
    for e, ref in enumerate((near0, near1, near2, near3)):
        all_ref[(y + 4 - e) % 4] = ref[...]
    groups = [([], []) for _ in range(16)]
    for q in range(4):
        for t in range(8):
            both = all_ref[q, 16 * t : 16 * t + 16, :].astype(F32)
            groups[2 * t][q % 2].append(both[0:8])
            groups[2 * t + 1][q % 2].append(both[8:16])
    groups = [[jnp.concatenate(v, axis=0) for v in pair] for pair in groups]
    row = rows8((16, 256))
    pad = jnp.zeros((16, 128), F32)

    def piece(c, dj, side):
        a, b, d, last, rest = [groups[g][side] for g in (3 * c, 3 * c + 1, 3 * c + 2, 9, 10 + c)]
        if dj == 0:
            return a + jnp.concatenate([rest[:, 0:128], pad], axis=1)
        if dj == 1:
            return jnp.where(row < 7, b, 0.0) + jnp.concatenate([rest[:, 128:256], pad], axis=1)
        if dj == 2:
            return jnp.where(row < 6, d, 0.0)
        e = jnp.where(row == 4, pltpu.roll(b, 13, 0), jnp.where(row > 1, pltpu.roll(d, 12, 0), shifted(last, -2 * c, 0)))
        return jnp.where(row < 5, e, 0.0)

    items, lows = [], []
    for c in range(3):
        four = [stacked(piece(c, dj, 0), piece(c, dj, 1)) for dj in range(4)]
        items += four
        lows.append(jnp.concatenate([v[:, 0:128] - v[:, 0:128].astype(BF).astype(F32) for v in four[0:2]], axis=1))
    last = groups[9][0] + groups[9][1]
    lane = lax.broadcasted_iota(jnp.int32, (16, 256), 1)
    here = (row == 6) & (lane < 12)
    row24 = lax.broadcasted_iota(jnp.int32, (24, 256), 0)
    lane24 = lax.broadcasted_iota(jnp.int32, (24, 256), 1)
    for t in range(4):
        rest = total(jnp.where(here & (lane % 4 == t), last, 0.0))
        for u in range(3):
            part = rest.astype(BF).astype(F32)
            rest = rest - part
            items[3] = items[3] + jnp.where((row24 == 19) & (lane24 == 4 * u + t), part, 0.0)
    items += lows
    for g in (13, 14, 15):
        even, odd = [v[:, 0:128] + v[:, 128:256] for v in groups[g]]
        v = stacked(even, odd)
        items.append(jnp.concatenate([v, v - v.astype(BF).astype(F32)], axis=1))
    room = jnp.zeros((16, 256), F32)
    pairs = []
    for p in range(9):
        a, b = [jnp.concatenate([v, room], axis=0) for v in items[2 * p : 2 * p + 2]]
        pairs.append(a + pltpu.roll(b, 20, 0))
    out_ref[...] = jnp.concatenate(pairs, axis=0).astype(BF)


def unpack(pos_ref, far, all_ref):
    z = pos_ref[1] // 4
    for d in range(4):
        all_ref[(z + 4 - d) % 4] = far[d][...]
    blocks = [all_ref[t].astype(F32) for t in range(4)]
    row = lax.broadcasted_iota(jnp.int32, (8, 256), 0)
    lane = lax.broadcasted_iota(jnp.int32, (8, 256), 1)
    eight = jnp.zeros((8, 256), F32)
    out = []
    sums = None
    for i in range(18):
        body, tails = [], [eight, eight]
        for t in range(4):
            full = blocks[t][40 * (i // 2) : 40 * (i // 2) + 40]
            if i % 2:
                full = pltpu.roll(full, 20, 0)
            body.append(full[0:16])
            tail = full[16:24]
            if i == 3:
                sums = tail if sums is None else sums + tail
            tails += [jnp.where(row < (3 if i == 3 else 4), tail, 0.0), eight]
        out.append(jnp.concatenate(body + [eight], axis=0) + jnp.concatenate(tails[:-1], axis=0))
    here = (row == 3) & (lane < 12)
    return out, [total(jnp.where(here & (lane % 4 == t), sums, 0.0)) for t in range(4)]


def build_operator(items, a1, a2):
    lane = lax.broadcasted_iota(jnp.int32, (EXT, 128), 1)
    low = lane < 64
    for dj in range(4):
        for pair in range(2):
            three = []
            for c in range(3):
                v = items[4 * c + dj][:, 128 * pair : 128 * pair + 128]
                if pair == 0 and dj < 2:
                    v = v + items[12 + c][:, 128 * dj : 128 * dj + 128]
                three.append(v)
            xx, xy, yy = three
            xx_s, xy_s, yy_s = [pltpu.roll(v, 64, 1) for v in (xx, xy, yy)]
            for odd in range(2):
                di = 2 * pair + odd
                if odd == 0:
                    one = jnp.where(low, xx, yy_s)
                    two = jnp.where(low, xy, xy_s)
                else:
                    one = jnp.where(low, xx_s, yy)
                    two = jnp.where(low, xy_s, xy)
                a1[dj * 7 + 3 + di] = one
                a2[dj * 7 + 3 + di] = two
                if di > 0:
                    a1[dj * 7 + 3 - di] = pltpu.roll(one, di, 1)
                    a2[dj * 7 + 3 - di] = pltpu.roll(two, di, 1)


def apply_operator(a1, a2, c):
    cs = pltpu.roll(c, 64, 1)
    plain = [(shifted(c, -di, 1), shifted(cs, -di, 1)) for di in range(-3, 4)]
    y = jnp.zeros((EXT, 128), F32)
    for dj in range(4):
        ahead = jnp.zeros((EXT, 128), F32)
        back = jnp.zeros((EXT, 128), F32)
        for t in range(7):
            p, s = plain[t]
            u, v = a1[dj * 7 + t], a2[dj * 7 + t]
            ahead = ahead + u * shifted(p, -dj, 0) + v * shifted(s, -dj, 0)
            if dj:
                back = back + u * p + v * s
        y = y + ahead
        if dj:
            y = y + pltpu.roll(back, dj, 0)
    return y


def total(a):
    return jnp.sum(jnp.sum(a, axis=0, keepdims=True), axis=1, keepdims=True)


def fields(items):
    row = lax.broadcasted_iota(jnp.int32, (EXT, 128), 0)
    valid = (row >= 2) & (row < 66)
    return valid, [jnp.where(valid, v[:, 0:128] + v[:, 128:256], 0.0) for v in items[15:18]]


def narrow(a):
    return pltpu.roll(a, EXT - 2, 0)[0:GRID]


def widen(a):
    return pltpu.roll(jnp.concatenate([a, jnp.zeros((EXT - GRID, 128), F32)], axis=0), 2, 0)


def direction(valid, grads, sums, c, hc):
    gf, gm, g1 = grads
    s_fm, s_f, s_m, s_mm = sums
    mean_f = s_f / PIXELS
    if c is None:
        s_w, s_ww, s_fw, gw = s_m, s_mm, s_fm, gm
    else:
        s_w = s_m + total(g1 * c)
        s_ww = s_mm + total(c * (2.0 * gm + hc))
        s_fw = s_fm + total(gf * c)
        gw = gm + hc
    mean_w = s_w / PIXELS
    var = s_ww - PIXELS * mean_w * mean_w
    cross = s_fw - PIXELS * mean_f * mean_w
    den = jnp.sqrt(var + EPS)
    ratio = cross / den / (var + EPS)
    g = PIXELS * ((gf - mean_f * g1) / den - ratio * (gw - mean_w * g1))
    g = jnp.where(valid, g, 0.0)
    return g / jnp.sqrt(total(g * g) / 8192.0 + EPS)


def solve_a(pos_ref, far0, far1, far2, far3, out_ref, lead_ref, a1, a2, kept_ref, all_ref):
    items, sums = unpack(pos_ref, (far0, far1, far2, far3), all_ref)
    build_operator(items, a1, a2)
    valid, grads = fields(items)
    for t in range(3):
        kept_ref[EXT * t : EXT * t + EXT, :] = grads[t]
    for t in range(4):
        kept_ref[3 * EXT + t : 3 * EXT + t + 1, :] = jnp.broadcast_to(sums[t], (1, 128))
    c = RATE * direction(valid, grads, sums, None, None)
    d = direction(valid, grads, sums, c, apply_operator(a1, a2, c))
    lead = narrow(c)
    out_ref[0:GRID, :] = lead
    lead_ref[...] = lead
    out_ref[GRID : 2 * GRID, :] = narrow(d)


def solve_b(pos_ref, a1, a2, kept_ref, own_ref, prev_ref, next_ref, prev2_ref, next2_ref, out_ref):
    k = pos_ref[0]
    row = lax.broadcasted_iota(jnp.int32, (EXT, 128), 0)
    valid = (row >= 2) & (row < 66)
    grads = [kept_ref[EXT * t : EXT * t + EXT, :] for t in range(3)]
    sums = [kept_ref[3 * EXT + t : 3 * EXT + t + 1, 0:1] for t in range(4)]

    def lap(a, b, c):
        return a - 2.0 * b + c

    def pair(ref, there):
        return [jnp.where(there, widen(ref[GRID * t : GRID * t + GRID, :]), 0.0) for t in range(2)]

    has_prev, has_next = k > 0, k < 7
    c1, d1 = pair(own_ref, k >= 0)
    cl, dl = pair(prev_ref, has_prev)
    cr, dr = pair(next_ref, has_next)
    cll = jnp.where(k > 1, widen(prev2_ref[...]), 0.0)
    crr = jnp.where(k < 6, widen(next2_ref[...]), 0.0)
    c2 = c1 + RATE * d1 + SMOOTH * lap(cl, c1, cr)
    c2l = jnp.where(has_prev, cl + RATE * dl + SMOOTH * lap(cll, cl, c1), 0.0)
    c2r = jnp.where(has_next, cr + RATE * dr + SMOOTH * lap(c1, cr, crr), 0.0)
    d2 = direction(valid, grads, sums, c2, apply_operator(a1, a2, c2))
    c3 = c2 + RATE * d2 + SMOOTH * lap(c2l, c2, c2r)
    d3 = direction(valid, grads, sums, c3, apply_operator(a1, a2, c3))
    out_ref[0:GRID, :] = narrow(c3 + RATE * d3)
    out_ref[GRID : 2 * GRID, :] = narrow(c3)


def pair_sum(pos_ref, own_ref, other_ref, out_ref, more_ref):
    k = pos_ref[0]
    even = jnp.where(k % 2 == 0, own_ref[GRID : 2 * GRID, :], other_ref[GRID : 2 * GRID, :])
    both = own_ref[0:GRID, :] + other_ref[0:GRID, :] - jnp.where(k < 2, SMOOTH, 0.0) * even
    out_ref[...] = both
    more_ref[0:GRID, :] = both
    more_ref[GRID : 2 * GRID, :] = even


def finish(pos_ref, m_ref, xs, ys, own_ref, other_ref, one_ref, two_ref, more_ref, r8_hbm, turned_ref, out_ref, acc_ref, sx, sy, total_ref, mixed, buf, r8_ref, sems, fetched):
    bring = pltpu.make_async_copy(r8_hbm, r8_ref, fetched)
    bring.start()
    k = pos_ref[0]
    odd = k % 2 == 1
    own_c, other_c = own_ref[GRID : 2 * GRID, :], other_ref[GRID : 2 * GRID, :]
    after = jnp.where(odd, jnp.where(k < 7, more_ref[GRID : 2 * GRID, :], 0.0), other_c)
    acc = own_ref[0:GRID, :] + jnp.where(odd, other_ref[0:GRID, :], 0.0) + SMOOTH * (after - own_c)
    acc = acc - jnp.where(k < 2, SMOOTH, 0.0) * jnp.where(odd, other_c, own_c)
    acc = acc + jnp.where(k > 1, one_ref[...], 0.0) + jnp.where(k > 3, two_ref[...], 0.0)
    acc = acc + jnp.where(k > 5, more_ref[0:GRID, :], 0.0)
    acc_ref[...] = acc
    total_ref[...] = widen(acc)
    c8 = total_ref[pl.ds(4 * pos_ref[1], 8), :]
    bring.wait()
    mixed[...] = jnp.dot(r8_ref[...], c8, precision=lax.Precision.HIGHEST, preferred_element_type=F32).astype(BF)

    def copy(step):
        return pltpu.make_async_copy(buf.at[:, tile(step)], out_ref.at[:, tile(step)], sems.at[step])

    def body(step, carry):
        sx[...] = dot(mixed[:, 0:64], turned_ref[:, tile(step)])
        sy[...] = dot(mixed[:, 64:128], turned_ref[:, tile(step)])
        for s in range(BLOCK // 256):
            at = pl.ds(256 * s, 256)
            from_m = pl.ds(pl.multiple_of(BLOCK * step + 256 * s, 256), 256)
            for c in range(ROWS // CHUNK):
                rows = pl.ds(CHUNK * c, CHUNK)
                m = m_ref[rows, from_m].astype(F32)
                buf[rows, from_m] = (m + sx[rows, at] * xs[rows, from_m] + sy[rows, at] * ys[rows, from_m]).astype(BF)
        copy(step).start()
        return carry

    lax.fori_loop(0, STEPS, body, 0)
    for step in range(STEPS):
        copy(step).wait()


def around_four(array, stride, by):
    def to(q):
        here = q // stride % 4
        return q + stride * ((here + by) % 4 - here)

    return lax.ppermute(array, "quad", [(q, to(q)) for q in range(16)])


def ring(array, axis, by):
    n = lax.axis_size(axis)
    return lax.ppermute(array, axis, [(i, (i + by) % n) for i in range(n)])


FIELD = pltpu.VMEM((ROWS, BLOCK), BF)
WIDE = pltpu.VMEM((ROWS, BLOCK), F32)
SMALL = pltpu.VMEM((8, 128), F32)


def call(kernel, name, args, outs, scratch, limit, hbm_out=False, hbm_in=()):
    def body(*refs):
        kernel((lax.axis_index("chain"), lax.axis_index("quad")), *refs)

    vm = pl.BlockSpec(memory_space=pltpu.VMEM)
    specs = [vm] * len(args)
    for i in hbm_in:
        specs[i] = pl.BlockSpec(memory_space=pltpu.HBM)
    return pl.pallas_call(
        body,
        in_specs=specs,
        out_specs=[pl.BlockSpec(memory_space=pl.ANY) if hbm_out and i == 0 else vm for i in range(len(outs))],
        out_shape=outs,
        scratch_shapes=scratch,
        name=name,
        compiler_params=pltpu.CompilerParams(vmem_limit_bytes=limit << 20),
    )(*args)


def local(sections, anchor):
    strip = sections[0]
    r8, blob, edge = host_tables()
    prior = ring(strip, "chain", 1)
    up = ring(strip[ROWS - 1 : ROWS], "quad", 1)
    dn = ring(strip[0:1], "quad", -1)
    turned = col_table()
    shape = jax.ShapeDtypeStruct
    slope = shape((ROWS, COLS), F32)
    h, p, xs, ys, before = call(
        stage0,
        "stage0",
        (strip, up, dn, blob, edge, anchor),
        [shape((96, 256), F32), shape((24, 128), F32), slope, slope, shape((ROWS, COLS), BF)],
        [pltpu.SemaphoreType.DMA] + [FIELD] * 7 + [pltpu.VMEM((96 * STEPS, 128), F32), pltpu.VMEM((24 * STEPS, 128), F32), pltpu.VMEM((8, COLS), F32), SMALL],
        24,
        hbm_in=(5,),
    )
    (packed,) = call(
        stage1,
        "stage1",
        (strip, xs, ys, blob, before, prior, h, p),
        [shape((128, 256), BF)],
        [FIELD] * 4 + [pltpu.VMEM((16 * STEPS, 128), F32), SMALL],
        20,
    )
    packed, turned = lax.optimization_barrier((packed, turned))
    four = [packed] + [around_four(packed, 1, d) for d in (1, 2, 3)]
    (near,) = call(merge, "merge", tuple(four), [shape((360, 256), BF)], [pltpu.VMEM((4, 128, 256), BF)], 12)
    far = [near] + [around_four(near, 4, d) for d in (1, 2, 3)]
    operator = [shape((28, EXT, 128), F32)] * 2
    first, lead, a1, a2, kept = call(
        solve_a,
        "solve_a",
        tuple(far),
        [shape((2 * GRID, 128), F32), shape((GRID, 128), F32), *operator, shape((3 * EXT + 8, 128), F32)],
        [pltpu.VMEM((4, 360, 256), BF)],
        12,
    )
    around = [ring(first, "chain", 1), ring(first, "chain", -1), ring(lead, "chain", 2), ring(lead, "chain", -2)]
    (own,) = call(solve_b, "solve_b", (a1, a2, kept, first, *around), [shape((2 * GRID, 128), F32)], [], 12)
    other = lax.ppermute(own, "chain", [(i, i ^ 1) for i in range(8)])
    both, more = call(pair_sum, "pair_sum", (own, other), [shape((GRID, 128), F32), shape((2 * GRID, 128), F32)], [], 12)
    earlier = [ring(both, "chain", 2), ring(both, "chain", 4), ring(more, "chain", -2)]
    registered, accumulated = call(
        finish,
        "finish",
        (strip, xs, ys, own, other, *earlier, jnp.asarray(r8), turned),
        [shape((ROWS, COLS), BF), shape((GRID, 128), F32)],
        [WIDE] * 2
        + [pltpu.VMEM((EXT, 128), F32), pltpu.VMEM((ROWS, 128), BF), pltpu.VMEM((ROWS, COLS), BF), pltpu.VMEM((ROWS, 8), F32)]
        + [pltpu.SemaphoreType.DMA((STEPS,)), pltpu.SemaphoreType.DMA],
        24,
        hbm_out=True,
        hbm_in=(8,),
    )
    return registered[None], accumulated[None]


def solution(mesh):
    in_specs = (P("chain", "quad", None), P("quad", None))
    out_specs = (P("chain", "quad", None), P("chain", None, None))
    return jax.shard_map(local, mesh=mesh, in_specs=in_specs, out_specs=out_specs, check_vma=False)
```

```python
import jax
import jax.numpy as jnp
import numpy as np
from jax import lax
from jax.experimental import pallas as pl
from jax.experimental.pallas import tpu as pltpu
from jax.sharding import PartitionSpec as P

GRID = 64
SPACING = 64
ROWS = 256
COLS = 4096
BLOCK = 1024
STEPS = COLS // BLOCK
CHUNK = 32
EXT = 72
PIXELS = 4096.0 * 4096.0
EPS = 1e-6
RATE = 0.25
SMOOTH = 0.25
BF = jnp.bfloat16
F32 = jnp.float32


def weight(offset, xp):
    d = xp.abs(offset)
    near = 2.0 / 3.0 - d * d + 0.5 * d * d * d
    r = 2.0 - d
    far = r * r * r / 6.0
    return xp.where(d < 1.0, near, xp.where(d < 2.0, far, 0.0 * d))


def local_rows():
    r = np.arange(ROWS, dtype=np.float32)
    j = np.arange(8, dtype=np.float32) - 2.0
    off = (r[:, None] + np.float32(0.5)) / np.float32(SPACING) - j[None, :] - np.float32(0.5)
    return weight(off.astype(np.float32), np).astype(np.float32)


def hi_lo(a):
    hi = a.astype(BF)
    return hi, (a - hi.astype(F32)).astype(BF)


def split3(a):
    hi = a.astype(BF)
    rest = a - hi.astype(F32)
    mid = rest.astype(BF)
    lo = (rest - mid.astype(F32)).astype(BF)
    return jnp.concatenate([hi.astype(F32), mid.astype(F32), lo.astype(F32)], axis=0).astype(BF)


def sum3(a, n):
    return a[0:n] + a[n : 2 * n] + a[2 * n : 3 * n]


def two(a):
    hi = a.astype(np.dtype(BF)).astype(np.float32)
    return np.concatenate([hi, a - hi], 0)


def host_tables():
    r8 = local_rows()
    pairs = np.zeros((32, ROWS), np.float32)
    c8 = r8.astype(np.dtype(BF)).astype(np.float32)
    lanes = np.zeros((BLOCK, 128), np.float32)
    cols = np.zeros((BLOCK, 128), np.float32)
    place = np.zeros((STEPS * 128, 256), np.float32)
    put = np.zeros((STEPS * 128, 128), np.float32)
    for s in range(4):
        cols[256 * s : 256 * s + 256, 8 * s : 8 * s + 8] = c8
    for d in range(4):
        for e in range(8 - d):
            pairs[d * 8 + e] = r8[:, e] * r8[:, e + d]
            for s in range(4):
                lanes[256 * s : 256 * s + 256, 32 * s + 8 * d + e] = c8[:, e] * c8[:, e + d]
                for t in range(STEPS):
                    i = 16 * t + 4 * s - 2 + e
                    if i >= 0 and i + d < GRID:
                        place[128 * t + 32 * s + 8 * d + e, 64 * d + i] = 1.0
    for t in range(STEPS):
        for s in range(4):
            for e in range(8):
                i = 16 * t + 4 * s - 2 + e
                if 0 <= i < GRID:
                    put[128 * t + 8 * s + e, i] = 1.0
    diff = np.zeros((8, ROWS), np.float32)
    diff[:, 1:] += 0.5 * r8.T[:, :-1]
    diff[:, :-1] -= 0.5 * r8.T[:, 1:]
    lanes_hi = lanes.astype(np.dtype(BF)).astype(np.float32)
    down = 0.5 * (np.eye(ROWS, k=1) - np.eye(ROWS, k=-1))
    across = np.zeros((512, 256), np.float32)
    o = np.arange(256)
    across[o + 129, o] = 0.5
    across[o + 127, o] = -0.5
    plain = np.concatenate([two(r8.T), two(diff), np.ones((16, ROWS), np.float32)], 0)
    wide = np.concatenate([lanes_hi, lanes - lanes_hi], 1)
    halves = np.concatenate([np.concatenate([cols[0:512], cols[512:1024]], 1), np.concatenate([put[0:256], put[256:512]], 1)], 0)
    blob = np.concatenate([down, across, two(pairs), two(r8.T), plain, wide, place, halves], 0)
    edge = np.stack([-0.5 * r8[0], 0.5 * r8[ROWS - 1]], 0).reshape(16, 1) * np.ones((1, 128), np.float32)
    return r8, jnp.asarray(blob.astype(np.dtype(BF))), jnp.asarray(edge.astype(np.float32))


DOWN, ACROSS, PAIRS, LIN, PLAIN, TABLE, PLACE, COLT, PUT = 0, 256, 768, 832, 848, 896, 1920, 2432, 2944


def col_part(blob_ref, lhs):
    return dot(lhs[:, 0:512], blob_ref[COLT : COLT + 512, 0:128]) + dot(lhs[:, 512:1024], blob_ref[COLT : COLT + 512, 128:256])


def put_rows(blob_ref, t):
    return blob_ref[PUT + 128 * (t % 2) : PUT + 128 * (t % 2) + 128, 128 * (t // 2) : 128 * (t // 2) + 128]


def col_table():
    x = jnp.arange(COLS, dtype=jnp.int32).astype(F32)
    j = jnp.arange(GRID, dtype=jnp.int32).astype(F32)
    return weight((x[None, :] + 0.5) / SPACING - j[:, None] - 0.5, jnp).astype(BF)


def dot(a, b):
    return jnp.dot(a, b, preferred_element_type=F32)


def tile(step, size=BLOCK):
    return pl.ds(pl.multiple_of(size * step, size), size)


def slopes(pos_ref, m_ref, up_ref, dn_ref, blob_ref, lhs, xs, ys, step):
    start = BLOCK * step
    left = m_ref[:, pl.ds(pl.multiple_of(jnp.maximum(start - 128, 0), 128), 128)]
    right = m_ref[:, pl.ds(pl.multiple_of(jnp.minimum(start + BLOCK, COLS - 128), 128), 128)]
    left = jnp.where(step > 0, left.astype(F32), 0.0).astype(BF)
    right = jnp.where(step < STEPS - 1, right.astype(F32), 0.0).astype(BF)
    block = m_ref[:, tile(step)]
    ext = jnp.concatenate([left, block, right], axis=1)
    stack = jnp.concatenate([ext[:, 256 * s : 256 * s + 512] for s in range(4)], axis=0)
    x = dot(stack, blob_ref[ACROSS : ACROSS + 512, :])
    for s in range(4):
        xs[:, pl.ds(pl.multiple_of(start + 256 * s, 256), 256)] = x[256 * s : 256 * s + 256]
    up = jnp.where(pos_ref[1] > 0, up_ref[:, tile(step)].astype(F32), 0.0)
    dn = jnp.where(pos_ref[1] < 15, dn_ref[:, tile(step)].astype(F32), 0.0)
    both = dot(jnp.concatenate([blob_ref[DOWN : DOWN + 256, :], lhs], axis=0), block)
    at = tile(step)
    ys[:, at] = both[0:256]
    ys[0:1, at] = ys[0:1, at] - 0.5 * up
    ys[ROWS - 1 : ROWS, at] = ys[ROWS - 1 : ROWS, at] + 0.5 * dn
    return up, dn, both[256:]


def fold8(a):
    return jnp.sum(a.reshape(CHUNK // 8, 8, a.shape[1]), axis=0)


def lanes_to_row(a):
    s = jnp.sum(a, axis=0, keepdims=True)
    out = s[:, 0:128]
    for t in range(1, s.shape[1] // 128):
        out = out + s[:, 128 * t : 128 * t + 128]
    return out


def rows_of(lin, hi, lo):
    a = dot(lin, hi)
    b = dot(lin, lo)
    return a[0:8] + a[8:16] + b[0:8]


def stage0(pos_ref, m_ref, up_ref, dn_ref, blob_ref, edge_ref, anchor_hbm, h_ref, p_ref, xs, ys, anchor_ref, fetched, fxx, fxy, fyy, mxh, mxl, myh, myl, zacc, lacc, l1_ref, sums):
    bring = pltpu.make_async_copy(anchor_hbm, anchor_ref, fetched)
    bring.start()
    sums[...] = jnp.zeros((8, 128), F32)

    def body(step, carry):
        up, dn, ones = slopes(pos_ref, m_ref, up_ref, dn_ref, blob_ref, blob_ref[PLAIN : PLAIN + 48, :], xs, ys, step)
        pairs = blob_ref[PAIRS : PAIRS + 64, :]
        lin = blob_ref[LIN : LIN + 16, :]
        sumsq = jnp.zeros((8, 256), F32)
        t_parts, lx, ly = [], [], []
        for s in range(BLOCK // 256):
            at = pl.ds(256 * s, 256)
            from_m = pl.ds(pl.multiple_of(BLOCK * step + 256 * s, 256), 256)
            for c in range(ROWS // CHUNK):
                rows = pl.ds(CHUNK * c, CHUNK)
                m, x, y = m_ref[rows, from_m].astype(F32), xs[rows, from_m], ys[rows, from_m]
                fxx[rows, at] = (x * x).astype(BF)
                fxy[rows, at] = (x * y).astype(BF)
                fyy[rows, at] = (y * y).astype(BF)
                mxh[rows, at], mxl[rows, at] = hi_lo(m * x)
                myh[rows, at], myl[rows, at] = hi_lo(m * y)
                sumsq = sumsq + fold8(m * m)
            trio = []
            for f in (fxx, fxy, fyy):
                t = dot(pairs, f[:, at])
                trio.append(t[0:32] + t[32:64])
            t_parts.append(jnp.concatenate(trio, axis=0))
            lx.append(rows_of(lin, mxh[:, at], mxl[:, at]))
            ly.append(rows_of(lin, myh[:, at], myl[:, at]))
        t_hi, t_lo = hi_lo(jnp.concatenate(t_parts, axis=1))
        z = dot(jnp.concatenate([t_hi, t_lo], axis=0), blob_ref[TABLE : TABLE + 1024, :])
        z = z[0:96] + z[96:192]
        zacc[tile(step, 96), :] = z[:, 0:128] + z[:, 128:256]
        l1_ref[:, tile(step)] = ones[0:8] + ones[8:16]
        l1y = ones[16:24] + ones[24:32]
        l1y = l1y + edge_ref[0:8, 0:1] * up + edge_ref[8:16, 0:1] * dn
        rows3 = jnp.concatenate([jnp.concatenate(lx, axis=1), jnp.concatenate(ly, axis=1), l1y], axis=0)
        lacc[tile(step, 24), :] = sum3(col_part(blob_ref, split3(rows3)), 24)
        sums[0:1, :] += lanes_to_row(ones[32:33])
        sums[1:2, :] += lanes_to_row(sumsq)
        return carry

    lax.fori_loop(0, STEPS, body, 0)
    bring.wait()
    l1 = l1_ref[...]
    col = lax.broadcasted_iota(jnp.int32, l1.shape, 1)
    after = jnp.where(col < COLS - 1, pltpu.roll(l1, COLS - 1, 1), 0.0)
    before = jnp.where(col > 0, pltpu.roll(l1, 1, 1), 0.0)
    l1x = split3(0.5 * (after - before))
    h = jnp.zeros((288, 256), F32)
    p = jnp.zeros((96, 128), F32)
    for t in range(STEPS):
        h = h + dot(split3(zacc[96 * t : 96 * t + 96, :]), blob_ref[PLACE + 128 * t : PLACE + 128 * t + 128, :])
        one = sum3(col_part(blob_ref, l1x[:, BLOCK * t : BLOCK * t + BLOCK]), 8)
        p = p + dot(split3(jnp.concatenate([lacc[24 * t : 24 * t + 24, :], one], axis=0)), put_rows(blob_ref, t))
    h_ref[...] = sum3(h, 96)
    p = sum3(p, 32)
    p_ref[0:8, :] = p[0:8] + pltpu.roll(p[8:16], 64, 1)
    p_ref[8:16, :] = p[24:32] + pltpu.roll(p[16:24], 64, 1)
    p_ref[16:24, :] = sums[...]


def cross_part(pos_ref, m_ref, xs, ys, blob_ref, anchor_ref, prior_ref, fxh, fxl, fyh, fyl, lacc, sums):
    sums[...] = jnp.zeros((8, 128), F32)

    def body(f_ref, step, carry):
        lin = blob_ref[LIN : LIN + 16, :]
        cross = jnp.zeros((8, 256), F32)
        whole_sum = jnp.zeros((8, 256), F32)
        lx, ly = [], []
        for s in range(BLOCK // 256):
            at = pl.ds(256 * s, 256)
            from_m = pl.ds(pl.multiple_of(BLOCK * step + 256 * s, 256), 256)
            for c in range(ROWS // CHUNK):
                rows = pl.ds(CHUNK * c, CHUNK)
                m, x, y = m_ref[rows, from_m].astype(F32), xs[rows, from_m], ys[rows, from_m]
                f = f_ref[rows, from_m].astype(F32)
                fxh[rows, at], fxl[rows, at] = hi_lo(f * x)
                fyh[rows, at], fyl[rows, at] = hi_lo(f * y)
                cross = cross + fold8(f * m)
                whole_sum = whole_sum + fold8(f)
            lx.append(rows_of(lin, fxh[:, at], fxl[:, at]))
            ly.append(rows_of(lin, fyh[:, at], fyl[:, at]))
        rows2 = jnp.concatenate([jnp.concatenate(lx, axis=1), jnp.concatenate(ly, axis=1)], axis=0)
        lacc[tile(step, 16), :] = sum3(col_part(blob_ref, split3(rows2)), 16)
        sums[0:1, :] += lanes_to_row(cross)
        sums[1:2, :] += lanes_to_row(whole_sum)
        return carry

    @pl.when(pos_ref[0] == 0)
    def _():
        lax.fori_loop(0, STEPS, lambda i, c: body(anchor_ref, i, c), 0)

    @pl.when(pos_ref[0] > 0)
    def _():
        lax.fori_loop(0, STEPS, lambda i, c: body(prior_ref, i, c), 0)

    p = jnp.zeros((48, 128), F32)
    for i in range(STEPS):
        p = p + dot(split3(lacc[16 * i : 16 * i + 16, :]), put_rows(blob_ref, i))
    p = sum3(p, 16)
    return p[0:8] + pltpu.roll(p[8:16], 64, 1)


def rows8(shape):
    return lax.broadcasted_iota(jnp.int32, shape, 0) % 8


def stage1(pos_ref, m_ref, xs, ys, blob_ref, anchor_ref, prior_ref, h_ref, p_ref, out_ref, *scratch):
    sums = scratch[-1]
    part = cross_part(pos_ref, m_ref, xs, ys, blob_ref, anchor_ref, prior_ref, *scratch)
    row = rows8((8, 256))
    lane = lax.broadcasted_iota(jnp.int32, (8, 256), 1)
    last = jnp.zeros((8, 256), F32)
    for t, v in enumerate((sums[0:1, :], sums[1:2, :], p_ref[16:17, :], p_ref[17:18, :])):
        rest = jnp.sum(v, axis=1, keepdims=True)
        for u in range(3):
            piece = rest.astype(BF).astype(F32)
            rest = rest - piece
            last = last + jnp.where((row == 6) & (lane == 4 * u + t), piece, 0.0)
    groups = []
    lows = []
    for c in range(3):
        a, b, d, e = [h_ref[32 * c + 8 * t : 32 * c + 8 * t + 8, :] for t in range(4)]
        groups += [a, b + jnp.where(row == 7, pltpu.roll(e, 3, 0), 0.0), d + jnp.where(row > 5, pltpu.roll(e, 4, 0), 0.0)]
        last = last + jnp.where((row == 2 * c) | (row == 2 * c + 1), shifted(e, 2 * c, 0), 0.0)
        low = [v[:, 0:128] - v[:, 0:128].astype(BF).astype(F32) for v in (a, b)]
        lows.append(jnp.concatenate(low, axis=1))
    groups.append(last)
    groups += lows
    for v in (part, p_ref[0:8, :], p_ref[8:16, :]):
        groups.append(jnp.concatenate([v, v - v.astype(BF).astype(F32)], axis=1))
    packed = jnp.concatenate(groups, axis=0).astype(BF)
    out_ref[...] = packed


def shifted(a, by, axis):
    n = a.shape[axis]
    by = by % n
    return a if by == 0 else pltpu.roll(a, by, axis)


def stacked(even, odd):
    pad = jnp.zeros((8, even.shape[1]), F32)
    return jnp.concatenate([even, pad], axis=0) + pltpu.roll(jnp.concatenate([odd, pad], axis=0), 4, 0)


def merge(pos_ref, near0, near1, near2, near3, out_ref, all_ref):
    y = pos_ref[1] % 4
    for e, ref in enumerate((near0, near1, near2, near3)):
        all_ref[(y + 4 - e) % 4] = ref[...]
    groups = [([], []) for _ in range(16)]
    for q in range(4):
        for t in range(8):
            both = all_ref[q, 16 * t : 16 * t + 16, :].astype(F32)
            groups[2 * t][q % 2].append(both[0:8])
            groups[2 * t + 1][q % 2].append(both[8:16])
    groups = [[jnp.concatenate(v, axis=0) for v in pair] for pair in groups]
    row = rows8((16, 256))
    pad = jnp.zeros((16, 128), F32)

    def piece(c, dj, side):
        a, b, d, last, rest = [groups[g][side] for g in (3 * c, 3 * c + 1, 3 * c + 2, 9, 10 + c)]
        if dj == 0:
            return a + jnp.concatenate([rest[:, 0:128], pad], axis=1)
        if dj == 1:
            return jnp.where(row < 7, b, 0.0) + jnp.concatenate([rest[:, 128:256], pad], axis=1)
        if dj == 2:
            return jnp.where(row < 6, d, 0.0)
        e = jnp.where(row == 4, pltpu.roll(b, 13, 0), jnp.where(row > 1, pltpu.roll(d, 12, 0), shifted(last, -2 * c, 0)))
        return jnp.where(row < 5, e, 0.0)

    items, lows = [], []
    for c in range(3):
        four = [stacked(piece(c, dj, 0), piece(c, dj, 1)) for dj in range(4)]
        items += four
        lows.append(jnp.concatenate([v[:, 0:128] - v[:, 0:128].astype(BF).astype(F32) for v in four[0:2]], axis=1))
    last = groups[9][0] + groups[9][1]
    lane = lax.broadcasted_iota(jnp.int32, (16, 256), 1)
    here = (row == 6) & (lane < 12)
    row24 = lax.broadcasted_iota(jnp.int32, (24, 256), 0)
    lane24 = lax.broadcasted_iota(jnp.int32, (24, 256), 1)
    for t in range(4):
        rest = total(jnp.where(here & (lane % 4 == t), last, 0.0))
        for u in range(3):
            part = rest.astype(BF).astype(F32)
            rest = rest - part
            items[3] = items[3] + jnp.where((row24 == 19) & (lane24 == 4 * u + t), part, 0.0)
    items += lows
    for g in (13, 14, 15):
        even, odd = [v[:, 0:128] + v[:, 128:256] for v in groups[g]]
        v = stacked(even, odd)
        items.append(jnp.concatenate([v, v - v.astype(BF).astype(F32)], axis=1))
    room = jnp.zeros((16, 256), F32)
    pairs = []
    for p in range(9):
        a, b = [jnp.concatenate([v, room], axis=0) for v in items[2 * p : 2 * p + 2]]
        pairs.append(a + pltpu.roll(b, 20, 0))
    out_ref[...] = jnp.concatenate(pairs, axis=0).astype(BF)


def unpack(pos_ref, far, all_ref):
    z = pos_ref[1] // 4
    for d in range(4):
        all_ref[(z + 4 - d) % 4] = far[d][...]
    blocks = [all_ref[t].astype(F32) for t in range(4)]
    row = lax.broadcasted_iota(jnp.int32, (8, 256), 0)
    lane = lax.broadcasted_iota(jnp.int32, (8, 256), 1)
    eight = jnp.zeros((8, 256), F32)
    out = []
    sums = None
    for i in range(18):
        body, tails = [], [eight, eight]
        for t in range(4):
            full = blocks[t][40 * (i // 2) : 40 * (i // 2) + 40]
            if i % 2:
                full = pltpu.roll(full, 20, 0)
            body.append(full[0:16])
            tail = full[16:24]
            if i == 3:
                sums = tail if sums is None else sums + tail
            tails += [jnp.where(row < (3 if i == 3 else 4), tail, 0.0), eight]
        out.append(jnp.concatenate(body + [eight], axis=0) + jnp.concatenate(tails[:-1], axis=0))
    here = (row == 3) & (lane < 12)
    return out, [total(jnp.where(here & (lane % 4 == t), sums, 0.0)) for t in range(4)]


def build_operator(items, a1, a2):
    lane = lax.broadcasted_iota(jnp.int32, (EXT, 128), 1)
    low = lane < 64
    for dj in range(4):
        for pair in range(2):
            three = []
            for c in range(3):
                v = items[4 * c + dj][:, 128 * pair : 128 * pair + 128]
                if pair == 0 and dj < 2:
                    v = v + items[12 + c][:, 128 * dj : 128 * dj + 128]
                three.append(v)
            xx, xy, yy = three
            xx_s, xy_s, yy_s = [pltpu.roll(v, 64, 1) for v in (xx, xy, yy)]
            for odd in range(2):
                di = 2 * pair + odd
                if odd == 0:
                    one = jnp.where(low, xx, yy_s)
                    two = jnp.where(low, xy, xy_s)
                else:
                    one = jnp.where(low, xx_s, yy)
                    two = jnp.where(low, xy_s, xy)
                a1[dj * 7 + 3 + di] = one
                a2[dj * 7 + 3 + di] = two
                if di > 0:
                    a1[dj * 7 + 3 - di] = pltpu.roll(one, di, 1)
                    a2[dj * 7 + 3 - di] = pltpu.roll(two, di, 1)


def apply_operator(a1, a2, c):
    cs = pltpu.roll(c, 64, 1)
    plain = [(shifted(c, -di, 1), shifted(cs, -di, 1)) for di in range(-3, 4)]
    y = jnp.zeros((EXT, 128), F32)
    for dj in range(4):
        ahead = jnp.zeros((EXT, 128), F32)
        back = jnp.zeros((EXT, 128), F32)
        for t in range(7):
            p, s = plain[t]
            u, v = a1[dj * 7 + t], a2[dj * 7 + t]
            ahead = ahead + u * shifted(p, -dj, 0) + v * shifted(s, -dj, 0)
            if dj:
                back = back + u * p + v * s
        y = y + ahead
        if dj:
            y = y + pltpu.roll(back, dj, 0)
    return y


def total(a):
    return jnp.sum(jnp.sum(a, axis=0, keepdims=True), axis=1, keepdims=True)


def fields(items):
    row = lax.broadcasted_iota(jnp.int32, (EXT, 128), 0)
    valid = (row >= 2) & (row < 66)
    return valid, [jnp.where(valid, v[:, 0:128] + v[:, 128:256], 0.0) for v in items[15:18]]


def narrow(a):
    return pltpu.roll(a, EXT - 2, 0)[0:GRID]


def widen(a):
    return pltpu.roll(jnp.concatenate([a, jnp.zeros((EXT - GRID, 128), F32)], axis=0), 2, 0)


def direction(valid, grads, sums, c, hc):
    gf, gm, g1 = grads
    s_fm, s_f, s_m, s_mm = sums
    mean_f = s_f / PIXELS
    if c is None:
        s_w, s_ww, s_fw, gw = s_m, s_mm, s_fm, gm
    else:
        s_w = s_m + total(g1 * c)
        s_ww = s_mm + total(c * (2.0 * gm + hc))
        s_fw = s_fm + total(gf * c)
        gw = gm + hc
    mean_w = s_w / PIXELS
    var = s_ww - PIXELS * mean_w * mean_w
    cross = s_fw - PIXELS * mean_f * mean_w
    den = jnp.sqrt(var + EPS)
    ratio = cross / den / (var + EPS)
    g = PIXELS * ((gf - mean_f * g1) / den - ratio * (gw - mean_w * g1))
    g = jnp.where(valid, g, 0.0)
    return g / jnp.sqrt(total(g * g) / 8192.0 + EPS)


def solve_a(pos_ref, far0, far1, far2, far3, out_ref, lead_ref, a1, a2, kept_ref, all_ref):
    items, sums = unpack(pos_ref, (far0, far1, far2, far3), all_ref)
    build_operator(items, a1, a2)
    valid, grads = fields(items)
    for t in range(3):
        kept_ref[EXT * t : EXT * t + EXT, :] = grads[t]
    for t in range(4):
        kept_ref[3 * EXT + t : 3 * EXT + t + 1, :] = jnp.broadcast_to(sums[t], (1, 128))
    c = RATE * direction(valid, grads, sums, None, None)
    d = direction(valid, grads, sums, c, apply_operator(a1, a2, c))
    lead = narrow(c)
    out_ref[0:GRID, :] = lead
    lead_ref[...] = lead
    out_ref[GRID : 2 * GRID, :] = narrow(d)


def solve_b(pos_ref, a1, a2, kept_ref, own_ref, prev_ref, next_ref, prev2_ref, next2_ref, out_ref):
    k = pos_ref[0]
    row = lax.broadcasted_iota(jnp.int32, (EXT, 128), 0)
    valid = (row >= 2) & (row < 66)
    grads = [kept_ref[EXT * t : EXT * t + EXT, :] for t in range(3)]
    sums = [kept_ref[3 * EXT + t : 3 * EXT + t + 1, 0:1] for t in range(4)]

    def lap(a, b, c):
        return a - 2.0 * b + c

    def pair(ref, there):
        return [jnp.where(there, widen(ref[GRID * t : GRID * t + GRID, :]), 0.0) for t in range(2)]

    has_prev, has_next = k > 0, k < 7
    c1, d1 = pair(own_ref, k >= 0)
    cl, dl = pair(prev_ref, has_prev)
    cr, dr = pair(next_ref, has_next)
    cll = jnp.where(k > 1, widen(prev2_ref[...]), 0.0)
    crr = jnp.where(k < 6, widen(next2_ref[...]), 0.0)
    c2 = c1 + RATE * d1 + SMOOTH * lap(cl, c1, cr)
    c2l = jnp.where(has_prev, cl + RATE * dl + SMOOTH * lap(cll, cl, c1), 0.0)
    c2r = jnp.where(has_next, cr + RATE * dr + SMOOTH * lap(c1, cr, crr), 0.0)
    d2 = direction(valid, grads, sums, c2, apply_operator(a1, a2, c2))
    c3 = c2 + RATE * d2 + SMOOTH * lap(c2l, c2, c2r)
    d3 = direction(valid, grads, sums, c3, apply_operator(a1, a2, c3))
    out_ref[0:GRID, :] = narrow(c3 + RATE * d3)
    out_ref[GRID : 2 * GRID, :] = narrow(c3)


def pair_sum(pos_ref, own_ref, other_ref, out_ref, more_ref):
    k = pos_ref[0]
    even = jnp.where(k % 2 == 0, own_ref[GRID : 2 * GRID, :], other_ref[GRID : 2 * GRID, :])
    both = own_ref[0:GRID, :] + other_ref[0:GRID, :] - jnp.where(k < 2, SMOOTH, 0.0) * even
    out_ref[...] = both
    more_ref[0:GRID, :] = both
    more_ref[GRID : 2 * GRID, :] = even


def finish(pos_ref, m_ref, xs, ys, own_ref, other_ref, one_ref, two_ref, more_ref, r8_hbm, turned_ref, out_ref, acc_ref, sx, sy, total_ref, mixed, buf, r8_ref, sems, fetched):
    bring = pltpu.make_async_copy(r8_hbm, r8_ref, fetched)
    bring.start()
    k = pos_ref[0]
    odd = k % 2 == 1
    own_c, other_c = own_ref[GRID : 2 * GRID, :], other_ref[GRID : 2 * GRID, :]
    after = jnp.where(odd, jnp.where(k < 7, more_ref[GRID : 2 * GRID, :], 0.0), other_c)
    acc = own_ref[0:GRID, :] + jnp.where(odd, other_ref[0:GRID, :], 0.0) + SMOOTH * (after - own_c)
    acc = acc - jnp.where(k < 2, SMOOTH, 0.0) * jnp.where(odd, other_c, own_c)
    acc = acc + jnp.where(k > 1, one_ref[...], 0.0) + jnp.where(k > 3, two_ref[...], 0.0)
    acc = acc + jnp.where(k > 5, more_ref[0:GRID, :], 0.0)
    acc_ref[...] = acc
    total_ref[...] = widen(acc)
    c8 = total_ref[pl.ds(4 * pos_ref[1], 8), :]
    bring.wait()
    mixed[...] = jnp.dot(r8_ref[...], c8, precision=lax.Precision.HIGHEST, preferred_element_type=F32).astype(BF)

    def copy(step):
        return pltpu.make_async_copy(buf.at[:, tile(step)], out_ref.at[:, tile(step)], sems.at[step])

    def body(step, carry):
        sx[...] = dot(mixed[:, 0:64], turned_ref[:, tile(step)])
        sy[...] = dot(mixed[:, 64:128], turned_ref[:, tile(step)])
        for s in range(BLOCK // 256):
            at = pl.ds(256 * s, 256)
            from_m = pl.ds(pl.multiple_of(BLOCK * step + 256 * s, 256), 256)
            for c in range(ROWS // CHUNK):
                rows = pl.ds(CHUNK * c, CHUNK)
                m = m_ref[rows, from_m].astype(F32)
                buf[rows, from_m] = (m + sx[rows, at] * xs[rows, from_m] + sy[rows, at] * ys[rows, from_m]).astype(BF)
        copy(step).start()
        return carry

    lax.fori_loop(0, STEPS, body, 0)
    for step in range(STEPS):
        copy(step).wait()


def around_four(array, stride, by):
    def to(q):
        here = q // stride % 4
        return q + stride * ((here + by) % 4 - here)

    return lax.ppermute(array, "quad", [(q, to(q)) for q in range(16)])


def ring(array, axis, by):
    n = lax.axis_size(axis)
    return lax.ppermute(array, axis, [(i, (i + by) % n) for i in range(n)])


FIELD = pltpu.VMEM((ROWS, BLOCK), BF)
WIDE = pltpu.VMEM((ROWS, BLOCK), F32)
SMALL = pltpu.VMEM((8, 128), F32)


def call(kernel, args, outs, scratch, limit, hbm_out=False, hbm_in=()):
    def body(*refs):
        kernel((lax.axis_index("chain"), lax.axis_index("quad")), *refs)

    vm = pl.BlockSpec(memory_space=pltpu.VMEM)
    specs = [vm] * len(args)
    for i in hbm_in:
        specs[i] = pl.BlockSpec(memory_space=pltpu.HBM)
    return pl.pallas_call(
        body,
        in_specs=specs,
        out_specs=[pl.BlockSpec(memory_space=pl.ANY) if hbm_out and i == 0 else vm for i in range(len(outs))],
        out_shape=outs,
        scratch_shapes=scratch,
        compiler_params=pltpu.CompilerParams(vmem_limit_bytes=limit << 20),
    )(*args)


def registration(sections, anchor):
    strip = sections[0]
    r8, blob, edge = host_tables()
    prior = ring(strip, "chain", 1)
    up = ring(strip[ROWS - 1 : ROWS], "quad", 1)
    dn = ring(strip[0:1], "quad", -1)
    turned = col_table()
    shape = jax.ShapeDtypeStruct
    slope = shape((ROWS, COLS), F32)
    h, p, xs, ys, before = call(
        stage0,
        (strip, up, dn, blob, edge, anchor),
        [shape((96, 256), F32), shape((24, 128), F32), slope, slope, shape((ROWS, COLS), BF)],
        [pltpu.SemaphoreType.DMA] + [FIELD] * 7 + [pltpu.VMEM((96 * STEPS, 128), F32), pltpu.VMEM((24 * STEPS, 128), F32), pltpu.VMEM((8, COLS), F32), SMALL],
        24,
        hbm_in=(5,),
    )
    (packed,) = call(
        stage1,
        (strip, xs, ys, blob, before, prior, h, p),
        [shape((128, 256), BF)],
        [FIELD] * 4 + [pltpu.VMEM((16 * STEPS, 128), F32), SMALL],
        20,
    )
    packed, turned = lax.optimization_barrier((packed, turned))
    four = [packed] + [around_four(packed, 1, d) for d in (1, 2, 3)]
    (near,) = call(merge, tuple(four), [shape((360, 256), BF)], [pltpu.VMEM((4, 128, 256), BF)], 12)
    far = [near] + [around_four(near, 4, d) for d in (1, 2, 3)]
    operator = [shape((28, EXT, 128), F32)] * 2
    first, lead, a1, a2, kept = call(
        solve_a,
        tuple(far),
        [shape((2 * GRID, 128), F32), shape((GRID, 128), F32), *operator, shape((3 * EXT + 8, 128), F32)],
        [pltpu.VMEM((4, 360, 256), BF)],
        12,
    )
    around = [ring(first, "chain", 1), ring(first, "chain", -1), ring(lead, "chain", 2), ring(lead, "chain", -2)]
    (own,) = call(solve_b, (a1, a2, kept, first, *around), [shape((2 * GRID, 128), F32)], [], 12)
    other = lax.ppermute(own, "chain", [(i, i ^ 1) for i in range(8)])
    both, more = call(pair_sum, (own, other), [shape((GRID, 128), F32), shape((2 * GRID, 128), F32)], [], 12)
    steps = ((both, 2), (both, 4), (more, -2))
    earlier = [ring(a, "chain", by) for a, by in steps]
    registered, accumulated = call(
        finish,
        (strip, xs, ys, own, other, *earlier, jnp.asarray(r8), turned),
        [shape((ROWS, COLS), BF), shape((GRID, 128), F32)],
        [WIDE] * 2
        + [pltpu.VMEM((EXT, 128), F32), pltpu.VMEM((ROWS, 128), BF), pltpu.VMEM((ROWS, COLS), BF), pltpu.VMEM((ROWS, 8), F32)]
        + [pltpu.SemaphoreType.DMA((STEPS,)), pltpu.SemaphoreType.DMA],
        24,
        hbm_out=True,
        hbm_in=(8,),
    )
    return registered[None], accumulated[None]


def solution(mesh):
    in_specs = (P("chain", "quad", None), P("quad", None))
    out_specs = (P("chain", "quad", None), P("chain", None, None))
    return jax.shard_map(registration, mesh=mesh, in_specs=in_specs, out_specs=out_specs, check_vma=False)
```
